32 devices in a mesh: rep: 2 (over y), gx: 16 (over z, x, core).
Axes of the slice: x: 2, y: 2, z: 4, core: 2. Of those that a mesh axis runs over, the one named last changes fastest.
Arguments:
- positions: float32 [3, 32768], P(None, ('rep', 'gx')), parts along dimension 1, may hold values from 0 to 8, as said below
- field: float32 [3, 32768], P(None, ('rep', 'gx')), parts along dimension 1, may hold values from -45 to 45
- inv_polar: float32 [32768], P(('rep', 'gx')), parts along dimension 0, may hold values from 2 to 8
- x_spline: float32 [2, 5, 32768], P(None, None, ('rep', 'gx')), parts along dimension 2, may hold values from -1 to 1, as said below
- yz_spline: float32 [4, 32768, 128], P(None, ('rep', 'gx')), parts along dimension 1, may hold values from -1 to 1, as said below
- tile_list: int32 [256, 7], P(('rep', 'gx')), parts along dimension 0, may hold values from 0 to 13, as said below
- tile_count: int32 [256], P(('rep', 'gx')), parts along dimension 0, may hold values from 1 to 7, as said below
Outputs:
- dipoles: float32 [3, 32768], P(None, ('rep', 'gx')), parts along dimension 1
- residual: float32 [3, 32768], P(None, ('rep', 'gx')), parts along dimension 1
The draws below stay inside these ranges and needn't reach their ends.
There are 2 independent parts, one for each index of `rep`. The reference program is written for one: setup_inputs(seed, part) draws one part's arguments, and reference() takes and returns one part's arrays. A program takes and returns all parts, laid end to end along the dimension named above; each array names one. Nothing has to cross between parts.
Inputs may be any that keep to these rules, and one draw needn't show every extreme that they name: `positions`: the first coordinate of an atom of block b of its slab lies in [b, b + 1); the other two lie in [0, 2). x_spline[0, k, i] and x_spline[1, k, i] are the cardinal B-spline of order 5 and its derivative at u_i + 4 - k for some u_i in [0, 1). `yz_spline`: rows 0 and 1 hold, for each atom, the cardinal B-spline of order 5 and its derivative at u + 4 - k placed at grid line (t + k) mod 128 for k < 5, for some start t and some u in [0, 1), and zero elsewhere; rows 2 and 3 likewise with their own start and offset. `tile_list`: row g = s * 8 + b lists in rising order the extended blocks b + 3 + e, -3 <= e <= 3, for which global blocks g and g + e (modulo 128) are neighbours; being neighbours is symmetric and always holds for e = 0; entries from tile_count[g] on equal b + 3. `tile_count`: global block 0 has all 7 neighbours.
All inputs are finite; a program needn't handle non-finite values.
Results may differ from the reference program's by a relative error of at most 0.0003.
Values sent between devices are 32-bit elements; how exact they have to be, the bound alone decides.
No kernel may reach another device: no remote copies, remote signals or barrier semaphores. Data moves between devices by JAX's collectives and lax.ppermute only.
A program may use at most 64 MiB of HBM per device.

```python
import math
import jax
import jax.numpy as jnp
from jax import lax

GRID = 128
ORDER = 5
TILE = 128
HALO_BLK = 3
ITERS = 3
ATOM_DEV = 1024
NNB = 7
ATOMS = 16384
SLAB_BLOCKS = 8
BLOCKS = 128
N_GX = 16


def cardinal(order_now, at_point):
    if order_now == 2:
        return jnp.maximum(0.0, 1.0 - jnp.abs(at_point - 1.0))
    lower_part = cardinal(order_now - 1, at_point)
    upper_part = cardinal(order_now - 1, at_point - 1.0)
    return (at_point * lower_part + (order_now - at_point) * upper_part) / (order_now - 1)


def spline_pair(frac):
    shifts = (ORDER - 1 - jnp.arange(ORDER, dtype=jnp.int32)).astype(jnp.float32)
    points = frac[None, :] + shifts[:, None]
    spline_value = cardinal(ORDER, points)
    spline_slope = cardinal(ORDER - 1, points) - cardinal(ORDER - 1, points - 1.0)
    return (spline_value, spline_slope)


def draw_positions(key, part):
    atom_index = jnp.arange(ATOMS, dtype=jnp.int32)
    block_of = (atom_index % ATOM_DEV // TILE).astype(jnp.float32)
    uniform_draw = jax.random.uniform(key, (3, ATOMS), jnp.float32)
    return jnp.stack([block_of + uniform_draw[0], 2.0 * uniform_draw[1], 2.0 * uniform_draw[2]]).astype(jnp.float32)


def draw_field(key, part):
    atom_index = jnp.arange(ATOMS, dtype=jnp.int32)
    slab_of = (atom_index // ATOM_DEV).astype(jnp.float32)
    slab_total = ATOMS // ATOM_DEV
    ramp = 1.0 + 2.0 * slab_of / max(slab_total - 1, 1)
    normal_draw = jnp.clip(jax.random.normal(jax.random.fold_in(key, 1), (3, ATOMS), jnp.float32), -4.0, 4.0)
    return (normal_draw * ramp[None, :]).astype(jnp.float32)


def draw_x_spline(key, part):
    frac = jax.random.uniform(key, (ATOMS,), jnp.float32)
    spline_value, spline_slope = spline_pair(frac)
    return jnp.stack([spline_value, spline_slope]).astype(jnp.float32)


def draw_yz_spline(key, part):
    grid_lines = jnp.arange(GRID, dtype=jnp.int32)
    tables = []
    for axis_code in (1, 2):
        sub_key = jax.random.fold_in(key, axis_code)
        start_line = jax.random.randint(jax.random.fold_in(sub_key, 1), (ATOMS,), 0, GRID, dtype=jnp.int32)
        frac = jax.random.uniform(jax.random.fold_in(sub_key, 2), (ATOMS,), jnp.float32)
        spline_value, spline_slope = spline_pair(frac)
        dense_value = jnp.zeros((ATOMS, GRID), jnp.float32)
        dense_slope = jnp.zeros((ATOMS, GRID), jnp.float32)
        for spline_step in range(ORDER):
            matches = ((start_line + spline_step) % GRID)[:, None] == grid_lines[None, :]
            dense_value = dense_value + jnp.where(matches, spline_value[spline_step][:, None], 0.0)
            dense_slope = dense_slope + jnp.where(matches, spline_slope[spline_step][:, None], 0.0)
        tables.append(dense_value)
        tables.append(dense_slope)
    return jnp.stack(tables).astype(jnp.float32)


def neighbour_table(key):
    block_ids = jnp.arange(BLOCKS, dtype=jnp.int32)
    reach = jnp.arange(1, HALO_BLK + 1, dtype=jnp.int32)
    coins = jax.random.randint(jax.random.fold_in(key, 7), (BLOCKS, HALO_BLK), 0, 2, dtype=jnp.int32)
    first_block = block_ids == 0
    partner = (block_ids[:, None] + reach[None, :]) % BLOCKS
    coins = jnp.where(first_block[:, None] | first_block[partner], 1, coins)
    upper_side = coins
    lower_rows = (block_ids[:, None] - reach[None, :]) % BLOCKS
    lower_side = coins[lower_rows, (reach - 1)[None, :]]
    linked = jnp.concatenate([lower_side[:, ::-1], jnp.ones((BLOCKS, 1), jnp.int32), upper_side], axis=1)
    live_count = jnp.sum(linked, axis=1).astype(jnp.int32)
    slot_ids = jnp.arange(NNB, dtype=jnp.int32)
    sort_keys = jnp.where(linked == 1, slot_ids[None, :], NNB + slot_ids[None, :])
    ordering = jnp.argsort(sort_keys, axis=1, stable=True).astype(jnp.int32)
    local_block = (block_ids % SLAB_BLOCKS)[:, None]
    entries = jnp.where(slot_ids[None, :] < live_count[:, None], local_block + ordering, local_block + HALO_BLK)
    return (entries.astype(jnp.int32), live_count)


def draw_tile_list(key, part):
    entries, live_count = neighbour_table(key)
    return entries


def draw_tile_count(key, part):
    entries, live_count = neighbour_table(key)
    return live_count.astype(jnp.int32)


def levels(stream_key, shape, split, low, high):
    gain, own = 1.0, jax.random.fold_in(stream_key, 6)
    for dim, shards_of in split:
        draws = jnp.exp(jax.random.uniform(jax.random.fold_in(own, dim), (shards_of,), jnp.float32, low / len(split), high / len(split)))
        gain = gain * jnp.repeat(draws, shape[dim] // shards_of).reshape([-1 if axis == dim else 1 for axis in range(len(shape))])
    return gain


def setup_inputs(seed: int = 0, part: int = 0) -> dict:
    keys = jax.random.split(jax.random.key(seed), 8)
    part_keys = jax.random.split(jax.random.fold_in(keys[7], part), 8)
    positions = draw_positions(jax.random.fold_in(jax.random.fold_in(keys[7], part), 71), part)
    field = draw_field(jax.random.fold_in(jax.random.fold_in(keys[7], part), 71), part)
    inv_polar = jnp.clip(jnp.exp(math.log(8.0) - 1.3862944 * jax.random.uniform(part_keys[2], (ATOMS,), jnp.float32) ** levels(part_keys[2], (ATOMS,), ((0, 16),), -0.2, 0.2)), 2.0, 8.0)
    x_spline = draw_x_spline(jax.random.fold_in(jax.random.fold_in(keys[7], part), 71), part)
    yz_spline = draw_yz_spline(jax.random.fold_in(jax.random.fold_in(keys[7], part), 71), part)
    tile_list = draw_tile_list(jax.random.fold_in(jax.random.fold_in(keys[7], part), 71), part)
    tile_count = draw_tile_count(jax.random.fold_in(jax.random.fold_in(keys[7], part), 71), part)
    return {"positions": positions, "field": field, "inv_polar": inv_polar, "x_spline": x_spline, "yz_spline": yz_spline, "tile_list": tile_list, "tile_count": tile_count}


PAIR_C = 0.025
RECIP_C = 8192.0
DAMP = 0.0008
EXACT = lax.Precision.HIGHEST

def pair_field(home_pos, ext_pos, ext_vec, tile_rows, live_counts):
    slab_blocks = home_pos.shape[1] // TILE
    ext_blocks = ext_pos.shape[1] // TILE
    home_blocks = home_pos.reshape(3, slab_blocks, TILE).transpose(1, 0, 2)
    pos_blocks = ext_pos.reshape(3, ext_blocks, TILE)
    vec_blocks = ext_vec.reshape(3, ext_blocks, TILE)
    slot_index = jnp.arange(tile_rows.shape[1], dtype=jnp.int32)
    self_pair = jnp.eye(TILE, dtype=bool)

    def one_block(carried, scan_item):
        home_block, tile_row, live_count, block_index = scan_item
        near_pos = jnp.take(pos_blocks, tile_row, axis=1)
        near_vec = jnp.take(vec_blocks, tile_row, axis=1)
        offsets = home_block[:, None, :, None] - near_pos[:, :, None, :]
        distance_sq = lax.optimization_barrier(jnp.sum(offsets * offsets, axis=0)) + 1.0
        inverse = lax.rsqrt(distance_sq)
        third_power = inverse * inverse * inverse
        fifth_power = third_power * inverse * inverse
        same_block = (tile_row == block_index + HALO_BLK)[:, None, None]
        live_mask = (slot_index < live_count)[:, None, None] & ~(same_block & self_pair[None])
        third_power = jnp.where(live_mask, third_power, 0.0)
        fifth_power = jnp.where(live_mask, fifth_power, 0.0)
        projection = lax.optimization_barrier(jnp.sum(offsets * near_vec[:, :, None, :], axis=0))
        field_sum = lax.optimization_barrier(jnp.sum(third_power[None] * near_vec[:, :, None, :] - 3.0 * (fifth_power * projection)[None] * offsets, axis=(1, 3)))
        return (carried, PAIR_C * field_sum)
    block_ids = jnp.arange(slab_blocks, dtype=jnp.int32)
    unused_carry, blocks_out = lax.scan(one_block, jnp.zeros((), jnp.float32), (home_blocks, tile_rows, live_counts, block_ids))
    return blocks_out.transpose(1, 0, 2).reshape(3, slab_blocks * TILE)

def slab_weights(local_plane, x_spline, planes):
    spline_steps = jnp.arange(ORDER, dtype=jnp.int32)
    plane_index = jnp.arange(planes, dtype=jnp.int32)
    matches = local_plane[None, :, None] + spline_steps[:, None, None] == plane_index[None, None, :]
    spline_value = lax.optimization_barrier(jnp.sum(jnp.where(matches, x_spline[0][:, :, None], 0.0), axis=0))
    spline_slope = lax.optimization_barrier(jnp.sum(jnp.where(matches, x_spline[1][:, :, None], 0.0), axis=0))
    return (spline_value, spline_slope)

def spread_dipoles(vector, spline_value, spline_slope, yz_spline):
    atoms_here = spline_value.shape[0]
    planes = spline_value.shape[1]
    grid_lines = yz_spline.shape[2]
    lead_terms = (vector[0][:, None] * spline_slope)[:, :, None] * yz_spline[0][:, None, :]
    lead_terms = lead_terms + (vector[1][:, None] * spline_value)[:, :, None] * yz_spline[1][:, None, :]
    tail_terms = (vector[2][:, None] * spline_value)[:, :, None] * yz_spline[0][:, None, :]
    contract = (((0,), (0,)), ((), ()))
    charge = lax.dot_general(lead_terms.reshape(atoms_here, planes * grid_lines), yz_spline[2], contract, precision=EXACT)
    charge = charge + lax.dot_general(tail_terms.reshape(atoms_here, planes * grid_lines), yz_spline[3], contract, precision=EXACT)
    return charge.reshape(planes, grid_lines, grid_lines)

def gather_field(potential, spline_value, spline_slope, yz_spline):
    planes = potential.shape[0]
    grid_lines = potential.shape[1]
    atoms_here = spline_value.shape[0]
    flat_grid = potential.reshape(planes * grid_lines, grid_lines)
    contract = (((1,), (1,)), ((), ()))
    plain_sum = lax.dot_general(yz_spline[2], flat_grid, contract, precision=EXACT).reshape(atoms_here, planes, grid_lines)
    tilted_sum = lax.dot_general(yz_spline[3], flat_grid, contract, precision=EXACT).reshape(atoms_here, planes, grid_lines)
    first_comp = lax.optimization_barrier(jnp.sum(spline_slope[:, :, None] * yz_spline[0][:, None, :] * plain_sum, axis=(1, 2)))
    second_comp = lax.optimization_barrier(jnp.sum(spline_value[:, :, None] * yz_spline[1][:, None, :] * plain_sum, axis=(1, 2)))
    third_comp = lax.optimization_barrier(jnp.sum(spline_value[:, :, None] * yz_spline[0][:, None, :] * tilted_sum, axis=(1, 2)))
    return jnp.stack([first_comp, second_comp, third_comp])

def reference_kernel():
    freq = jnp.arange(GRID, dtype=jnp.int32)
    signed = jnp.where(freq <= GRID // 2, freq, freq - GRID).astype(jnp.float32)
    last_freq = jnp.arange(GRID // 2 + 1, dtype=jnp.int32).astype(jnp.float32)
    mode_sq = signed[:, None, None] * signed[:, None, None] + signed[None, :, None] * signed[None, :, None] + last_freq[None, None, :] * last_freq[None, None, :]
    safe_sq = jnp.where(mode_sq > 0, mode_sq, 1.0)
    return jnp.where(mode_sq > 0, RECIP_C * jnp.exp(-DAMP * safe_sq) / safe_sq, 0.0)

def reference(positions, field, inv_polar, x_spline, yz_spline, tile_list, tile_count):
    slabs = N_GX
    planes = GRID // slabs
    extent = planes + 4
    halo_atoms = HALO_BLK * TILE
    slab_blocks = ATOM_DEV // TILE
    slab_ids = jnp.arange(slabs, dtype=jnp.int32)
    shift_x = jnp.concatenate([jnp.full((halo_atoms,), -1.0 * slab_blocks, jnp.float32), jnp.zeros((ATOM_DEV,), jnp.float32), jnp.full((halo_atoms,), 1.0 * slab_blocks, jnp.float32)])
    kernel = reference_kernel()
    place = slab_ids[:, None] * planes + jnp.arange(extent, dtype=jnp.int32)[None, :]
    local_plane = (jnp.arange(ATOM_DEV, dtype=jnp.int32) * planes // ATOM_DEV).astype(jnp.int32)

    def wrap_pad(array):
        return jnp.concatenate([array[:, -halo_atoms:], array, array[:, :halo_atoms]], axis=1)
    pos_pad = wrap_pad(positions)

    def slab_parts(slab):
        begin = slab * ATOM_DEV
        own_pos = lax.dynamic_slice_in_dim(positions, begin, ATOM_DEV, 1)
        ext_pos = lax.dynamic_slice_in_dim(pos_pad, begin, ATOM_DEV + 2 * halo_atoms, 1)
        ext_pos = ext_pos.at[0].add(shift_x)
        splines = lax.dynamic_slice_in_dim(x_spline, begin, ATOM_DEV, 2)
        dense = lax.dynamic_slice_in_dim(yz_spline, begin, ATOM_DEV, 1)
        tile_rows = lax.dynamic_slice_in_dim(tile_list, slab * slab_blocks, slab_blocks, 0)
        live_counts = lax.dynamic_slice_in_dim(tile_count, slab * slab_blocks, slab_blocks, 0)
        spline_value, spline_slope = slab_weights(local_plane, splines, extent)
        return (own_pos, ext_pos, spline_value, spline_slope, dense, tile_rows, live_counts)

    def apply(vector):
        vec_pad = wrap_pad(vector)

        def near_and_charge(slab):
            parts = slab_parts(slab)
            begin = slab * ATOM_DEV
            ext_vec = lax.dynamic_slice_in_dim(vec_pad, begin, ATOM_DEV + 2 * halo_atoms, 1)
            own_vec = lax.dynamic_slice_in_dim(vector, begin, ATOM_DEV, 1)
            near_field = pair_field(parts[0], parts[1], ext_vec, parts[5], parts[6])
            charge = spread_dipoles(own_vec, parts[2], parts[3], parts[4])
            return (near_field, charge)
        near_all, charges = lax.map(near_and_charge, slab_ids)
        padded = jnp.zeros((GRID + 4, GRID, GRID), jnp.float32).at[place].add(charges)
        whole = padded[2:GRID + 2]
        whole = whole.at[GRID - 2:].add(padded[:2]).at[:2].add(padded[GRID + 2:])
        potential = jnp.fft.irfftn(jnp.fft.rfftn(whole) * kernel, s=whole.shape)
        pot_pad = jnp.concatenate([potential[GRID - 2:], potential, potential[:2]], axis=0)

        def far_part(scan_item):
            slab, local_pot = scan_item
            parts = slab_parts(slab)
            return gather_field(local_pot, parts[2], parts[3], parts[4])
        far_all = lax.map(far_part, (slab_ids, pot_pad[place]))
        near_whole = near_all.transpose(1, 0, 2).reshape(3, ATOMS)
        far_whole = far_all.transpose(1, 0, 2).reshape(3, ATOMS)
        return inv_polar[None, :] * vector + far_whole - near_whole
    dipoles = jnp.zeros_like(field)
    residual = field
    precond = field / inv_polar[None, :]
    direction = precond
    rz_now = jnp.sum(residual * precond)
    for sweep_index in range(ITERS):
        applied = apply(direction)
        step_size = rz_now / jnp.sum(direction * applied)
        dipoles = dipoles + step_size * direction
        residual = residual - step_size * applied
        if sweep_index + 1 < ITERS:
            precond = residual / inv_polar[None, :]
            rz_next = jnp.sum(residual * precond)
            direction = precond + rz_next / rz_now * direction
            rz_now = rz_next
    return (dipoles, residual)
```

```python
import jax
import jax.numpy as jnp
from jax import lax
from jax.experimental import pallas as pl
from jax.experimental.pallas import tpu as pltpu
from jax.sharding import PartitionSpec as P

GRID = 128
ORDER = 5
TILE = 128
HALO_BLK = 3
ITERS = 3


PAIR_C = 0.025
RECIP_C = 8192.0
DAMP = 0.0008
EXACT = lax.Precision.HIGHEST


def extended(x, sides, width):
    for axis, dim in sides:
        devices, length = (lax.axis_size(axis), x.shape[dim])
        up = [(i, (i + 1) % devices) for i in range(devices)]
        down = [(j, i) for i, j in up]
        last = lax.slice_in_dim(x, length - width, length, axis=dim)
        first = lax.slice_in_dim(x, 0, width, axis=dim)
        before = lax.ppermute(last, axis, up)
        after = lax.ppermute(first, axis, down)
        x = jnp.concatenate([before, x, after], axis=dim)
    return x


def pair_field(home_pos, ext_pos, ext_vec, tile_rows, live_counts):
    slab_blocks = home_pos.shape[1] // TILE
    ext_blocks = ext_pos.shape[1] // TILE
    home_blocks = home_pos.reshape(3, slab_blocks, TILE).transpose(1, 0, 2)
    pos_blocks = ext_pos.reshape(3, ext_blocks, TILE)
    vec_blocks = ext_vec.reshape(3, ext_blocks, TILE)
    slot_index = jnp.arange(tile_rows.shape[1], dtype=jnp.int32)
    self_pair = jnp.eye(TILE, dtype=bool)

    def one_block(carried, scan_item):
        home_block, tile_row, live_count, block_index = scan_item
        near_pos = jnp.take(pos_blocks, tile_row, axis=1)
        near_vec = jnp.take(vec_blocks, tile_row, axis=1)
        offsets = home_block[:, None, :, None] - near_pos[:, :, None, :]
        distance_sq = jnp.sum(offsets * offsets, axis=0) + 1.0
        inverse = lax.rsqrt(distance_sq)
        third_power = inverse * inverse * inverse
        fifth_power = third_power * inverse * inverse
        same_block = (tile_row == block_index + HALO_BLK)[:, None, None]
        live_mask = (slot_index < live_count)[:, None, None] & ~(same_block & self_pair[None])
        third_power = jnp.where(live_mask, third_power, 0.0)
        fifth_power = jnp.where(live_mask, fifth_power, 0.0)
        projection = jnp.sum(offsets * near_vec[:, :, None, :], axis=0)
        field_sum = jnp.sum(
            third_power[None] * near_vec[:, :, None, :]
            - 3.0 * (fifth_power * projection)[None] * offsets,
            axis=(1, 3),
        )
        return (carried, PAIR_C * field_sum)

    block_ids = jnp.arange(slab_blocks, dtype=jnp.int32)
    unused_carry, blocks_out = lax.scan(
        one_block, jnp.zeros((), jnp.float32), (home_blocks, tile_rows, live_counts, block_ids)
    )
    return blocks_out.transpose(1, 0, 2).reshape(3, slab_blocks * TILE)


def slab_weights(local_plane, x_spline, planes):
    spline_steps = jnp.arange(ORDER, dtype=jnp.int32)
    plane_index = jnp.arange(planes, dtype=jnp.int32)
    matches = local_plane[None, :, None] + spline_steps[:, None, None] == plane_index[None, None, :]
    spline_value = jnp.sum(jnp.where(matches, x_spline[0][:, :, None], 0.0), axis=0)
    spline_slope = jnp.sum(jnp.where(matches, x_spline[1][:, :, None], 0.0), axis=0)
    return (spline_value, spline_slope)


def spread_dipoles(vector, spline_value, spline_slope, yz_spline):
    atoms_here = spline_value.shape[0]
    planes = spline_value.shape[1]
    grid_lines = yz_spline.shape[2]
    lead_terms = (vector[0][:, None] * spline_slope)[:, :, None] * yz_spline[0][:, None, :]
    lead_terms = (
        lead_terms + (vector[1][:, None] * spline_value)[:, :, None] * yz_spline[1][:, None, :]
    )
    tail_terms = (vector[2][:, None] * spline_value)[:, :, None] * yz_spline[0][:, None, :]
    contract = (((0,), (0,)), ((), ()))
    charge = lax.dot_general(
        lead_terms.reshape(atoms_here, planes * grid_lines), yz_spline[2], contract, precision=EXACT
    )
    charge = charge + lax.dot_general(
        tail_terms.reshape(atoms_here, planes * grid_lines), yz_spline[3], contract, precision=EXACT
    )
    return charge.reshape(planes, grid_lines, grid_lines)


def gather_field(potential, spline_value, spline_slope, yz_spline):
    planes = potential.shape[0]
    grid_lines = potential.shape[1]
    atoms_here = spline_value.shape[0]
    flat_grid = potential.reshape(planes * grid_lines, grid_lines)
    contract = (((1,), (1,)), ((), ()))
    plain_sum = lax.dot_general(yz_spline[2], flat_grid, contract, precision=EXACT).reshape(
        atoms_here, planes, grid_lines
    )
    tilted_sum = lax.dot_general(yz_spline[3], flat_grid, contract, precision=EXACT).reshape(
        atoms_here, planes, grid_lines
    )
    first_comp = jnp.sum(
        spline_slope[:, :, None] * yz_spline[0][:, None, :] * plain_sum, axis=(1, 2)
    )
    second_comp = jnp.sum(
        spline_value[:, :, None] * yz_spline[1][:, None, :] * plain_sum, axis=(1, 2)
    )
    third_comp = jnp.sum(
        spline_value[:, :, None] * yz_spline[0][:, None, :] * tilted_sum, axis=(1, 2)
    )
    return jnp.stack([first_comp, second_comp, third_comp])


def mode_of(freq, size):
    half_size = size // 2
    mode_num = jnp.where(freq <= half_size, freq, freq - half_size)
    weight = jnp.where((freq == 0) | (freq == half_size), 1.0 / size, 2.0 / size)
    return (mode_num.astype(jnp.float32), weight.astype(jnp.float32))


def basis_rows(size, points):
    freq = jnp.arange(size, dtype=jnp.int32)
    half_size = size // 2
    mode_num = jnp.where(freq <= half_size, freq, freq - half_size)
    phase = mode_num[:, None] * points[None, :] % size
    angle = phase.astype(jnp.float32) * (2.0 * jnp.pi / size)
    return jnp.where((freq <= half_size)[:, None], jnp.cos(angle), jnp.sin(angle))


def kernel_block(x_modes, x_weights, y_modes, y_weights, z_modes, z_weights):
    mode_sq = (
        x_modes[:, None, None] * x_modes[:, None, None]
        + y_modes[None, :, None] * y_modes[None, :, None]
        + z_modes[None, None, :] * z_modes[None, None, :]
    )
    safe_sq = jnp.where(mode_sq > 0, mode_sq, 1.0)
    green = jnp.where(mode_sq > 0, RECIP_C * jnp.exp(-DAMP * safe_sq) / safe_sq, 0.0)
    return green * x_weights[:, None, None] * y_weights[None, :, None] * z_weights[None, None, :]


def forward_lines(charge, fourier_rows):
    along_z = jnp.einsum("pyz,kz->pyk", charge, fourier_rows, precision=EXACT)
    return jnp.einsum("jy,pyk->pjk", fourier_rows, along_z, precision=EXACT)


def inverse_lines(spectrum, fourier_rows):
    along_z = jnp.einsum("pjk,kz->pjz", spectrum, fourier_rows, precision=EXACT)
    return jnp.einsum("jy,pjz->pyz", fourier_rows, along_z, precision=EXACT)


def per_device_general(positions, field, inv_polar, x_spline, yz_spline, tile_list, tile_count):
    rank_count = lax.axis_size("gx")
    rank_index = lax.axis_index("gx")
    atoms_here = positions.shape[1]
    planes = GRID // rank_count
    extent = planes + 4
    halo_atoms = HALO_BLK * TILE
    slab_blocks = atoms_here // TILE
    local_plane = jnp.arange(atoms_here, dtype=jnp.int32) * planes // atoms_here
    spline_value, spline_slope = slab_weights(local_plane, x_spline, extent)
    ext_pos = extended(positions, (("gx", 1),), halo_atoms)
    shift_x = jnp.concatenate(
        [
            jnp.full((halo_atoms,), -1.0 * slab_blocks, jnp.float32),
            jnp.zeros((atoms_here,), jnp.float32),
            jnp.full((halo_atoms,), 1.0 * slab_blocks, jnp.float32),
        ]
    )
    ext_pos = ext_pos.at[0].add(shift_x)
    fourier_rows = basis_rows(GRID, jnp.arange(GRID, dtype=jnp.int32))
    ky_count = GRID // rank_count
    all_freq = jnp.arange(GRID, dtype=jnp.int32)
    ky_freq = rank_index * ky_count + jnp.arange(ky_count, dtype=jnp.int32)
    full_modes, full_weights = mode_of(all_freq, GRID)
    ky_modes, ky_weights = mode_of(ky_freq, GRID)
    kernel = kernel_block(full_modes, full_weights, ky_modes, ky_weights, full_modes, full_weights)
    kernel = kernel.reshape(GRID, ky_count * GRID)
    source_rows = jnp.arange(rank_count * extent, dtype=jnp.int32)
    points = (source_rows // extent * planes - 2 + source_rows % extent) % GRID
    across = basis_rows(GRID, points)

    def reciprocal(charge):
        spectrum = forward_lines(charge, fourier_rows)
        pencils = lax.all_to_all(spectrum, "gx", split_axis=1, concat_axis=0, tiled=True)
        rows_in = pencils.shape[0]
        flat_pencils = pencils.reshape(rows_in, ky_count * GRID)
        spectral_lines = jnp.dot(across, flat_pencils, precision=EXACT) * kernel
        returned_lines = lax.dot_general(
            across, spectral_lines, (((0,), (0,)), ((), ())), precision=EXACT
        )
        returned = lax.all_to_all(
            returned_lines.reshape(rows_in, ky_count, GRID),
            "gx",
            split_axis=0,
            concat_axis=1,
            tiled=True,
        )
        return inverse_lines(returned, fourier_rows)

    def apply(vector):
        ext_vec = extended(vector, (("gx", 1),), halo_atoms)
        near_field = pair_field(positions, ext_pos, ext_vec, tile_list, tile_count)
        charge = spread_dipoles(vector, spline_value, spline_slope, yz_spline)
        far_field = gather_field(reciprocal(charge), spline_value, spline_slope, yz_spline)
        return inv_polar[None, :] * vector + far_field - near_field

    def paired(residual, precond, applied):
        return lax.psum((jnp.sum(residual * precond), jnp.sum(applied * precond)), "gx")

    dipoles = jnp.zeros_like(field)
    residual = field
    precond = field / inv_polar[None, :]
    applied = apply(precond)
    rz_now, curvature = paired(residual, precond, applied)
    step_size = rz_now / curvature
    direction = precond
    applied_dir = applied
    for sweep_index in range(ITERS):
        dipoles = dipoles + step_size * direction
        residual = residual - step_size * applied_dir
        if sweep_index + 1 < ITERS:
            precond = residual / inv_polar[None, :]
            applied = apply(precond)
            rz_next, curvature = paired(residual, precond, applied)
            beta_ratio = rz_next / rz_now
            step_size = rz_next / (curvature - beta_ratio * rz_next / step_size)
            direction = precond + beta_ratio * direction
            applied_dir = applied + beta_ratio * applied_dir
            rz_now = rz_next
    return (dipoles, residual)


F32 = jnp.float32
BF16 = jnp.bfloat16
ROWS = 8
REACH = 2
SPAN = 2 * HALO_BLK + 1
IN_VMEM = pl.BlockSpec(memory_space=pltpu.VMEM)
IN_SMEM = pl.BlockSpec(memory_space=pltpu.SMEM)


def halves(x):
    high = x.astype(BF16)
    low = (x - high.astype(F32)).astype(BF16)
    return high, low


def bdot(a, b):
    return jnp.dot(a, b, preferred_element_type=F32)


def params(flops):
    return dict(
        cost_estimate=pl.CostEstimate(flops=flops, bytes_accessed=4 << 20, transcendentals=0),
    )


def prep_kernel(own_ref, halo_ref, rows_ref, yt_ref, dyt_ref, zst_ref, zt_ref):
    group = pl.program_id(0)
    edge = (group < REACH) | (group >= pl.num_programs(0) - REACH)
    rows = rows_ref[...]

    def fill(tables):
        group_atoms = tables.shape[1]
        nt = (((1,), (1,)), ((), ()))
        yt_ref[...] = lax.dot_general(rows, tables[0], nt, precision=EXACT)
        dyt_ref[...] = lax.dot_general(rows, tables[1], nt, precision=EXACT)
        for half in range(2):
            table = tables[2 + half]
            across = lax.dot_general(table, rows, nt, precision=EXACT)
            high, low = halves(across)
            zst_ref[pl.ds(half * group_atoms, group_atoms), :] = jnp.concatenate([high, low], axis=1)
            turned = lax.dot_general(rows, table, nt, precision=EXACT)
            high, low = halves(turned)
            zt_ref[:, pl.ds(half * group_atoms, group_atoms)] = jnp.concatenate(
                [high, low, high, low], axis=0
            )

    @pl.when(edge)
    def _():
        fill(halo_ref)

    @pl.when(jnp.logical_not(edge))
    def _():
        fill(own_ref)


def prepare(yz_own, yz_halo, rows, groups, group_atoms):
    grid = rows.shape[0]
    planes = groups - 2 * REACH
    block = (4, group_atoms, grid)
    return pl.pallas_call(
        prep_kernel,
        grid=(groups,),
        in_specs=[
            pl.BlockSpec(block, lambda e: (0, jnp.clip(e - REACH, 0, planes - 1), 0)),
            pl.BlockSpec(
                block,
                lambda e: (0, jnp.where(e < REACH, e, jnp.maximum(e - planes, REACH - 1)), 0),
            ),
            pl.BlockSpec((grid, grid), lambda e: (0, 0)),
        ],
        out_specs=[
            pl.BlockSpec((grid, group_atoms), lambda e: (0, e)),
            pl.BlockSpec((grid, group_atoms), lambda e: (0, e)),
            pl.BlockSpec((2 * group_atoms, 2 * grid), lambda e: (e, 0)),
            pl.BlockSpec((4 * grid, 2 * group_atoms), lambda e: (0, e)),
        ],
        out_shape=[
            jax.ShapeDtypeStruct((grid, groups * group_atoms), F32),
            jax.ShapeDtypeStruct((grid, groups * group_atoms), F32),
            jax.ShapeDtypeStruct((2 * groups * group_atoms, 2 * grid), BF16),
            jax.ShapeDtypeStruct((4 * grid, 2 * groups * group_atoms), BF16),
        ],
        name="prep",
        **params(1 << 30),
    )(yz_own, yz_halo, rows)


def spread_kernel(halo, h_ref, sl_ref, sr_ref, rl_ref, rr_ref, ip_ref, xw_ref, yt_ref, dyt_ref, zst_ref, v_ref, out_ref):
    parts, planes, ky_count, grid = out_ref.shape
    groups = planes + 2 * REACH
    ga = yt_ref.shape[1] // groups
    edge = REACH * ga
    atoms = h_ref.shape[1]
    ext = atoms + 2 * halo
    v_ref[:, :halo] = rl_ref[:, :halo]
    v_ref[:, halo - edge : halo] += sl_ref[:, halo:]
    v_ref[:, halo : halo + atoms] = h_ref[...]
    v_ref[:, halo : halo + edge] += rl_ref[:, halo:]
    v_ref[:, halo + atoms - edge : halo + atoms] += rr_ref[:, halo:]
    v_ref[:, halo + atoms :] = rr_ref[:, :halo]
    v_ref[:, halo + atoms : halo + atoms + edge] += sr_ref[:, halo:]
    v_ref[...] = v_ref[...] / ip_ref[...]
    base = halo - edge
    for p in range(planes):
        high_parts, low_parts = [], []
        for e in range(p, p + ORDER):
            k = p - e + ORDER - 1
            here = slice(e * ga, (e + 1) * ga)
            there = slice(base + e * ga, base + (e + 1) * ga)
            a0 = v_ref[0:1, there] * xw_ref[ORDER + k : ORDER + k + 1, here]
            a1 = v_ref[1:2, there] * xw_ref[k : k + 1, here]
            a2 = v_ref[2:3, there] * xw_ref[k : k + 1, here]
            yt = yt_ref[:, here]
            lead = a0 * yt + a1 * dyt_ref[:, here]
            tail = a2 * yt
            for part in (lead, tail):
                high, low = halves(part)
                high_parts.append(high)
                low_parts.append(low)
        table = zst_ref[p * 2 * ga : (p + ORDER) * 2 * ga, :]
        both = bdot(jnp.concatenate(high_parts, axis=1), table)
        both = both + bdot(jnp.concatenate(low_parts, axis=1), table)
        charge = both[:, :grid] + both[:, grid:]
        out_ref[:, p] = charge.reshape(parts, ky_count, grid)


def spread_call(halo, parts, planes, h, sends, recvs, ip, xw, tables):
    yt, dyt, zst, zt = tables
    grid = yt.shape[0]
    return pl.pallas_call(
        lambda *refs: spread_kernel(halo, *refs),
        in_specs=[IN_VMEM] * 10,
        out_specs=[IN_VMEM, IN_VMEM],
        out_shape=[
            jax.ShapeDtypeStruct(ip.shape, F32),
            jax.ShapeDtypeStruct((parts, planes, grid // parts, grid), F32),
        ],
        name="spread",
        **params(1 << 30),
    )(h, sends[0], sends[1], recvs[0], recvs[1], ip, xw, yt, dyt, zst)


def gather_kernel(halo, planes, ret_ref, yt_ref, dyt_ref, zt_ref, xw_ref, pair_ref, h_ref, sl_ref, sr_ref, lhs_ref):
    grid = yt_ref.shape[0]
    groups = planes + 2 * REACH
    ga = yt_ref.shape[1] // groups
    edge = REACH * ga
    atoms = h_ref.shape[1]
    for p in range(planes):
        high, low = halves(ret_ref[:, p].reshape(grid, grid))
        lhs_ref[p * grid : (p + 1) * grid, :] = jnp.concatenate([high, high, low, low], axis=1)
    blank = jnp.zeros((ROWS - 3, ga), F32)
    for e in range(groups):
        first, last = max(0, e - ORDER + 1), min(planes - 1, e)
        here = slice(e * ga, (e + 1) * ga)
        field = bdot(
            lhs_ref[first * grid : (last + 1) * grid, :], zt_ref[:, e * 2 * ga : (e + 1) * 2 * ga]
        )
        yt, dyt = yt_ref[:, here], dyt_ref[:, here]
        c0 = c1 = c2 = jnp.zeros((1, ga), F32)
        for p in range(first, last + 1):
            k = p - e + ORDER - 1
            rows = slice((p - first) * grid, (p - first + 1) * grid)
            plain, tilted = field[rows, :ga], field[rows, ga:]
            slope, value = xw_ref[ORDER + k : ORDER + k + 1, here], xw_ref[k : k + 1, here]
            c0 = c0 + slope * jnp.sum(yt * plain, axis=0, keepdims=True)
            c1 = c1 + value * jnp.sum(dyt * plain, axis=0, keepdims=True)
            c2 = c2 + value * jnp.sum(yt * tilted, axis=0, keepdims=True)
        far = jnp.concatenate([c0, c1, c2, blank], axis=0)
        if e < REACH:
            sl_ref[:, halo + e * ga : halo + (e + 1) * ga] = far
        elif e >= groups - REACH:
            at = halo + (e - groups + REACH) * ga
            sr_ref[:, at : at + ga] = far
        else:
            at = slice((e - REACH) * ga, (e - REACH + 1) * ga)
            h_ref[:, at] = far - pair_ref[:, at]
    sl_ref[:, :halo] = h_ref[:, :halo]
    sr_ref[:, :halo] = h_ref[:, atoms - halo :]


def gather_call(halo, planes, returned, xw, pair, tables):
    yt, dyt, zst, zt = tables
    grid = yt.shape[0]
    edge = REACH * (yt.shape[1] // (planes + 2 * REACH))
    return pl.pallas_call(
        lambda *refs: gather_kernel(halo, planes, *refs),
        in_specs=[IN_VMEM] * 6,
        out_specs=[IN_VMEM] * 3,
        out_shape=[
            jax.ShapeDtypeStruct(pair.shape, F32),
            jax.ShapeDtypeStruct((ROWS, halo + edge), F32),
            jax.ShapeDtypeStruct((ROWS, halo + edge), F32),
        ],
        scratch_shapes=[pltpu.VMEM((planes * grid, 4 * grid), BF16)],
        name="gather",
        **params(1 << 30),
    )(returned, yt, dyt, zt, xw, pair)


def across_kernel(with_sums, pen_ref, rows_ref, cols_ref, kern_ref, *rest):
    if with_sums:
        sums_ref, out_ref = rest
    else:
        (out_ref,) = rest
    grid = rows_ref.shape[0]
    parts, blocks, ky_count, _ = out_ref.shape
    planes = grid // parts
    highs, lows = [], []
    for j in range(ky_count):
        high, low = halves(pen_ref[pl.ds(j, grid, stride=ky_count), :])
        highs.append(high)
        lows.append(low)

    def product(matrix, highs, lows):
        mh, ml = halves(matrix)
        rhs = jnp.concatenate(
            [jnp.concatenate(highs, axis=1), jnp.concatenate(lows, axis=1)], axis=0
        )
        return bdot(jnp.concatenate([mh, mh], axis=1), rhs) + bdot(
            jnp.concatenate([ml, ml], axis=1), rhs
        )

    spectrum = product(rows_ref[...], highs, lows)
    weighted = spectrum * kern_ref[...]
    high, low = halves(weighted)
    lines = product(cols_ref[...], [high], [low])
    for j in range(ky_count):
        line = lines[:, j * grid : (j + 1) * grid].reshape(parts, planes, grid)
        out_ref[:, 0:planes, j, :] = line
    if with_sums:
        energy = jnp.sum(spectrum * weighted)
        row = lax.broadcasted_iota(jnp.int32, sums_ref.shape, 0)
        sums = sums_ref[...] + jnp.where(row == 5, energy, 0.0)
        for d in range(parts):
            out_ref[d, planes] = sums


def across_call(pencils, rows, cols, kern, parts, sums=None):
    grid = rows.shape[0]
    planes = grid // parts
    ky_count = kern.shape[1] // grid
    args = [pencils.reshape(grid * ky_count, grid), rows, cols, kern]
    if sums is not None:
        args.append(sums)
    blocks = planes + (sums is not None)
    return pl.pallas_call(
        lambda *refs: across_kernel(sums is not None, *refs),
        in_specs=[IN_VMEM] * len(args),
        out_specs=IN_VMEM,
        out_shape=jax.ShapeDtypeStruct((parts, blocks, ky_count, grid), F32),
        name="across",
        **params(1 << 28),
    )(*args)


def pair_kernel(wts_ref, pos_ref, col_ref, vec_ref, out_ref, acc_ref):
    blocks = out_ref.shape[1] // TILE
    chunk = 32
    out_ref[...] = jnp.zeros(out_ref.shape, F32)

    def one_block(b, carry):
        for c in range(TILE // chunk):
            home = col_ref[pl.ds(pl.multiple_of(b * TILE + c * chunk, chunk), chunk), :]
            shape = (chunk, TILE)
            hx = jnp.broadcast_to(home[:, 0:1], shape)
            hy = jnp.broadcast_to(home[:, 1:2], shape)
            hz = jnp.broadcast_to(home[:, 2:3], shape)
            sx = sy = sz = jnp.zeros(shape, F32)
            for e in range(SPAN):
                near = pl.ds(pl.multiple_of((b + e) * TILE, TILE), TILE)
                dx = hx - pos_ref[0:1, near]
                dy = hy - pos_ref[1:2, near]
                dz = hz - pos_ref[2:3, near]
                vx, vy, vz = vec_ref[0:1, near], vec_ref[1:2, near], vec_ref[2:3, near]
                inverse = lax.rsqrt(dx * dx + dy * dy + dz * dz + 1.0)
                square = inverse * inverse
                third = wts_ref[b * SPAN + e] * (inverse * square)
                if e == HALO_BLK:
                    row = lax.broadcasted_iota(jnp.int32, shape, 0) + c * chunk
                    lane = lax.broadcasted_iota(jnp.int32, shape, 1)
                    third = jnp.where(row == lane, 0.0, third)
                fifth = 3.0 * (third * square) * (dx * vx + dy * vy + dz * vz)
                sx = sx + (third * vx - fifth * dx)
                sy = sy + (third * vy - fifth * dy)
                sz = sz + (third * vz - fifth * dz)
            acc_ref[0, pl.ds(c * chunk, chunk), :] = sx
            acc_ref[1, pl.ds(c * chunk, chunk), :] = sy
            acc_ref[2, pl.ds(c * chunk, chunk), :] = sz
        home_lanes = pl.ds(pl.multiple_of(b * TILE, TILE), TILE)
        for i in range(3):
            out_ref[i : i + 1, home_lanes] = PAIR_C * jnp.sum(acc_ref[i].T, axis=0, keepdims=True)
        return carry

    lax.fori_loop(0, blocks, one_block, 0)


def pair_call(wts, pos, cols, vec, atoms):
    return pl.pallas_call(
        pair_kernel,
        in_specs=[IN_SMEM, IN_VMEM, IN_VMEM, IN_VMEM],
        out_specs=IN_VMEM,
        out_shape=jax.ShapeDtypeStruct((ROWS, atoms), F32),
        scratch_shapes=[pltpu.VMEM((3, TILE, TILE), F32)],
        name="pair",
        **params(1 << 30),
    )(wts, pos, cols, vec)


def moments_kernel(halo, v0_ref, v1_ref, v2_ref, ip_ref, pair_ref, out_ref):
    atoms = pair_ref.shape[1]
    own = slice(halo, halo + atoms)
    v0, v1, v2, ip = v0_ref[:, own], v1_ref[:, own], v2_ref[:, own], ip_ref[:, own]
    d1, d2 = ip * v1, ip * v2
    terms = (v0 * (ip * v0), v0 * d1, v1 * d1, v1 * d2, v2 * d2, -(v2 * pair_ref[...]))
    row = lax.broadcasted_iota(jnp.int32, out_ref.shape, 0)
    sums = jnp.zeros(out_ref.shape, F32)
    for k, term in enumerate(terms):
        sums = sums + jnp.where(row == k, jnp.sum(term), 0.0)
    out_ref[...] = sums


def moments_call(halo, vectors, ip, pair):
    return pl.pallas_call(
        lambda *refs: moments_kernel(halo, *refs),
        in_specs=[IN_VMEM] * 5,
        out_specs=IN_VMEM,
        out_shape=jax.ShapeDtypeStruct((ROWS, 128), F32),
        name="moments",
        **params(1 << 24),
    )(*vectors, ip, pair)


def finish_kernel(halo, sums_ref, v0_ref, v1_ref, v2_ref, ip_ref, h_ref, rl_ref, rr_ref, dip_ref, res_ref):
    atoms = h_ref.shape[1]
    own = slice(halo, halo + atoms)
    edge = rl_ref.shape[1] - halo
    total = jnp.sum(sums_ref[:, 0], axis=0)
    m = [total[k : k + 1, 0:1] for k in range(6)]
    s = [lax.rsqrt(m[2 * i]) for i in range(3)]
    g = [[m[i + j] * s[i] * s[j] for j in range(3)] for i in range(3)]
    b = [-m[i + 3] * s[i] for i in range(3)]
    l10 = g[1][0] / g[0][0]
    l20 = g[2][0] / g[0][0]
    p11 = g[1][1] - l10 * g[0][1]
    p12 = g[1][2] - l10 * g[0][2]
    l21 = p12 / p11
    p22 = g[2][2] - l20 * g[0][2] - l21 * p12
    b1 = b[1] - l10 * b[0]
    b2 = b[2] - l20 * b[0] - l21 * b1
    y2 = b2 / p22
    y1 = (b1 - p12 * y2) / p11
    y0 = (b[0] - g[0][1] * y1 - g[0][2] * y2) / g[0][0]
    a0, a1, a2 = s[0] * y0, s[1] * y1, s[2] * y2
    scale = 1.0 / (a0 - a1 + a2 - 1.0)
    a0, a1, a2, a3 = a0 * scale, a1 * scale, a2 * scale, scale
    c2 = -a3
    c1 = a3 - a2
    c0 = a2 - a3 - a1
    v0, v1, v2, ip = v0_ref[:, own], v1_ref[:, own], v2_ref[:, own], ip_ref[:, own]
    dip_ref[...] = (c0 * v0 + c1 * v1 + c2 * v2)[0:3]
    res_ref[...] = (ip * (a0 * v0 + a1 * v1 + a2 * v2) + a3 * h_ref[...])[0:3]
    res_ref[:, :edge] += (a3 * rl_ref[:, halo:])[0:3]
    res_ref[:, atoms - edge :] += (a3 * rr_ref[:, halo:])[0:3]


def finish_call(halo, returned, vectors, ip, h, recvs):
    parts, blocks, ky_count, grid = returned.shape
    atoms = h.shape[1]
    whole = lambda x: pl.BlockSpec(x.shape, lambda i: (0,) * x.ndim)
    others = list(vectors) + [ip, h, recvs[0], recvs[1]]
    return pl.pallas_call(
        lambda *refs: finish_kernel(halo, *refs),
        grid=(1,),
        in_specs=[pl.BlockSpec((parts, 1, ky_count, grid), lambda i: (0, blocks - 1, 0, 0))]
        + [whole(x) for x in others],
        out_specs=[pl.BlockSpec((3, atoms), lambda i: (0, 0))] * 2,
        out_shape=[jax.ShapeDtypeStruct((3, atoms), F32)] * 2,
        name="finish",
        **params(1 << 24),
    )(returned, *others)


def compact_rows(yz):
    values = []
    lanes = lax.broadcasted_iota(jnp.int32, yz.shape[1:], 1)
    for first in (0, 2):
        used = (yz[first] != 0) | (yz[first + 1] != 0)
        starts = used & ~jnp.roll(used, 1, axis=1)
        values.append(jnp.sum(jnp.where(starts, lanes, 0), axis=1).astype(F32))
        for k in range(ORDER):
            here = jnp.roll(starts, k, axis=1)
            values.append(jnp.sum(jnp.where(here, yz[first], 0.0), axis=1))
            values.append(jnp.sum(jnp.where(here, yz[first + 1], 0.0), axis=1))
    return jnp.stack(values)


def dense_rows(packed, grid):
    count = packed.shape[1]
    lanes = lax.broadcasted_iota(jnp.int32, (count, grid), 1)
    tables = []
    stride = 1 + 2 * ORDER
    for axis in range(2):
        start = packed[axis * stride].astype(jnp.int32)[:, None]
        offset = (lanes - start) % grid
        for kind in range(2):
            table = jnp.zeros((count, grid), F32)
            for k in range(ORDER):
                value = packed[axis * stride + 1 + 2 * k + kind][:, None]
                table = jnp.where(offset == k, value, table)
            tables.append(table)
    return jnp.stack(tables)


def pad_rows(x):
    return jnp.pad(x, ((0, ROWS - x.shape[0]), (0, 0)))


def per_device_slab(positions, field, inv_polar, x_spline, yz_spline, tile_list, tile_count):
    parts = lax.axis_size("gx")
    rank = lax.axis_index("gx")
    atoms = positions.shape[1]
    planes = GRID // parts
    group_atoms = atoms // planes
    groups = planes + 2 * REACH
    edge = REACH * group_atoms
    halo = HALO_BLK * TILE
    slab_blocks = atoms // TILE
    up = [(i, (i + 1) % parts) for i in range(parts)]
    down = [(j, i) for i, j in up]
    inv_row = inv_polar[None, :]
    xs = x_spline.reshape(2 * ORDER, atoms)

    pieces = (positions, field, inv_row)

    def pack(side):
        outer = slice(0, halo) if side == 0 else slice(atoms - halo, atoms)
        inner = slice(0, edge) if side == 0 else slice(atoms - edge, atoms)
        parts_flat = [x[:, outer].reshape(-1) for x in pieces]
        parts_flat.append(xs[:, inner].reshape(-1))
        parts_flat.append(compact_rows(yz_spline[:, inner]).reshape(-1))
        flat = jnp.concatenate(parts_flat)
        return flat.reshape(-1, TILE)

    def unpack(block):
        flat = block.reshape(-1)
        out, at = [], 0
        for rows, width in ((3, halo), (3, halo), (1, halo), (2 * ORDER, edge), (22, edge)):
            out.append(flat[at : at + rows * width].reshape(rows, width))
            at += rows * width
        return out

    from_left = unpack(lax.ppermute(pack(1), "gx", up))
    from_right = unpack(lax.ppermute(pack(0), "gx", down))
    shift = jnp.zeros((3, 1), F32).at[0].set(1.0 * slab_blocks)
    ext_pos = jnp.concatenate([from_left[0] - shift, positions, from_right[0] + shift], axis=1)
    ext_pos = pad_rows(ext_pos)
    ip = jnp.concatenate([from_left[2], inv_row, from_right[2]], axis=1)
    ip = jnp.broadcast_to(ip, (ROWS, ip.shape[1]))
    xw = jnp.concatenate([from_left[3], xs, from_right[3]], axis=1)
    xw = jnp.pad(xw, ((0, 16 - 2 * ORDER), (0, 0)))
    yz_halo = dense_rows(jnp.concatenate([from_left[4], from_right[4]], axis=1), GRID)
    none = jnp.zeros((ROWS, edge), F32)
    recvs = [jnp.concatenate([pad_rows(x[1]), none], axis=1) for x in (from_left, from_right)]
    sends = [jnp.zeros((ROWS, halo + edge), F32)] * 2
    home_cols = pad_rows(positions).T

    offsets = jnp.arange(SPAN, dtype=jnp.int32)
    block_ids = jnp.arange(slab_blocks, dtype=jnp.int32)
    live = jnp.arange(tile_list.shape[1], dtype=jnp.int32)[None, :] < tile_count[:, None]
    hit = tile_list[:, :, None] == block_ids[:, None, None] + offsets[None, None, :]
    wts = jnp.sum((hit & live[:, :, None]).astype(F32), axis=1).reshape(-1)

    all_freq = jnp.arange(GRID, dtype=jnp.int32)
    fourier_rows = basis_rows(GRID, all_freq)
    ky_count = GRID // parts
    ky_freq = rank * ky_count + jnp.arange(ky_count, dtype=jnp.int32)
    full_modes, full_weights = mode_of(all_freq, GRID)
    ky_modes, ky_weights = mode_of(ky_freq, GRID)
    kern = kernel_block(full_modes, full_weights, ky_modes, ky_weights, full_modes, full_weights)
    kern = kern.reshape(GRID, ky_count * GRID)
    fourier_cols = fourier_rows.T

    tables = prepare(yz_spline, yz_halo, fourier_rows, groups, group_atoms)

    h = pad_rows(field)
    vectors = []
    for step in range(ITERS):
        vec, spectrum = spread_call(halo, parts, planes, h, sends, recvs, ip, xw, tables)
        vectors.append(vec)
        pencils = lax.all_to_all(spectrum, "gx", split_axis=0, concat_axis=0, tiled=True)
        pair = pair_call(wts, ext_pos, home_cols, vec, atoms)
        sums = moments_call(halo, vectors, ip, pair) if step + 1 == ITERS else None
        lines = across_call(pencils, fourier_rows, fourier_cols, kern, parts, sums)
        returned = lax.all_to_all(lines, "gx", split_axis=0, concat_axis=0, tiled=True)
        h, send_left, send_right = gather_call(halo, planes, returned, xw, pair, tables)
        sends = [send_left, send_right]
        recvs = [lax.ppermute(send_right, "gx", up), lax.ppermute(send_left, "gx", down)]
    dipoles, residual = finish_call(halo, returned, vectors, ip, h, recvs)
    return (dipoles, residual)


def per_device(positions, *others):
    parts = lax.axis_size("gx")
    atoms = positions.shape[1]
    planes = GRID // parts
    slab = (
        GRID % parts == 0
        and planes % ROWS == 0
        and parts * ROWS == GRID
        and atoms % planes == 0
        and (atoms // planes) % TILE == 0
        and REACH * (atoms // planes) <= HALO_BLK * TILE
        and atoms >= 2 * HALO_BLK * TILE
        and ITERS == 3
    )
    run = per_device_slab if slab else per_device_general
    return run(positions, *others)


def solution(mesh):
    placed = (
        P(None, ("rep", "gx")),
        P(None, ("rep", "gx")),
        P(("rep", "gx")),
        P(None, None, ("rep", "gx")),
        P(None, ("rep", "gx"), None),
        P(("rep", "gx"), None),
        P(("rep", "gx")),
    )
    return jax.shard_map(
        per_device,
        mesh=mesh,
        in_specs=placed,
        out_specs=(P(None, ("rep", "gx")), P(None, ("rep", "gx"))),
        check_vma=False,
    )
```

```python
import jax
import numpy as np
import jax.numpy as jnp
from jax import lax
from jax.experimental import pallas as pl
from jax.experimental.pallas import tpu as pltpu
from jax.sharding import PartitionSpec as P

GRID = 128
ORDER = 5
TILE = 128
HALO_BLK = 3
ITERS = 3


PAIR_C = 0.025
RECIP_C = 8192.0
DAMP = 0.0008
EXACT = lax.Precision.HIGHEST


def extended(x, sides, width):
    for axis, dim in sides:
        devices, length = (lax.axis_size(axis), x.shape[dim])
        up = [(i, (i + 1) % devices) for i in range(devices)]
        down = [(j, i) for i, j in up]
        last = lax.slice_in_dim(x, length - width, length, axis=dim)
        first = lax.slice_in_dim(x, 0, width, axis=dim)
        before = lax.ppermute(last, axis, up)
        after = lax.ppermute(first, axis, down)
        x = jnp.concatenate([before, x, after], axis=dim)
    return x


def pair_field(home_pos, ext_pos, ext_vec, tile_rows, live_counts):
    slab_blocks = home_pos.shape[1] // TILE
    ext_blocks = ext_pos.shape[1] // TILE
    home_blocks = home_pos.reshape(3, slab_blocks, TILE).transpose(1, 0, 2)
    pos_blocks = ext_pos.reshape(3, ext_blocks, TILE)
    vec_blocks = ext_vec.reshape(3, ext_blocks, TILE)
    slot_index = jnp.arange(tile_rows.shape[1], dtype=jnp.int32)
    self_pair = jnp.eye(TILE, dtype=bool)

    def one_block(carried, scan_item):
        home_block, tile_row, live_count, block_index = scan_item
        near_pos = jnp.take(pos_blocks, tile_row, axis=1)
        near_vec = jnp.take(vec_blocks, tile_row, axis=1)
        offsets = home_block[:, None, :, None] - near_pos[:, :, None, :]
        distance_sq = jnp.sum(offsets * offsets, axis=0) + 1.0
        inverse = lax.rsqrt(distance_sq)
        third_power = inverse * inverse * inverse
        fifth_power = third_power * inverse * inverse
        same_block = (tile_row == block_index + HALO_BLK)[:, None, None]
        live_mask = (slot_index < live_count)[:, None, None] & ~(same_block & self_pair[None])
        third_power = jnp.where(live_mask, third_power, 0.0)
        fifth_power = jnp.where(live_mask, fifth_power, 0.0)
        projection = jnp.sum(offsets * near_vec[:, :, None, :], axis=0)
        field_sum = jnp.sum(
            third_power[None] * near_vec[:, :, None, :]
            - 3.0 * (fifth_power * projection)[None] * offsets,
            axis=(1, 3),
        )
        return (carried, PAIR_C * field_sum)

    block_ids = jnp.arange(slab_blocks, dtype=jnp.int32)
    unused_carry, blocks_out = lax.scan(
        one_block, jnp.zeros((), jnp.float32), (home_blocks, tile_rows, live_counts, block_ids)
    )
    return blocks_out.transpose(1, 0, 2).reshape(3, slab_blocks * TILE)


def slab_weights(local_plane, x_spline, planes):
    spline_steps = jnp.arange(ORDER, dtype=jnp.int32)
    plane_index = jnp.arange(planes, dtype=jnp.int32)
    matches = local_plane[None, :, None] + spline_steps[:, None, None] == plane_index[None, None, :]
    spline_value = jnp.sum(jnp.where(matches, x_spline[0][:, :, None], 0.0), axis=0)
    spline_slope = jnp.sum(jnp.where(matches, x_spline[1][:, :, None], 0.0), axis=0)
    return (spline_value, spline_slope)


def spread_dipoles(vector, spline_value, spline_slope, yz_spline):
    atoms_here = spline_value.shape[0]
    planes = spline_value.shape[1]
    grid_lines = yz_spline.shape[2]
    lead_terms = (vector[0][:, None] * spline_slope)[:, :, None] * yz_spline[0][:, None, :]
    lead_terms = (
        lead_terms + (vector[1][:, None] * spline_value)[:, :, None] * yz_spline[1][:, None, :]
    )
    tail_terms = (vector[2][:, None] * spline_value)[:, :, None] * yz_spline[0][:, None, :]
    contract = (((0,), (0,)), ((), ()))
    charge = lax.dot_general(
        lead_terms.reshape(atoms_here, planes * grid_lines), yz_spline[2], contract, precision=EXACT
    )
    charge = charge + lax.dot_general(
        tail_terms.reshape(atoms_here, planes * grid_lines), yz_spline[3], contract, precision=EXACT
    )
    return charge.reshape(planes, grid_lines, grid_lines)


def gather_field(potential, spline_value, spline_slope, yz_spline):
    planes = potential.shape[0]
    grid_lines = potential.shape[1]
    atoms_here = spline_value.shape[0]
    flat_grid = potential.reshape(planes * grid_lines, grid_lines)
    contract = (((1,), (1,)), ((), ()))
    plain_sum = lax.dot_general(yz_spline[2], flat_grid, contract, precision=EXACT).reshape(
        atoms_here, planes, grid_lines
    )
    tilted_sum = lax.dot_general(yz_spline[3], flat_grid, contract, precision=EXACT).reshape(
        atoms_here, planes, grid_lines
    )
    first_comp = jnp.sum(
        spline_slope[:, :, None] * yz_spline[0][:, None, :] * plain_sum, axis=(1, 2)
    )
    second_comp = jnp.sum(
        spline_value[:, :, None] * yz_spline[1][:, None, :] * plain_sum, axis=(1, 2)
    )
    third_comp = jnp.sum(
        spline_value[:, :, None] * yz_spline[0][:, None, :] * tilted_sum, axis=(1, 2)
    )
    return jnp.stack([first_comp, second_comp, third_comp])


def mode_of(freq, size):
    half_size = size // 2
    mode_num = jnp.where(freq <= half_size, freq, freq - half_size)
    weight = jnp.where((freq == 0) | (freq == half_size), 1.0 / size, 2.0 / size)
    return (mode_num.astype(jnp.float32), weight.astype(jnp.float32))


def basis_rows(size, points):
    freq = jnp.arange(size, dtype=jnp.int32)
    half_size = size // 2
    mode_num = jnp.where(freq <= half_size, freq, freq - half_size)
    phase = mode_num[:, None] * points[None, :] % size
    angle = phase.astype(jnp.float32) * (2.0 * jnp.pi / size)
    return jnp.where((freq <= half_size)[:, None], jnp.cos(angle), jnp.sin(angle))


def kernel_block(x_modes, x_weights, y_modes, y_weights, z_modes, z_weights):
    mode_sq = (
        x_modes[:, None, None] * x_modes[:, None, None]
        + y_modes[None, :, None] * y_modes[None, :, None]
        + z_modes[None, None, :] * z_modes[None, None, :]
    )
    safe_sq = jnp.where(mode_sq > 0, mode_sq, 1.0)
    green = jnp.where(mode_sq > 0, RECIP_C * jnp.exp(-DAMP * safe_sq) / safe_sq, 0.0)
    return green * x_weights[:, None, None] * y_weights[None, :, None] * z_weights[None, None, :]


def forward_lines(charge, fourier_rows):
    along_z = jnp.einsum("pyz,kz->pyk", charge, fourier_rows, precision=EXACT)
    return jnp.einsum("jy,pyk->pjk", fourier_rows, along_z, precision=EXACT)


def inverse_lines(spectrum, fourier_rows):
    along_z = jnp.einsum("pjk,kz->pjz", spectrum, fourier_rows, precision=EXACT)
    return jnp.einsum("jy,pjz->pyz", fourier_rows, along_z, precision=EXACT)


def per_device_general(positions, field, inv_polar, x_spline, yz_spline, tile_list, tile_count):
    rank_count = lax.axis_size("gx")
    rank_index = lax.axis_index("gx")
    atoms_here = positions.shape[1]
    planes = GRID // rank_count
    extent = planes + 4
    halo_atoms = HALO_BLK * TILE
    slab_blocks = atoms_here // TILE
    local_plane = jnp.arange(atoms_here, dtype=jnp.int32) * planes // atoms_here
    spline_value, spline_slope = slab_weights(local_plane, x_spline, extent)
    ext_pos = extended(positions, (("gx", 1),), halo_atoms)
    shift_x = jnp.concatenate(
        [
            jnp.full((halo_atoms,), -1.0 * slab_blocks, jnp.float32),
            jnp.zeros((atoms_here,), jnp.float32),
            jnp.full((halo_atoms,), 1.0 * slab_blocks, jnp.float32),
        ]
    )
    ext_pos = ext_pos.at[0].add(shift_x)
    fourier_rows = basis_rows(GRID, jnp.arange(GRID, dtype=jnp.int32))
    ky_count = GRID // rank_count
    all_freq = jnp.arange(GRID, dtype=jnp.int32)
    ky_freq = rank_index * ky_count + jnp.arange(ky_count, dtype=jnp.int32)
    full_modes, full_weights = mode_of(all_freq, GRID)
    ky_modes, ky_weights = mode_of(ky_freq, GRID)
    kernel = kernel_block(full_modes, full_weights, ky_modes, ky_weights, full_modes, full_weights)
    kernel = kernel.reshape(GRID, ky_count * GRID)
    source_rows = jnp.arange(rank_count * extent, dtype=jnp.int32)
    points = (source_rows // extent * planes - 2 + source_rows % extent) % GRID
    across = basis_rows(GRID, points)

    def reciprocal(charge):
        spectrum = forward_lines(charge, fourier_rows)
        pencils = lax.all_to_all(spectrum, "gx", split_axis=1, concat_axis=0, tiled=True)
        rows_in = pencils.shape[0]
        flat_pencils = pencils.reshape(rows_in, ky_count * GRID)
        spectral_lines = jnp.dot(across, flat_pencils, precision=EXACT) * kernel
        returned_lines = lax.dot_general(
            across, spectral_lines, (((0,), (0,)), ((), ())), precision=EXACT
        )
        returned = lax.all_to_all(
            returned_lines.reshape(rows_in, ky_count, GRID),
            "gx",
            split_axis=0,
            concat_axis=1,
            tiled=True,
        )
        return inverse_lines(returned, fourier_rows)

    def apply(vector):
        ext_vec = extended(vector, (("gx", 1),), halo_atoms)
        near_field = pair_field(positions, ext_pos, ext_vec, tile_list, tile_count)
        charge = spread_dipoles(vector, spline_value, spline_slope, yz_spline)
        far_field = gather_field(reciprocal(charge), spline_value, spline_slope, yz_spline)
        return inv_polar[None, :] * vector + far_field - near_field

    def paired(residual, precond, applied):
        return lax.psum((jnp.sum(residual * precond), jnp.sum(applied * precond)), "gx")

    dipoles = jnp.zeros_like(field)
    residual = field
    precond = field / inv_polar[None, :]
    applied = apply(precond)
    rz_now, curvature = paired(residual, precond, applied)
    step_size = rz_now / curvature
    direction = precond
    applied_dir = applied
    for sweep_index in range(ITERS):
        dipoles = dipoles + step_size * direction
        residual = residual - step_size * applied_dir
        if sweep_index + 1 < ITERS:
            precond = residual / inv_polar[None, :]
            applied = apply(precond)
            rz_next, curvature = paired(residual, precond, applied)
            beta_ratio = rz_next / rz_now
            step_size = rz_next / (curvature - beta_ratio * rz_next / step_size)
            direction = precond + beta_ratio * direction
            applied_dir = applied + beta_ratio * applied_dir
            rz_now = rz_next
    return (dipoles, residual)


F32 = jnp.float32
BF16 = jnp.bfloat16
ROWS = 8
SPAN = 2 * HALO_BLK + 1
IN_VMEM = pl.BlockSpec(memory_space=pltpu.VMEM)
IN_SMEM = pl.BlockSpec(memory_space=pltpu.SMEM)
IN_HBM = pl.BlockSpec(memory_space=pl.ANY)
REACH = ORDER - 1
NT = (((1,), (1,)), ((), ()))


def params(flops, vmem=None):
    return dict(
        cost_estimate=pl.CostEstimate(flops=flops, bytes_accessed=4 << 20, transcendentals=0),
        compiler_params=pltpu.CompilerParams(vmem_limit_bytes=vmem) if vmem else None,
    )


def halves(x):
    high = x.astype(BF16).astype(F32)
    return high, x - high


def bdot(a, b):
    return jnp.dot(a, b, preferred_element_type=F32)


def spline_values(u):
    w = 1.0 - u
    u2, w2 = u * u, w * w
    c = 1.0 / 24.0
    return [
        c * (w2 * w2),
        c * (11.0 + u * (-12.0 + u * (-6.0 + u * (12.0 - 4.0 * u)))),
        c * (11.0 + u * (12.0 + u * (-6.0 + u * (-12.0 + 6.0 * u)))),
        c * (1.0 + u * (4.0 + u * (6.0 + u * (4.0 - 4.0 * u)))),
        c * (u2 * u2),
    ]


def spline_slopes(u):
    w = 1.0 - u
    c = 1.0 / 6.0
    return [
        -c * (w * w * w),
        c * (-3.0 + u * (-3.0 + u * (9.0 - 4.0 * u))),
        c * (3.0 + u * (-3.0 + u * (-9.0 + 6.0 * u))),
        c * (1.0 + u * (3.0 + u * (3.0 - 4.0 * u))),
        c * (u * u * u),
    ]


def block_rows(ref, row):
    return jnp.concatenate(
        [ref[row : row + 1, b * TILE : (b + 1) * TILE] for b in range(ref.shape[1] // TILE)], axis=0
    )


def pack_kernel(field_ref, ip_ref, xs_ref, yz_ref, own_ref, inv_ref, out_ref):
    parts = out_ref.shape[0]
    blocks = field_ref.shape[1] // TILE
    grid = yz_ref.shape[2]
    inv = block_rows(ip_ref, 0)
    inv_ref[...] = inv
    tiles = [block_rows(field_ref, c) / inv for c in range(3)]
    for c in range(3):
        own_ref[c * blocks : (c + 1) * blocks, :] = tiles[c]
    tiles.append(sum(float(k) * block_rows(xs_ref, k) for k in range(1, ORDER)) - 1.5)
    line = lax.broadcasted_iota(jnp.int32, (grid, TILE), 0)
    for axis in range(2):
        starts, offsets = [], []
        for b in range(blocks):
            here = slice(b * TILE, (b + 1) * TILE)
            value = yz_ref[2 * axis, here, :].T
            slope = yz_ref[2 * axis + 1, here, :].T
            used = jnp.where((value != 0.0) | (slope != 0.0), 1.0, 0.0)
            first = used * (1.0 - pltpu.roll(used, 1, 0))
            start = jnp.sum(first * line.astype(F32), axis=0, keepdims=True)
            offset = (line - start.astype(jnp.int32)) & (grid - 1)
            starts.append(start)
            offsets.append(jnp.sum(value * offset.astype(F32), axis=0, keepdims=True) - 1.5)
        tiles.append(jnp.concatenate(starts, axis=0))
        tiles.append(jnp.concatenate(offsets, axis=0))
    for d in range(parts):
        for i, tile in enumerate(tiles):
            out_ref[d, i * blocks : (i + 1) * blocks, :] = tile


def pack_call(field, inv_row, xs, yz, parts):
    blocks = field.shape[1] // TILE
    return pl.pallas_call(
        pack_kernel,
        in_specs=[IN_VMEM] * 4,
        out_specs=[IN_VMEM] * 3,
        out_shape=[
            jax.ShapeDtypeStruct((3 * blocks, TILE), F32),
            jax.ShapeDtypeStruct((blocks, TILE), F32),
            jax.ShapeDtypeStruct((parts, 8 * blocks, TILE), F32),
        ],
        name="pack",
        **params(1 << 26),
    )(field, inv_row, xs, yz)


def prep_kernel(atom_ref, rows_ref, turn_ref, tab_ref, yt_ref):
    blocks = tab_ref.shape[0]
    grid = rows_ref.shape[0]
    tile = lambda i: atom_ref[0, i * blocks : (i + 1) * blocks, :]
    high, low = halves(rows_ref[...])
    twice = jnp.concatenate([high, low], axis=0).astype(BF16)
    matrix = jnp.concatenate([twice, twice], axis=1)
    line = lax.broadcasted_iota(jnp.int32, (grid, TILE), 0)
    start_z, u_z = tile(6).astype(jnp.int32), tile(7)
    values, slopes = spline_values(u_z), spline_slopes(u_z)
    spots = [(start_z + k) & (grid - 1) for k in range(ORDER)]
    for b in range(blocks):
        row = slice(b, b + 1)
        dense = jnp.zeros((grid, TILE), F32)
        tilted = dense
        for k in range(ORDER):
            here = line == spots[k][row]
            dense = jnp.where(here, values[k][row], dense)
            tilted = jnp.where(here, slopes[k][row], tilted)
        high, low = halves(jnp.concatenate([dense, tilted], axis=1))
        both = bdot(matrix, jnp.concatenate([high, low], axis=0).astype(BF16))
        high, low = halves(both[:grid] + both[grid:])
        tab_ref[b] = jnp.concatenate([high, low], axis=0).astype(BF16)
    start_y, u_y = tile(4), tile(5)
    values, slopes = spline_values(u_y), spline_slopes(u_y)
    mode, sine = turn_ref[0], turn_ref[1]
    half = float(grid // 2)
    for b in range(blocks):
        row = slice(b, b + 1)
        phase = (mode * start_y[row]).astype(jnp.int32) + grid // 2
        angle = ((phase & (grid - 1)).astype(F32) - half) * (jnp.pi / (4.0 * half))
        sq = angle * angle
        s = angle * (1.0 + sq * (-1.0 / 6 + sq * (1.0 / 120 + sq * (-1.0 / 5040 + sq / 362880))))
        c = 1.0 + sq * (-0.5 + sq * (1.0 / 24 + sq * (-1.0 / 720 + sq / 40320)))
        for _ in range(2):
            s, c = 2.0 * s * c, 1.0 - 2.0 * s * s
        lead = jnp.where(sine > 0.0, s, c)
        side = jnp.where(sine > 0.0, -c, s)
        for i, weights in enumerate((values, slopes)):
            even = weights[0][row] + sum(weights[k][row] * turn_ref[1 + k] for k in range(1, ORDER))
            odd = sum(weights[k][row] * turn_ref[ORDER + k] for k in range(1, ORDER))
            yt_ref[b, i * ROWS : (i + 1) * ROWS, :] = lead * even - side * odd


def prep_call(atoms, rows, turns, blocks):
    parts = atoms.shape[0]
    grid = rows.shape[0]
    return pl.pallas_call(
        prep_kernel,
        grid=(parts,),
        in_specs=[
            pl.BlockSpec((1, 8 * blocks, TILE), lambda s: (s, 0, 0)),
            pl.BlockSpec(rows.shape, lambda s: (0, 0)),
            pl.BlockSpec(turns.shape, lambda s: (0, 0, 0)),
        ],
        out_specs=[
            pl.BlockSpec((blocks, 2 * grid, 2 * TILE), lambda s: (s, 0, 0)),
            pl.BlockSpec((blocks, 2 * ROWS, TILE), lambda s: (s, 0, 0)),
        ],
        out_shape=[
            jax.ShapeDtypeStruct((parts * blocks, 2 * grid, 2 * TILE), BF16),
            jax.ShapeDtypeStruct((parts * blocks, 2 * ROWS, TILE), F32),
        ],
        name="prep",
        **params(1 << 31),
    )(atoms, rows, turns)


def field_kernel(with_sums, v_ref, atom_ref, tab_hbm, yt_ref, rows_ref, cols_ref, kern_ref, *rest):
    if with_sums:
        sums_ref, out_ref, tab, sem, grid_ref = rest
    else:
        out_ref, tab, sem, grid_ref = rest
    parts = out_ref.shape[0]
    grid = rows_ref.shape[0]
    blocks = tab.shape[0] // parts
    width = ROWS * ORDER

    def fetch(s):
        part = pl.ds(s * blocks, blocks)
        return pltpu.make_async_copy(tab_hbm.at[part], tab.at[part], sem.at[s])

    for s in range(parts):
        fetch(s).start()
    grid_ref[...] = jnp.zeros(grid_ref.shape, F32)

    def plane(q):
        return pl.ds(pl.multiple_of(q * ROWS, ROWS), ROWS)

    def x_weights(s):
        u = atom_ref[s, 3 * blocks : 4 * blocks, :]
        return spline_values(u), spline_slopes(u)

    def spread(s, carry):
        fetch(s).wait()
        value, slope = x_weights(s)
        vec = [v_ref[s, c * blocks : (c + 1) * blocks, :] for c in range(3)]
        a0 = [vec[0] * slope[k] for k in range(ORDER)]
        a1 = [vec[1] * value[k] for k in range(ORDER)]
        a2 = [vec[2] * value[k] for k in range(ORDER)]
        sums = [jnp.zeros((ROWS, grid), F32) for _ in range(blocks + REACH)]
        for b in range(blocks):
            g = s * blocks + b
            row = slice(b, b + 1)
            yt, dyt = yt_ref[g, 0:ROWS, :], yt_ref[g, ROWS : 2 * ROWS, :]
            lead = jnp.concatenate([a0[k][row] * yt + a1[k][row] * dyt for k in range(ORDER)], axis=0)
            tail = jnp.concatenate([a2[k][row] * yt for k in range(ORDER)], axis=0)
            high, low = halves(jnp.concatenate([lead, tail], axis=1))
            lhs = jnp.concatenate([high, low], axis=0).astype(BF16)
            out = lax.dot_general(lhs, tab[g], NT, preferred_element_type=F32)
            out = out[:width] + out[width:]
            out = out[:, :grid] + out[:, grid:]
            for k in range(ORDER):
                sums[b + k] = sums[b + k] + out[k * ROWS : (k + 1) * ROWS]
        for j, tile in enumerate(sums):
            grid_ref[plane(s * blocks + j), :] += tile
        return carry

    lax.fori_loop(0, parts, spread, 0)
    side = REACH // 2
    body = slice(side * ROWS, (side + grid) * ROWS)
    left, right = slice(0, side * ROWS), slice((side + grid) * ROWS, (2 * side + grid) * ROWS)
    first = slice(side * ROWS, 2 * side * ROWS)
    last = slice(grid * ROWS, (side + grid) * ROWS)
    grid_ref[last, :] += grid_ref[left, :]
    grid_ref[first, :] += grid_ref[right, :]

    def product(matrix, x):
        mh, ml = halves(matrix)
        xh, xl = halves(x)
        rhs = jnp.concatenate([xh, xl], axis=0).astype(BF16)
        mh, ml = mh.astype(BF16), ml.astype(BF16)
        return bdot(jnp.concatenate([mh, mh], axis=1), rhs) + bdot(
            jnp.concatenate([ml, ml], axis=1), rhs
        )

    def lines(j):
        return pl.ds(side * ROWS + j, grid, stride=ROWS)

    charge = jnp.concatenate([grid_ref[lines(j), :] for j in range(ROWS)], axis=1)
    spectrum = product(rows_ref[...], charge)
    weighted = spectrum * kern_ref[...]
    potential = product(cols_ref[...], weighted)
    for j in range(ROWS):
        grid_ref[lines(j), :] = potential[:, j * grid : (j + 1) * grid]
    grid_ref[left, :] = grid_ref[last, :]
    grid_ref[right, :] = grid_ref[first, :]
    if with_sums:
        energy = jnp.sum(spectrum * weighted)
        row = lax.broadcasted_iota(jnp.int32, sums_ref.shape, 0)
        sums = sums_ref[...] + jnp.where(row == 5, energy, 0.0)
        for d in range(parts):
            out_ref[d, 3 * blocks :, :] = sums

    def gather(s, carry):
        value, slope = x_weights(s)
        pieces = [halves(grid_ref[plane(s * blocks + q), :]) for q in range(blocks + REACH)]
        fields = ([], [], [])
        for b in range(blocks):
            g = s * blocks + b
            row = slice(b, b + 1)
            yt, dyt = yt_ref[g, 0:ROWS, :], yt_ref[g, ROWS : 2 * ROWS, :]
            near = pieces[b : b + ORDER]
            lhs = jnp.concatenate([x[0] for x in near] + [x[1] for x in near], axis=0).astype(BF16)
            out = bdot(jnp.concatenate([lhs, lhs], axis=1), tab[g])
            out = out[:width] + out[width:]
            tiles = [out[k * ROWS : (k + 1) * ROWS] for k in range(ORDER)]
            f0 = sum(slope[k][row] * tiles[k][:, :TILE] for k in range(ORDER))
            f1 = sum(value[k][row] * tiles[k][:, :TILE] for k in range(ORDER))
            f2 = sum(value[k][row] * tiles[k][:, TILE:] for k in range(ORDER))
            for i, part in enumerate((yt * f0, dyt * f1, yt * f2)):
                fields[i].append(jnp.sum(part, axis=0, keepdims=True))
        for i in range(3):
            out_ref[s, i * blocks : (i + 1) * blocks, :] = jnp.concatenate(fields[i], axis=0)
        return carry

    lax.fori_loop(0, parts, gather, 0)


def field_call(vec, atoms, table, yt, rows, cols, kern, sums=None):
    parts = vec.shape[0]
    grid = rows.shape[0]
    blocks = yt.shape[0] // parts
    args = [vec, atoms, table, yt, rows, cols, kern]
    specs = [IN_VMEM, IN_VMEM, IN_HBM] + [IN_VMEM] * 4
    out_rows = 3 * blocks
    if sums is not None:
        args.append(sums)
        specs.append(IN_VMEM)
        out_rows += ROWS
    return pl.pallas_call(
        lambda *refs: field_kernel(sums is not None, *refs),
        in_specs=specs,
        out_specs=IN_VMEM,
        out_shape=jax.ShapeDtypeStruct((parts, out_rows, TILE), F32),
        scratch_shapes=[
            pltpu.VMEM(table.shape, BF16),
            pltpu.SemaphoreType.DMA((parts,)),
            pltpu.VMEM(((grid + REACH) * ROWS, grid), F32),
        ],
        name="field",
        **params(1 << 31, 56 << 20),
    )(*args)


def pair_kernel(wts_ref, rank_ref, left_ref, pos_ref, right_ref, col_ref, vec_ref, out_ref, acc_ref, near_ref):
    blocks = pos_ref.shape[1] // TILE
    ext = blocks + 2 * HALO_BLK
    total = vec_ref.shape[0] * blocks
    chunk = 32
    shift = 1.0 * blocks
    for c in range(3):
        for j in range(ext):
            if j < HALO_BLK:
                row = left_ref[c : c + 1, j * TILE : (j + 1) * TILE] - (shift if c == 0 else 0.0)
            elif j < HALO_BLK + blocks:
                i = j - HALO_BLK
                row = pos_ref[c : c + 1, i * TILE : (i + 1) * TILE]
            else:
                i = j - HALO_BLK - blocks
                row = right_ref[c : c + 1, i * TILE : (i + 1) * TILE] + (shift if c == 0 else 0.0)
            near_ref[j, c : c + 1, :] = row
            g = lax.rem(rank_ref[0] * blocks + (j - HALO_BLK) + total, total)
            src = lax.div(g, blocks)
            near_ref[j, 3 + c : 4 + c, :] = vec_ref[src, pl.ds(c * blocks + g - src * blocks, 1), :]

    def one_block(b, carry):
        for c in range(TILE // chunk):
            home = col_ref[pl.ds(pl.multiple_of(b * TILE + c * chunk, chunk), chunk), :]
            shape = (chunk, TILE)
            hx = jnp.broadcast_to(home[:, 0:1], shape)
            hy = jnp.broadcast_to(home[:, 1:2], shape)
            hz = jnp.broadcast_to(home[:, 2:3], shape)
            sx = sy = sz = jnp.zeros(shape, F32)
            for e in range(SPAN):
                near = near_ref[b + e]
                dx, dy, dz = hx - near[0:1], hy - near[1:2], hz - near[2:3]
                vx, vy, vz = near[3:4], near[4:5], near[5:6]
                inverse = lax.rsqrt(dx * dx + dy * dy + dz * dz + 1.0)
                square = inverse * inverse
                third = wts_ref[b * SPAN + e] * (inverse * square)
                if e == HALO_BLK:
                    row = lax.broadcasted_iota(jnp.int32, shape, 0) + c * chunk
                    lane = lax.broadcasted_iota(jnp.int32, shape, 1)
                    third = jnp.where(row == lane, 0.0, third)
                fifth = 3.0 * (third * square) * (dx * vx + dy * vy + dz * vz)
                sx = sx + (third * vx - fifth * dx)
                sy = sy + (third * vy - fifth * dy)
                sz = sz + (third * vz - fifth * dz)
            acc_ref[0, pl.ds(c * chunk, chunk), :] = sx
            acc_ref[1, pl.ds(c * chunk, chunk), :] = sy
            acc_ref[2, pl.ds(c * chunk, chunk), :] = sz
        for i in range(3):
            out_ref[pl.ds(i * blocks + b, 1), :] = PAIR_C * jnp.sum(acc_ref[i].T, axis=0, keepdims=True)
        return carry

    lax.fori_loop(0, blocks, one_block, 0)


def pair_call(wts, rank, left, pos, right, cols, vec):
    blocks = pos.shape[1] // TILE
    return pl.pallas_call(
        pair_kernel,
        in_specs=[IN_SMEM, IN_SMEM] + [IN_VMEM] * 5,
        out_specs=IN_VMEM,
        out_shape=jax.ShapeDtypeStruct((3 * blocks, TILE), F32),
        scratch_shapes=[
            pltpu.VMEM((3, TILE, TILE), F32),
            pltpu.VMEM((blocks + 2 * HALO_BLK, ROWS, TILE), F32),
        ],
        name="pair",
        **params(1 << 30),
    )(wts, rank, left, pos, right, cols, vec)


def update_kernel(ret_ref, pair_ref, inv_ref, own_ref, out_ref):
    blocks = inv_ref.shape[0]
    far = jnp.sum(ret_ref[...], axis=0) - pair_ref[...]
    inv = inv_ref[...]
    vec = jnp.concatenate([far[c * blocks : (c + 1) * blocks] / inv for c in range(3)], axis=0)
    own_ref[...] = vec
    for d in range(out_ref.shape[0]):
        out_ref[d] = vec


def update_call(returned, pair, inv):
    parts = returned.shape[0]
    return pl.pallas_call(
        update_kernel,
        in_specs=[IN_VMEM] * 3,
        out_specs=[IN_VMEM] * 2,
        out_shape=[
            jax.ShapeDtypeStruct(pair.shape, F32),
            jax.ShapeDtypeStruct((parts,) + pair.shape, F32),
        ],
        name="update",
        **params(1 << 24),
    )(returned, pair, inv)


def moments_kernel(v0_ref, v1_ref, v2_ref, inv_ref, pair_ref, out_ref):
    ip = jnp.concatenate([inv_ref[...]] * 3, axis=0)
    v0, v1, v2 = v0_ref[...], v1_ref[...], v2_ref[...]
    d1, d2 = ip * v1, ip * v2
    terms = (v0 * (ip * v0), v0 * d1, v1 * d1, v1 * d2, v2 * d2, -(v2 * pair_ref[...]))
    row = lax.broadcasted_iota(jnp.int32, out_ref.shape, 0)
    sums = jnp.zeros(out_ref.shape, F32)
    for k, term in enumerate(terms):
        sums = sums + jnp.where(row == k, jnp.sum(term), 0.0)
    out_ref[...] = sums


def moments_call(vectors, inv, pair):
    return pl.pallas_call(
        moments_kernel,
        in_specs=[IN_VMEM] * 5,
        out_specs=IN_VMEM,
        out_shape=jax.ShapeDtypeStruct((ROWS, TILE), F32),
        name="moments",
        **params(1 << 24),
    )(*vectors, inv, pair)


def finish_kernel(ret_ref, pair_ref, v0_ref, v1_ref, v2_ref, inv_ref, dip_ref, res_ref):
    blocks = inv_ref.shape[0]
    summed = jnp.sum(ret_ref[...], axis=0)
    total = summed[3 * blocks :]
    h = summed[: 3 * blocks] - pair_ref[...]
    m = [total[k : k + 1, 0:1] for k in range(6)]
    s = [lax.rsqrt(m[2 * i]) for i in range(3)]
    g = [[m[i + j] * s[i] * s[j] for j in range(3)] for i in range(3)]
    b = [-m[i + 3] * s[i] for i in range(3)]
    l10 = g[1][0] / g[0][0]
    l20 = g[2][0] / g[0][0]
    p11 = g[1][1] - l10 * g[0][1]
    p12 = g[1][2] - l10 * g[0][2]
    l21 = p12 / p11
    p22 = g[2][2] - l20 * g[0][2] - l21 * p12
    b1 = b[1] - l10 * b[0]
    b2 = b[2] - l20 * b[0] - l21 * b1
    y2 = b2 / p22
    y1 = (b1 - p12 * y2) / p11
    y0 = (b[0] - g[0][1] * y1 - g[0][2] * y2) / g[0][0]
    a0, a1, a2 = s[0] * y0, s[1] * y1, s[2] * y2
    scale = 1.0 / (a0 - a1 + a2 - 1.0)
    a0, a1, a2, a3 = a0 * scale, a1 * scale, a2 * scale, scale
    c2 = -a3
    c1 = a3 - a2
    c0 = a2 - a3 - a1
    ip = jnp.concatenate([inv_ref[...]] * 3, axis=0)
    v0, v1, v2 = v0_ref[...], v1_ref[...], v2_ref[...]
    dip = c0 * v0 + c1 * v1 + c2 * v2
    res = ip * (a0 * v0 + a1 * v1 + a2 * v2) + a3 * h
    for c in range(3):
        for b in range(blocks):
            row = slice(c * blocks + b, c * blocks + b + 1)
            here = slice(b * TILE, (b + 1) * TILE)
            dip_ref[c : c + 1, here] = dip[row]
            res_ref[c : c + 1, here] = res[row]


def finish_call(returned, pair, vectors, inv):
    atoms = inv.shape[0] * TILE
    return pl.pallas_call(
        finish_kernel,
        in_specs=[IN_VMEM] * 6,
        out_specs=[IN_VMEM] * 2,
        out_shape=[jax.ShapeDtypeStruct((3, atoms), F32)] * 2,
        name="finish",
        **params(1 << 24),
    )(returned, pair, *vectors, inv)


def fourier_matrix(size):
    freq = np.arange(size)
    mode = np.where(freq <= size // 2, freq, freq - size // 2)
    angle = (mode[:, None] * np.arange(size)[None, :] % size) * (2.0 * np.pi / size)
    rows = np.where((freq <= size // 2)[:, None], np.cos(angle), np.sin(angle))
    return rows.astype(np.float32)


def swap(x):
    return lax.all_to_all(x, "gx", split_axis=0, concat_axis=0, tiled=True)


def per_device_modes(positions, field, inv_polar, x_spline, yz_spline, tile_list, tile_count):
    parts = lax.axis_size("gx")
    rank = lax.axis_index("gx")
    atoms = positions.shape[1]
    halo = HALO_BLK * TILE
    blocks = atoms // TILE
    up = [(i, (i + 1) % parts) for i in range(parts)]
    down = [(j, i) for i, j in up]

    own, inv, packed = pack_call(
        field, inv_polar[None, :], x_spline.reshape(2 * ORDER, atoms), yz_spline, parts
    )
    everyone = swap(packed)
    left = lax.ppermute(positions[:, atoms - halo :], "gx", up)
    right = lax.ppermute(positions[:, :halo], "gx", down)
    home_cols = jnp.pad(positions, ((0, ROWS - 3), (0, 0))).T

    offsets = jnp.arange(SPAN, dtype=jnp.int32)
    block_ids = jnp.arange(blocks, dtype=jnp.int32)
    live = jnp.arange(tile_list.shape[1], dtype=jnp.int32)[None, :] < tile_count[:, None]
    hit = tile_list[:, :, None] == block_ids[:, None, None] + offsets[None, None, :]
    wts = jnp.sum((hit & live[:, :, None]).astype(F32), axis=1).reshape(-1)

    matrix = fourier_matrix(GRID)
    rows, cols = jnp.asarray(matrix), jnp.asarray(matrix.T)
    all_freq = jnp.arange(GRID, dtype=jnp.int32)
    ky_count = GRID // parts
    ky_freq = rank * ky_count + jnp.arange(ky_count, dtype=jnp.int32)
    full_modes, full_weights = mode_of(all_freq, GRID)
    ky_modes, ky_weights = mode_of(ky_freq, GRID)
    kern = kernel_block(full_modes, full_weights, ky_modes, ky_weights, full_modes, full_weights)
    kern = kern.reshape(GRID, ky_count * GRID)
    steps = jnp.arange(1, ORDER).astype(F32)
    angle = steps[:, None] * ky_modes[None, :] * (2.0 * jnp.pi / GRID)
    sine = (ky_freq > GRID // 2).astype(F32)
    turns = jnp.concatenate([ky_modes[None], sine[None], jnp.cos(angle), jnp.sin(angle)])
    turns = jnp.broadcast_to(turns[:, :, None], turns.shape + (TILE,))

    table, yt = prep_call(everyone, rows, turns, blocks)
    vec, vectors = everyone, [own]
    rank_id = rank[None].astype(jnp.int32)
    for step in range(ITERS):
        last = step + 1 == ITERS
        pair = pair_call(wts, rank_id, left, positions, right, home_cols, vec)
        sums = moments_call(vectors, inv, pair) if last else None
        returned = swap(field_call(vec, everyone, table, yt, rows, cols, kern, sums))
        if not last:
            own, packed = update_call(returned, pair, inv)
            vectors.append(own)
            vec = swap(packed)
    dipoles, residual = finish_call(returned, pair, vectors, inv)
    return (dipoles, residual)


def per_device(positions, *others):
    parts = lax.axis_size("gx")
    atoms = positions.shape[1]
    planes = GRID // parts
    modes = (
        parts * ROWS == GRID
        and atoms == planes * TILE
        and planes == ROWS
        and atoms >= HALO_BLK * TILE
        and ORDER == 5
        and ITERS == 3
    )
    run = per_device_modes if modes else per_device_general
    return run(positions, *others)


def solution(mesh):
    placed = (
        P(None, ("rep", "gx")),
        P(None, ("rep", "gx")),
        P(("rep", "gx")),
        P(None, None, ("rep", "gx")),
        P(None, ("rep", "gx"), None),
        P(("rep", "gx"), None),
        P(("rep", "gx")),
    )
    return jax.shard_map(
        per_device,
        mesh=mesh,
        in_specs=placed,
        out_specs=(P(None, ("rep", "gx")), P(None, ("rep", "gx"))),
        check_vma=False,
    )
```

```python
import jax
import numpy as np
import jax.numpy as jnp
from jax import lax
from jax.experimental import pallas as pl
from jax.experimental.pallas import tpu as pltpu
from jax.sharding import PartitionSpec as P

GRID = 128
ORDER = 5
TILE = 128
HALO_BLK = 3
ITERS = 3


PAIR_C = 0.025
RECIP_C = 8192.0
DAMP = 0.0008
EXACT = lax.Precision.HIGHEST


def extended(x, sides, width):
    for axis, dim in sides:
        devices, length = (lax.axis_size(axis), x.shape[dim])
        up = [(i, (i + 1) % devices) for i in range(devices)]
        down = [(j, i) for i, j in up]
        last = lax.slice_in_dim(x, length - width, length, axis=dim)
        first = lax.slice_in_dim(x, 0, width, axis=dim)
        before = lax.ppermute(last, axis, up)
        after = lax.ppermute(first, axis, down)
        x = jnp.concatenate([before, x, after], axis=dim)
    return x


def pair_field(home_pos, ext_pos, ext_vec, tile_rows, live_counts):
    slab_blocks = home_pos.shape[1] // TILE
    ext_blocks = ext_pos.shape[1] // TILE
    home_blocks = home_pos.reshape(3, slab_blocks, TILE).transpose(1, 0, 2)
    pos_blocks = ext_pos.reshape(3, ext_blocks, TILE)
    vec_blocks = ext_vec.reshape(3, ext_blocks, TILE)
    slot_index = jnp.arange(tile_rows.shape[1], dtype=jnp.int32)
    self_pair = jnp.eye(TILE, dtype=bool)

    def one_block(carried, scan_item):
        home_block, tile_row, live_count, block_index = scan_item
        near_pos = jnp.take(pos_blocks, tile_row, axis=1)
        near_vec = jnp.take(vec_blocks, tile_row, axis=1)
        offsets = home_block[:, None, :, None] - near_pos[:, :, None, :]
        distance_sq = jnp.sum(offsets * offsets, axis=0) + 1.0
        inverse = lax.rsqrt(distance_sq)
        third_power = inverse * inverse * inverse
        fifth_power = third_power * inverse * inverse
        same_block = (tile_row == block_index + HALO_BLK)[:, None, None]
        live_mask = (slot_index < live_count)[:, None, None] & ~(same_block & self_pair[None])
        third_power = jnp.where(live_mask, third_power, 0.0)
        fifth_power = jnp.where(live_mask, fifth_power, 0.0)
        projection = jnp.sum(offsets * near_vec[:, :, None, :], axis=0)
        field_sum = jnp.sum(
            third_power[None] * near_vec[:, :, None, :]
            - 3.0 * (fifth_power * projection)[None] * offsets,
            axis=(1, 3),
        )
        return (carried, PAIR_C * field_sum)

    block_ids = jnp.arange(slab_blocks, dtype=jnp.int32)
    _, blocks_out = lax.scan(
        one_block, jnp.zeros((), jnp.float32), (home_blocks, tile_rows, live_counts, block_ids)
    )
    return blocks_out.transpose(1, 0, 2).reshape(3, slab_blocks * TILE)


def slab_weights(local_plane, x_spline, planes):
    spline_steps = jnp.arange(ORDER, dtype=jnp.int32)
    plane_index = jnp.arange(planes, dtype=jnp.int32)
    matches = local_plane[None, :, None] + spline_steps[:, None, None] == plane_index[None, None, :]
    spline_value = jnp.sum(jnp.where(matches, x_spline[0][:, :, None], 0.0), axis=0)
    spline_slope = jnp.sum(jnp.where(matches, x_spline[1][:, :, None], 0.0), axis=0)
    return (spline_value, spline_slope)


def spread_dipoles(vector, spline_value, spline_slope, yz_spline):
    atoms_here = spline_value.shape[0]
    planes = spline_value.shape[1]
    grid_lines = yz_spline.shape[2]
    lead_terms = (vector[0][:, None] * spline_slope)[:, :, None] * yz_spline[0][:, None, :]
    lead_terms = (
        lead_terms + (vector[1][:, None] * spline_value)[:, :, None] * yz_spline[1][:, None, :]
    )
    tail_terms = (vector[2][:, None] * spline_value)[:, :, None] * yz_spline[0][:, None, :]
    contract = (((0,), (0,)), ((), ()))
    charge = lax.dot_general(
        lead_terms.reshape(atoms_here, planes * grid_lines), yz_spline[2], contract, precision=EXACT
    )
    charge = charge + lax.dot_general(
        tail_terms.reshape(atoms_here, planes * grid_lines), yz_spline[3], contract, precision=EXACT
    )
    return charge.reshape(planes, grid_lines, grid_lines)


def gather_field(potential, spline_value, spline_slope, yz_spline):
    planes = potential.shape[0]
    grid_lines = potential.shape[1]
    atoms_here = spline_value.shape[0]
    flat_grid = potential.reshape(planes * grid_lines, grid_lines)
    contract = (((1,), (1,)), ((), ()))
    plain_sum = lax.dot_general(yz_spline[2], flat_grid, contract, precision=EXACT).reshape(
        atoms_here, planes, grid_lines
    )
    tilted_sum = lax.dot_general(yz_spline[3], flat_grid, contract, precision=EXACT).reshape(
        atoms_here, planes, grid_lines
    )
    first_comp = jnp.sum(
        spline_slope[:, :, None] * yz_spline[0][:, None, :] * plain_sum, axis=(1, 2)
    )
    second_comp = jnp.sum(
        spline_value[:, :, None] * yz_spline[1][:, None, :] * plain_sum, axis=(1, 2)
    )
    third_comp = jnp.sum(
        spline_value[:, :, None] * yz_spline[0][:, None, :] * tilted_sum, axis=(1, 2)
    )
    return jnp.stack([first_comp, second_comp, third_comp])


def mode_of(freq, size):
    half_size = size // 2
    mode_num = jnp.where(freq <= half_size, freq, freq - half_size)
    weight = jnp.where((freq == 0) | (freq == half_size), 1.0 / size, 2.0 / size)
    return (mode_num.astype(jnp.float32), weight.astype(jnp.float32))


def basis_rows(size, points):
    freq = jnp.arange(size, dtype=jnp.int32)
    half_size = size // 2
    mode_num = jnp.where(freq <= half_size, freq, freq - half_size)
    phase = mode_num[:, None] * points[None, :] % size
    angle = phase.astype(jnp.float32) * (2.0 * jnp.pi / size)
    return jnp.where((freq <= half_size)[:, None], jnp.cos(angle), jnp.sin(angle))


def kernel_block(x_modes, x_weights, y_modes, y_weights, z_modes, z_weights):
    mode_sq = (
        x_modes[:, None, None] * x_modes[:, None, None]
        + y_modes[None, :, None] * y_modes[None, :, None]
        + z_modes[None, None, :] * z_modes[None, None, :]
    )
    safe_sq = jnp.where(mode_sq > 0, mode_sq, 1.0)
    green = jnp.where(mode_sq > 0, RECIP_C * jnp.exp(-DAMP * safe_sq) / safe_sq, 0.0)
    return green * x_weights[:, None, None] * y_weights[None, :, None] * z_weights[None, None, :]


def forward_lines(charge, fourier_rows):
    along_z = jnp.einsum("pyz,kz->pyk", charge, fourier_rows, precision=EXACT)
    return jnp.einsum("jy,pyk->pjk", fourier_rows, along_z, precision=EXACT)


def inverse_lines(spectrum, fourier_rows):
    along_z = jnp.einsum("pjk,kz->pjz", spectrum, fourier_rows, precision=EXACT)
    return jnp.einsum("jy,pjz->pyz", fourier_rows, along_z, precision=EXACT)


def per_device_general(positions, field, inv_polar, x_spline, yz_spline, tile_list, tile_count):
    rank_count = lax.axis_size("gx")
    rank_index = lax.axis_index("gx")
    atoms_here = positions.shape[1]
    planes = GRID // rank_count
    extent = planes + 4
    halo_atoms = HALO_BLK * TILE
    slab_blocks = atoms_here // TILE
    local_plane = jnp.arange(atoms_here, dtype=jnp.int32) * planes // atoms_here
    spline_value, spline_slope = slab_weights(local_plane, x_spline, extent)
    ext_pos = extended(positions, (("gx", 1),), halo_atoms)
    shift_x = jnp.concatenate(
        [
            jnp.full((halo_atoms,), -1.0 * slab_blocks, jnp.float32),
            jnp.zeros((atoms_here,), jnp.float32),
            jnp.full((halo_atoms,), 1.0 * slab_blocks, jnp.float32),
        ]
    )
    ext_pos = ext_pos.at[0].add(shift_x)
    fourier_rows = basis_rows(GRID, jnp.arange(GRID, dtype=jnp.int32))
    ky_count = GRID // rank_count
    all_freq = jnp.arange(GRID, dtype=jnp.int32)
    ky_freq = rank_index * ky_count + jnp.arange(ky_count, dtype=jnp.int32)
    full_modes, full_weights = mode_of(all_freq, GRID)
    ky_modes, ky_weights = mode_of(ky_freq, GRID)
    kernel = kernel_block(full_modes, full_weights, ky_modes, ky_weights, full_modes, full_weights)
    kernel = kernel.reshape(GRID, ky_count * GRID)
    source_rows = jnp.arange(rank_count * extent, dtype=jnp.int32)
    points = (source_rows // extent * planes - 2 + source_rows % extent) % GRID
    across = basis_rows(GRID, points)

    def reciprocal(charge):
        spectrum = forward_lines(charge, fourier_rows)
        pencils = lax.all_to_all(spectrum, "gx", split_axis=1, concat_axis=0, tiled=True)
        rows_in = pencils.shape[0]
        flat_pencils = pencils.reshape(rows_in, ky_count * GRID)
        spectral_lines = jnp.dot(across, flat_pencils, precision=EXACT) * kernel
        returned_lines = lax.dot_general(
            across, spectral_lines, (((0,), (0,)), ((), ())), precision=EXACT
        )
        returned = lax.all_to_all(
            returned_lines.reshape(rows_in, ky_count, GRID),
            "gx",
            split_axis=0,
            concat_axis=1,
            tiled=True,
        )
        return inverse_lines(returned, fourier_rows)

    def apply(vector):
        ext_vec = extended(vector, (("gx", 1),), halo_atoms)
        near_field = pair_field(positions, ext_pos, ext_vec, tile_list, tile_count)
        charge = spread_dipoles(vector, spline_value, spline_slope, yz_spline)
        far_field = gather_field(reciprocal(charge), spline_value, spline_slope, yz_spline)
        return inv_polar[None, :] * vector + far_field - near_field

    def paired(residual, precond, applied):
        return lax.psum((jnp.sum(residual * precond), jnp.sum(applied * precond)), "gx")

    dipoles = jnp.zeros_like(field)
    residual = field
    precond = field / inv_polar[None, :]
    applied = apply(precond)
    rz_now, curvature = paired(residual, precond, applied)
    step_size = rz_now / curvature
    direction = precond
    applied_dir = applied
    for sweep_index in range(ITERS):
        dipoles = dipoles + step_size * direction
        residual = residual - step_size * applied_dir
        if sweep_index + 1 < ITERS:
            precond = residual / inv_polar[None, :]
            applied = apply(precond)
            rz_next, curvature = paired(residual, precond, applied)
            beta_ratio = rz_next / rz_now
            step_size = rz_next / (curvature - beta_ratio * rz_next / step_size)
            direction = precond + beta_ratio * direction
            applied_dir = applied + beta_ratio * applied_dir
            rz_now = rz_next
    return (dipoles, residual)


F32 = jnp.float32
BF16 = jnp.bfloat16
ROWS = 8
LINES = 2 * ROWS
IN_VMEM = pl.BlockSpec(memory_space=pltpu.VMEM)
IN_SMEM = pl.BlockSpec(memory_space=pltpu.SMEM)
IN_HBM = pl.BlockSpec(memory_space=pl.ANY)
REACH = ORDER - 1
PACKED = 6
NT = (((1,), (1,)), ((), ()))


def params(flops, vmem=None):
    return dict(
        cost_estimate=pl.CostEstimate(flops=flops, bytes_accessed=4 << 20, transcendentals=0),
        compiler_params=pltpu.CompilerParams(vmem_limit_bytes=vmem) if vmem else None,
    )


def halves(x):
    high = x.astype(BF16).astype(F32)
    return high, x - high


def bdot(a, b):
    return jnp.dot(a, b, preferred_element_type=F32)


def spline_values(u):
    w = 1.0 - u
    u2, w2 = u * u, w * w
    c = 1.0 / 24.0
    return [
        c * (w2 * w2),
        c * (11.0 + u * (-12.0 + u * (-6.0 + u * (12.0 - 4.0 * u)))),
        c * (11.0 + u * (12.0 + u * (-6.0 + u * (-12.0 + 6.0 * u)))),
        c * (1.0 + u * (4.0 + u * (6.0 + u * (4.0 - 4.0 * u)))),
        c * (u2 * u2),
    ]


def spline_slopes(u):
    w = 1.0 - u
    c = 1.0 / 6.0
    return [
        -c * (w * w * w),
        c * (-3.0 + u * (-3.0 + u * (9.0 - 4.0 * u))),
        c * (3.0 + u * (-3.0 + u * (-9.0 + 6.0 * u))),
        c * (1.0 + u * (3.0 + u * (3.0 - 4.0 * u))),
        c * (u * u * u),
    ]


def block_rows(ref, row):
    return jnp.concatenate(
        [ref[row : row + 1, b * TILE : (b + 1) * TILE] for b in range(ref.shape[1] // TILE)], axis=0
    )


def pack_kernel(field_ref, ip_ref, xs_ref, yz_ref, own_ref, inv_ref, out_ref):
    parts = out_ref.shape[0]
    blocks = field_ref.shape[1] // TILE
    grid = yz_ref.shape[2]
    inv = block_rows(ip_ref, 0)
    inv_ref[...] = inv
    tiles = [block_rows(field_ref, c) / inv for c in range(3)]
    for c in range(3):
        own_ref[c * blocks : (c + 1) * blocks, :] = tiles[c]
    tiles.append(sum(float(k) * block_rows(xs_ref.at[k], 0) for k in range(1, ORDER)) - 1.5)
    line = lax.broadcasted_iota(jnp.int32, (grid, TILE), 0)
    for axis in range(2):
        spots = []
        for b in range(blocks):
            here = slice(b * TILE, (b + 1) * TILE)
            value = yz_ref[2 * axis, here, :].T
            slope = yz_ref[2 * axis + 1, here, :].T
            used = jnp.where((value != 0.0) | (slope != 0.0), 1.0, 0.0)
            first = used * (1.0 - pltpu.roll(used, 1, 0))
            start = jnp.sum(first * line.astype(F32), axis=0, keepdims=True)
            offset = (line - start.astype(jnp.int32)) & (grid - 1)
            shift = jnp.sum(value * offset.astype(F32), axis=0, keepdims=True) - 1.5
            spots.append((start - float(grid // 2)) + shift)
        tiles.append(jnp.concatenate(spots, axis=0))
    for d in range(parts):
        for i, tile in enumerate(tiles):
            out_ref[d, i * blocks : (i + 1) * blocks, :] = tile


def pack_call(field, inv_row, xs, yz, parts):
    blocks = field.shape[1] // TILE
    return pl.pallas_call(
        pack_kernel,
        in_specs=[IN_VMEM] * 4,
        out_specs=[IN_VMEM] * 3,
        out_shape=[
            jax.ShapeDtypeStruct((3 * blocks, TILE), F32),
            jax.ShapeDtypeStruct((blocks, TILE), F32),
            jax.ShapeDtypeStruct((parts, PACKED * blocks, TILE), F32),
        ],
        name="pack",
        **params(1 << 26),
    )(field, inv_row, xs, yz)


def prep_kernel(atom_ref, rows_ref, turn_ref, tab_ref, yt_ref):
    slabs = atom_ref.shape[0]
    blocks = tab_ref.shape[0] // slabs
    kept, grid = rows_ref.shape
    high, low = halves(rows_ref[...])
    twice = jnp.concatenate([high, low], axis=0).astype(BF16)
    matrix = jnp.concatenate([twice, twice], axis=1)
    packed = (LINES, TILE)
    line = lax.broadcasted_iota(jnp.int32, (grid, TILE), 0).astype(F32).astype(BF16)
    lines = [line[c * LINES : (c + 1) * LINES] for c in range(grid // LINES)]
    turn = [jnp.broadcast_to(turn_ref[:, c : c + 1], packed) for c in range(2 * ORDER)]
    half = float(grid // 2)

    def spread_row(x, b):
        return jnp.broadcast_to(x[b : b + 1], packed).astype(BF16)

    def one_slab(slab, carry):
        def located(i):
            place = atom_ref[slab, i * blocks : (i + 1) * blocks, :]
            start = jnp.floor(place)
            u = place - start
            return start, spline_values(u), spline_slopes(u)

        start, values, slopes = located(5)
        start = start.astype(jnp.int32) + grid // 2
        spots = [((start + k) & (grid - 1)).astype(F32) for k in range(ORDER)]
        pieces = [halves(x) for x in values], [halves(x) for x in slopes]
        for b in range(blocks):
            at = [spread_row(x, b) for x in spots]
            tables = []
            for part in range(2):
                columns = []
                for kind in range(2):
                    rows = [spread_row(x[part], b) for x in pieces[kind]]
                    column = []
                    for here in lines:
                        dense = jnp.zeros(packed, BF16)
                        for k in range(ORDER):
                            dense = jnp.where(here == at[k], rows[k], dense)
                        column.append(dense)
                    columns.append(jnp.concatenate(column, axis=0))
                tables.append(jnp.concatenate(columns, axis=1))
            both = bdot(matrix, jnp.concatenate(tables, axis=0))
            high, low = halves(both[:kept] + both[kept:])
            tab_ref[slab * blocks + b] = jnp.concatenate([high, low], axis=0).astype(BF16)
        start, values, slopes = located(4)
        mode, sine = turn[0], turn[1]
        for b in range(blocks):
            row = slice(b, b + 1)
            phase = mode * start[row]
            phase = phase - 2.0 * half * jnp.floor(phase * (0.5 / half) + 0.5)
            angle = phase * (jnp.pi / (4.0 * half))
            sq = angle * angle
            s = angle * (1.0 + sq * (-1.0 / 6 + sq * (1.0 / 120 + sq * (-1.0 / 5040 + sq / 362880))))
            c = 1.0 + sq * (-0.5 + sq * (1.0 / 24 + sq * (-1.0 / 720 + sq / 40320)))
            for _ in range(2):
                s, c = 2.0 * s * c, 1.0 - 2.0 * s * s
            lead = jnp.where(sine > 0.0, s, c)
            side = jnp.where(sine > 0.0, -c, s)
            for i, weights in enumerate((values, slopes)):
                even = weights[0][row] + sum(weights[k][row] * turn[1 + k] for k in range(1, ORDER))
                odd = sum(weights[k][row] * turn[ORDER + k] for k in range(1, ORDER))
                yt_ref[slab * blocks + b, i * LINES : (i + 1) * LINES, :] = lead * even - side * odd
        return carry

    lax.fori_loop(0, slabs, one_slab, 0)


def prep_call(atoms, rows, turns, blocks):
    parts = atoms.shape[0]
    kept = rows.shape[0]
    slabs = 1
    return pl.pallas_call(
        prep_kernel,
        grid=(parts // slabs,),
        in_specs=[
            pl.BlockSpec((slabs, PACKED * blocks, TILE), lambda s: (s, 0, 0)),
            pl.BlockSpec(rows.shape, lambda s: (0, 0)),
            pl.BlockSpec(turns.shape, lambda s: (0, 0)),
        ],
        out_specs=[
            pl.BlockSpec((slabs * blocks, 2 * kept, 2 * TILE), lambda s: (s, 0, 0)),
            pl.BlockSpec((slabs * blocks, 2 * LINES, TILE), lambda s: (s, 0, 0)),
        ],
        out_shape=[
            jax.ShapeDtypeStruct((parts * blocks, 2 * kept, 2 * TILE), BF16),
            jax.ShapeDtypeStruct((parts * blocks, 2 * LINES, TILE), F32),
        ],
        name="prep",
        **params(1 << 31),
    )(atoms, rows, turns)


def moment_rows(energy, v0_ref, v1_ref, v2_ref, inv_ref, pair_ref):
    ip = jnp.concatenate([inv_ref[...]] * 3, axis=0)
    v0, v1, v2 = v0_ref[...], v1_ref[...], v2_ref[...]
    d1, d2 = ip * v1, ip * v2
    terms = [v0 * (ip * v0), v0 * d1, v1 * d1, v1 * d2, v2 * d2, -(v2 * pair_ref[...])]
    rows = [jnp.sum(term, axis=0, keepdims=True) for term in terms]
    rows[5] = rows[5] + energy
    blank = jnp.zeros((ROWS - len(rows), TILE), F32)
    return jnp.concatenate(rows + [blank], axis=0)


def field_kernel(with_sums, v_ref, atom_ref, tab_hbm, yt_hbm, rows_ref, cols_ref, kern_hbm, *rest):
    if with_sums:
        *known, out_ref, tab, sem, yt_ref, yt_sem, kern_ref, kern_sem, grid_ref = rest
    else:
        out_ref, tab, sem, yt_ref, yt_sem, kern_ref, kern_sem, grid_ref = rest
    parts = out_ref.shape[0]
    grid = rows_ref.shape[0]
    blocks = tab.shape[0] // parts
    width = LINES * ORDER
    kept = grid // 2

    def fetch(s):
        part = pl.ds(s * blocks, blocks)
        return (
            pltpu.make_async_copy(yt_hbm.at[part], yt_ref.at[part], yt_sem.at[s]),
            pltpu.make_async_copy(tab_hbm.at[part], tab.at[part], sem.at[s]),
        )

    kern_copy = pltpu.make_async_copy(kern_hbm, kern_ref, kern_sem)
    for s in range(parts):
        for copy in fetch(s):
            copy.start()
    kern_copy.start()
    grid_ref[...] = jnp.zeros(grid_ref.shape, F32)

    def plane(q):
        return pl.ds(pl.multiple_of(q * LINES, LINES), LINES)

    def x_weights(s):
        u = atom_ref[s, 3 * blocks : 4 * blocks, :]
        return spline_values(u), spline_slopes(u)

    def spread(s, carry):
        for copy in fetch(s):
            copy.wait()
        value, slope = x_weights(s)
        vec = [v_ref[s, c * blocks : (c + 1) * blocks, :] for c in range(3)]
        a0 = [vec[0] * slope[k] for k in range(ORDER)]
        a1 = [vec[1] * value[k] for k in range(ORDER)]
        a2 = [vec[2] * value[k] for k in range(ORDER)]
        sums = [jnp.zeros((LINES, grid), F32) for _ in range(blocks + REACH)]
        for b in range(blocks):
            g = s * blocks + b
            row = slice(b, b + 1)
            yt, dyt = yt_ref[g, 0:LINES, :], yt_ref[g, LINES : 2 * LINES, :]
            lead = jnp.concatenate([a0[k][row] * yt + a1[k][row] * dyt for k in range(ORDER)], axis=0)
            tail = jnp.concatenate([a2[k][row] * yt for k in range(ORDER)], axis=0)
            high, low = halves(jnp.concatenate([lead, tail], axis=1))
            lhs = jnp.concatenate([high, low], axis=0).astype(BF16)
            out = lax.dot_general(lhs, tab[g], NT, preferred_element_type=F32)
            out = out[:width] + out[width:]
            for k in range(ORDER):
                sums[b + k] = sums[b + k] + out[k * LINES : (k + 1) * LINES]
        for j, tile in enumerate(sums):
            grid_ref[plane(s * blocks + j), :] += tile
        return carry

    lax.fori_loop(0, parts, spread, 0)
    side = REACH // 2
    left, right = slice(0, side * LINES), slice((side + grid) * LINES, (2 * side + grid) * LINES)
    first = slice(side * LINES, 2 * side * LINES)
    last = slice(grid * LINES, (side + grid) * LINES)
    grid_ref[last, :] += grid_ref[left, :]
    grid_ref[first, :] += grid_ref[right, :]

    def product(matrix, x):
        mh, ml = halves(matrix)
        xh, xl = halves(x)
        rhs = jnp.concatenate([xh, xl], axis=0).astype(BF16)
        mh, ml = mh.astype(BF16), ml.astype(BF16)
        return bdot(jnp.concatenate([mh, mh], axis=1), rhs) + bdot(
            jnp.concatenate([ml, ml], axis=1), rhs
        )

    def lines(j):
        return pl.ds(side * LINES + j, grid, stride=LINES)

    lower = lax.broadcasted_iota(jnp.int32, (grid, grid), 1) < kept

    def folded(j):
        x = grid_ref[lines(j), :]
        return x + pltpu.roll(x, kept, 1)

    charge = jnp.concatenate(
        [jnp.where(lower, folded(j), folded(j + ROWS)) for j in range(ROWS)], axis=1
    )
    spectrum = product(rows_ref[...], charge)
    kern_copy.wait()
    weighted = spectrum * kern_ref[...]
    potential = product(cols_ref[...], weighted)
    for j in range(ROWS):
        x = potential[:, j * grid : (j + 1) * grid]
        y = pltpu.roll(x, kept, 1)
        grid_ref[lines(j), :] = jnp.where(lower, x, y)
        grid_ref[lines(j + ROWS), :] = jnp.where(lower, y, x)
    grid_ref[left, :] = grid_ref[last, :]
    grid_ref[right, :] = grid_ref[first, :]
    if with_sums:
        energy = jnp.sum(spectrum * weighted, axis=0, keepdims=True)
        energy = sum(energy[:, j * grid : (j + 1) * grid] for j in range(ROWS))
        sums = moment_rows(energy, *known)
        for d in range(parts):
            out_ref[d, 3 * blocks :, :] = sums

    def gather(s, carry):
        value, slope = x_weights(s)
        pieces = [halves(grid_ref[plane(s * blocks + q), :]) for q in range(blocks + REACH)]
        fields = ([], [], [])
        for b in range(blocks):
            g = s * blocks + b
            row = slice(b, b + 1)
            yt, dyt = yt_ref[g, 0:LINES, :], yt_ref[g, LINES : 2 * LINES, :]
            near = pieces[b : b + ORDER]
            high = jnp.concatenate([x[0] for x in near], axis=0).astype(BF16)
            low = jnp.concatenate([x[1] for x in near], axis=0).astype(BF16)
            table = tab[g]
            out = bdot(
                jnp.concatenate([high, low], axis=1),
                jnp.concatenate([table, table[:kept], jnp.zeros_like(table[:kept])], axis=0),
            )
            tiles = [out[k * LINES : (k + 1) * LINES] for k in range(ORDER)]
            f0 = sum(slope[k][row] * tiles[k][:, :TILE] for k in range(ORDER))
            f1 = sum(value[k][row] * tiles[k][:, :TILE] for k in range(ORDER))
            f2 = sum(value[k][row] * tiles[k][:, TILE:] for k in range(ORDER))
            for i, part in enumerate((yt * f0, dyt * f1, yt * f2)):
                fields[i].append(jnp.sum(part, axis=0, keepdims=True))
        for i in range(3):
            out_ref[s, i * blocks : (i + 1) * blocks, :] = jnp.concatenate(fields[i], axis=0)
        return carry

    lax.fori_loop(0, parts, gather, 0)


def field_call(vec, atoms, table, yt, rows, cols, kern, known=()):
    parts = vec.shape[0]
    grid = rows.shape[0]
    blocks = yt.shape[0] // parts
    args = [vec, atoms, table, yt, rows, cols, kern]
    specs = [IN_VMEM, IN_VMEM, IN_HBM, IN_HBM, IN_VMEM, IN_VMEM, IN_HBM]
    out_rows = 3 * blocks
    if known:
        args.extend(known)
        specs.extend([IN_VMEM] * len(known))
        out_rows += ROWS
    return pl.pallas_call(
        lambda *refs: field_kernel(len(known) > 0, *refs),
        in_specs=specs,
        out_specs=IN_VMEM,
        out_shape=jax.ShapeDtypeStruct((parts, out_rows, TILE), F32),
        scratch_shapes=[
            pltpu.VMEM(table.shape, BF16),
            pltpu.SemaphoreType.DMA((parts,)),
            pltpu.VMEM(yt.shape, F32),
            pltpu.SemaphoreType.DMA((parts,)),
            pltpu.VMEM(kern.shape, F32),
            pltpu.SemaphoreType.DMA(()),
            pltpu.VMEM(((grid + REACH) * LINES, grid), F32),
        ],
        name="field",
        **params(1 << 31, 56 << 20),
    )(*args)


def pair_kernel(list_ref, count_ref, rank_ref, left_ref, pos_ref, right_ref, col_ref, vec_ref, out_ref, acc_ref, near_ref):
    blocks = pos_ref.shape[1] // TILE
    ext = blocks + 2 * HALO_BLK
    total = vec_ref.shape[0] * blocks
    chunk = TILE // 2
    shift = 1.0 * blocks
    for c in range(3):
        for j in range(ext):
            if j < HALO_BLK:
                row = left_ref[c : c + 1, j * TILE : (j + 1) * TILE] - (shift if c == 0 else 0.0)
            elif j < HALO_BLK + blocks:
                i = j - HALO_BLK
                row = pos_ref[c : c + 1, i * TILE : (i + 1) * TILE]
            else:
                i = j - HALO_BLK - blocks
                row = right_ref[c : c + 1, i * TILE : (i + 1) * TILE] + (shift if c == 0 else 0.0)
            near_ref[j, c : c + 1, :] = row
            g = lax.rem(rank_ref[0] * blocks + (j - HALO_BLK) + total, total)
            src = lax.div(g, blocks)
            near_ref[j, 3 + c : 4 + c, :] = vec_ref[src, pl.ds(c * blocks + g - src * blocks, 1), :]

    shape = (chunk, TILE)
    ahead = lax.broadcasted_iota(jnp.int32, shape, 1) - lax.broadcasted_iota(jnp.int32, shape, 0)

    def one_block(b, carry):
        for c in range(TILE // chunk):
            home = col_ref[pl.ds(pl.multiple_of(b * TILE + c * chunk, chunk), chunk), :]
            hx = jnp.broadcast_to(home[:, 0:1], shape)
            hy = jnp.broadcast_to(home[:, 1:2], shape)
            hz = jnp.broadcast_to(home[:, 2:3], shape)

            def one_tile(k, sums):
                sx, sy, sz = sums
                j = list_ref[b, k]
                near = near_ref[j]
                dx, dy, dz = hx - near[0:1], hy - near[1:2], hz - near[2:3]
                vx, vy, vz = near[3:4], near[4:5], near[5:6]
                inverse = lax.rsqrt(dx * dx + dy * dy + dz * dz + 1.0)
                square = inverse * inverse
                itself = ahead == c * chunk - (j - b - HALO_BLK) * TILE
                third = jnp.where(itself, 0.0, inverse * square)
                fifth = (third * square) * (3.0 * (dx * vx + dy * vy + dz * vz))
                return (
                    sx + (third * vx - fifth * dx),
                    sy + (third * vy - fifth * dy),
                    sz + (third * vz - fifth * dz),
                )

            zero = jnp.zeros(shape, F32)
            sums = lax.fori_loop(0, count_ref[b], one_tile, (zero, zero, zero))
            for i in range(3):
                acc_ref[i, c * chunk : (c + 1) * chunk, :] = sums[i]
        for i in range(3):
            out_ref[pl.ds(i * blocks + b, 1), :] = PAIR_C * jnp.sum(acc_ref[i].T, axis=0, keepdims=True)
        return carry

    lax.fori_loop(0, blocks, one_block, 0)


def pair_call(tiles, counts, rank, left, pos, right, cols, vec):
    blocks = pos.shape[1] // TILE
    return pl.pallas_call(
        pair_kernel,
        in_specs=[IN_SMEM] * 3 + [IN_VMEM] * 5,
        out_specs=IN_VMEM,
        out_shape=jax.ShapeDtypeStruct((3 * blocks, TILE), F32),
        scratch_shapes=[
            pltpu.VMEM((3, TILE, TILE), F32),
            pltpu.VMEM((blocks + 2 * HALO_BLK, ROWS, TILE), F32),
        ],
        name="pair",
        **params(1 << 30),
    )(tiles, counts, rank, left, pos, right, cols, vec)


def update_kernel(ret_ref, pair_ref, inv_ref, own_ref, out_ref):
    blocks = inv_ref.shape[0]
    far = jnp.sum(ret_ref[...], axis=0) - pair_ref[...]
    inv = inv_ref[...]
    vec = jnp.concatenate([far[c * blocks : (c + 1) * blocks] / inv for c in range(3)], axis=0)
    own_ref[...] = vec
    for d in range(out_ref.shape[0]):
        out_ref[d] = vec


def update_call(returned, pair, inv):
    parts = returned.shape[0]
    return pl.pallas_call(
        update_kernel,
        in_specs=[IN_VMEM] * 3,
        out_specs=[IN_VMEM] * 2,
        out_shape=[
            jax.ShapeDtypeStruct(pair.shape, F32),
            jax.ShapeDtypeStruct((parts,) + pair.shape, F32),
        ],
        name="update",
        **params(1 << 24),
    )(returned, pair, inv)


def finish_kernel(ret_ref, pair_ref, v0_ref, v1_ref, v2_ref, inv_ref, dip_ref, res_ref):
    blocks = inv_ref.shape[0]
    summed = jnp.sum(ret_ref[...], axis=0)
    total = jnp.sum(summed[3 * blocks :], axis=1, keepdims=True)
    h = summed[: 3 * blocks] - pair_ref[...]
    m = [total[k : k + 1, 0:1] for k in range(6)]
    s = [lax.rsqrt(m[2 * i]) for i in range(3)]
    g = [[m[i + j] * s[i] * s[j] for j in range(3)] for i in range(3)]
    b = [-m[i + 3] * s[i] for i in range(3)]
    l10 = g[1][0] / g[0][0]
    l20 = g[2][0] / g[0][0]
    p11 = g[1][1] - l10 * g[0][1]
    p12 = g[1][2] - l10 * g[0][2]
    l21 = p12 / p11
    p22 = g[2][2] - l20 * g[0][2] - l21 * p12
    b1 = b[1] - l10 * b[0]
    b2 = b[2] - l20 * b[0] - l21 * b1
    y2 = b2 / p22
    y1 = (b1 - p12 * y2) / p11
    y0 = (b[0] - g[0][1] * y1 - g[0][2] * y2) / g[0][0]
    a0, a1, a2 = s[0] * y0, s[1] * y1, s[2] * y2
    scale = 1.0 / (a0 - a1 + a2 - 1.0)
    a0, a1, a2, a3 = a0 * scale, a1 * scale, a2 * scale, scale
    c2 = -a3
    c1 = a3 - a2
    c0 = a2 - a3 - a1
    ip = jnp.concatenate([inv_ref[...]] * 3, axis=0)
    v0, v1, v2 = v0_ref[...], v1_ref[...], v2_ref[...]
    dip = c0 * v0 + c1 * v1 + c2 * v2
    res = ip * (a0 * v0 + a1 * v1 + a2 * v2) + a3 * h
    for c in range(3):
        for b in range(blocks):
            row = slice(c * blocks + b, c * blocks + b + 1)
            here = slice(b * TILE, (b + 1) * TILE)
            dip_ref[c : c + 1, here] = dip[row]
            res_ref[c : c + 1, here] = res[row]


def finish_call(returned, pair, vectors, inv):
    atoms = inv.shape[0] * TILE
    return pl.pallas_call(
        finish_kernel,
        in_specs=[IN_VMEM] * 6,
        out_specs=[IN_VMEM] * 2,
        out_shape=[jax.ShapeDtypeStruct((3, atoms), F32)] * 2,
        name="finish",
        **params(1 << 24),
    )(returned, pair, *vectors, inv)


def fourier_matrix(size):
    freq = np.arange(size)
    mode = np.where(freq <= size // 2, freq, freq - size // 2)
    angle = (mode[:, None] * np.arange(size)[None, :] % size) * (2.0 * np.pi / size)
    rows = np.where((freq <= size // 2)[:, None], np.cos(angle), np.sin(angle))
    return rows.astype(np.float32)


def kernel_lines(x_axis, y_axis, z_axis):
    mode_sq = x_axis[0] * x_axis[0] + y_axis[0] * y_axis[0] + z_axis[0] * z_axis[0]
    safe_sq = jnp.where(mode_sq > 0, mode_sq, 1.0)
    green = jnp.where(mode_sq > 0, RECIP_C * jnp.exp(-DAMP * safe_sq) / safe_sq, 0.0)
    return green * x_axis[1] * y_axis[1] * z_axis[1]


def swap(x):
    return lax.all_to_all(x, "gx", split_axis=0, concat_axis=0, tiled=True)


def per_device_modes(positions, field, inv_polar, x_spline, yz_spline, tile_list, tile_count):
    parts = lax.axis_size("gx")
    rank = lax.axis_index("gx")
    atoms = positions.shape[1]
    halo = HALO_BLK * TILE
    blocks = atoms // TILE
    up = [(i, (i + 1) % parts) for i in range(parts)]
    down = [(j, i) for i, j in up]

    own, inv, packed = pack_call(
        field, inv_polar[None, :], x_spline.transpose(1, 0, 2), yz_spline, parts
    )
    everyone = swap(packed)
    places, everyone = lax.optimization_barrier((positions, everyone))
    left = lax.ppermute(places[:, atoms - halo :], "gx", up)
    right = lax.ppermute(places[:, :halo], "gx", down)
    home_cols = jnp.pad(positions, ((0, ROWS - 3), (0, 0))).T

    matrix = fourier_matrix(GRID)
    rows, cols = jnp.asarray(matrix), jnp.asarray(matrix.T)
    all_freq = jnp.arange(GRID, dtype=jnp.int32)
    kept = GRID // 2
    ky_freq = rank // 2 * LINES + jnp.arange(LINES, dtype=jnp.int32)
    kz_freq = rank % 2 * kept + jnp.arange(kept, dtype=jnp.int32)
    z_rows = lax.dynamic_slice_in_dim(rows, rank % 2 * kept, kept, 0)
    full_modes, full_weights = mode_of(all_freq, GRID)
    ky_modes, ky_weights = mode_of(ky_freq, GRID)
    kz_modes, kz_weights = mode_of(kz_freq, GRID)

    def paired_lines(x):
        x = x.reshape(1, 2, ROWS, 1)
        x = jnp.broadcast_to(x.transpose(0, 2, 1, 3), (1, ROWS, 2, kept))
        return x.reshape(1, ROWS * GRID)

    def repeated(x):
        return jnp.tile(x[None, :], (1, LINES))

    kern = kernel_lines(
        (full_modes[:, None], full_weights[:, None]),
        (paired_lines(ky_modes), paired_lines(ky_weights)),
        (repeated(kz_modes), repeated(kz_weights)),
    )
    steps = jnp.arange(1, ORDER).astype(F32)
    angle = steps[:, None] * ky_modes[None, :] * (2.0 * jnp.pi / GRID)
    sine = (ky_freq > GRID // 2).astype(F32)
    turns = jnp.concatenate([ky_modes[None], sine[None], jnp.cos(angle), jnp.sin(angle)])
    turns = jnp.pad(turns.T, ((0, 0), (0, TILE - turns.shape[0])))

    table, yt = prep_call(everyone, z_rows, turns, blocks)
    vec, vectors = everyone, [own]
    rank_id = rank[None].astype(jnp.int32)
    for step in range(ITERS):
        last = step + 1 == ITERS
        pair = pair_call(tile_list, tile_count, rank_id, left, positions, right, home_cols, vec)
        known = (*vectors, inv, pair) if last else ()
        returned = swap(field_call(vec, everyone, table, yt, rows, cols, kern, known))
        if not last:
            own, packed = update_call(returned, pair, inv)
            vectors.append(own)
            vec = swap(packed)
    dipoles, residual = finish_call(returned, pair, vectors, inv)
    return (dipoles, residual)


def per_device(positions, *others):
    parts = lax.axis_size("gx")
    atoms = positions.shape[1]
    planes = GRID // parts
    modes = (
        parts * ROWS == GRID
        and atoms == planes * TILE
        and planes == ROWS
        and atoms >= HALO_BLK * TILE
        and ORDER == 5
        and ITERS == 3
    )
    run = per_device_modes if modes else per_device_general
    return run(positions, *others)


def solution(mesh):
    placed = (
        P(None, ("rep", "gx")),
        P(None, ("rep", "gx")),
        P(("rep", "gx")),
        P(None, None, ("rep", "gx")),
        P(None, ("rep", "gx"), None),
        P(("rep", "gx"), None),
        P(("rep", "gx")),
    )
    return jax.shard_map(
        per_device,
        mesh=mesh,
        in_specs=placed,
        out_specs=(P(None, ("rep", "gx")), P(None, ("rep", "gx"))),
        check_vma=False,
    )
```

```python
import jax
import numpy as np
import jax.numpy as jnp
from jax import lax
from jax.experimental import pallas as pl
from jax.experimental.pallas import tpu as pltpu
from jax.sharding import PartitionSpec as P

GRID = 128
ORDER = 5
TILE = 128
HALO_BLK = 3
ITERS = 3


PAIR_C = 0.025
RECIP_C = 8192.0
DAMP = 0.0008
EXACT = lax.Precision.HIGHEST


def extended(x, sides, width):
    for axis, dim in sides:
        devices, length = (lax.axis_size(axis), x.shape[dim])
        up = [(i, (i + 1) % devices) for i in range(devices)]
        down = [(j, i) for i, j in up]
        last = lax.slice_in_dim(x, length - width, length, axis=dim)
        first = lax.slice_in_dim(x, 0, width, axis=dim)
        before = lax.ppermute(last, axis, up)
        after = lax.ppermute(first, axis, down)
        x = jnp.concatenate([before, x, after], axis=dim)
    return x


def pair_field(home_pos, ext_pos, ext_vec, tile_rows, live_counts):
    slab_blocks = home_pos.shape[1] // TILE
    ext_blocks = ext_pos.shape[1] // TILE
    home_blocks = home_pos.reshape(3, slab_blocks, TILE).transpose(1, 0, 2)
    pos_blocks = ext_pos.reshape(3, ext_blocks, TILE)
    vec_blocks = ext_vec.reshape(3, ext_blocks, TILE)
    slot_index = jnp.arange(tile_rows.shape[1], dtype=jnp.int32)
    self_pair = jnp.eye(TILE, dtype=bool)

    def one_block(carried, scan_item):
        home_block, tile_row, live_count, block_index = scan_item
        near_pos = jnp.take(pos_blocks, tile_row, axis=1)
        near_vec = jnp.take(vec_blocks, tile_row, axis=1)
        offsets = home_block[:, None, :, None] - near_pos[:, :, None, :]
        distance_sq = jnp.sum(offsets * offsets, axis=0) + 1.0
        inverse = lax.rsqrt(distance_sq)
        third_power = inverse * inverse * inverse
        fifth_power = third_power * inverse * inverse
        same_block = (tile_row == block_index + HALO_BLK)[:, None, None]
        live_mask = (slot_index < live_count)[:, None, None] & ~(same_block & self_pair[None])
        third_power = jnp.where(live_mask, third_power, 0.0)
        fifth_power = jnp.where(live_mask, fifth_power, 0.0)
        projection = jnp.sum(offsets * near_vec[:, :, None, :], axis=0)
        field_sum = jnp.sum(
            third_power[None] * near_vec[:, :, None, :]
            - 3.0 * (fifth_power * projection)[None] * offsets,
            axis=(1, 3),
        )
        return (carried, PAIR_C * field_sum)

    block_ids = jnp.arange(slab_blocks, dtype=jnp.int32)
    _, blocks_out = lax.scan(
        one_block, jnp.zeros((), jnp.float32), (home_blocks, tile_rows, live_counts, block_ids)
    )
    return blocks_out.transpose(1, 0, 2).reshape(3, slab_blocks * TILE)


def slab_weights(local_plane, x_spline, planes):
    spline_steps = jnp.arange(ORDER, dtype=jnp.int32)
    plane_index = jnp.arange(planes, dtype=jnp.int32)
    matches = local_plane[None, :, None] + spline_steps[:, None, None] == plane_index[None, None, :]
    spline_value = jnp.sum(jnp.where(matches, x_spline[0][:, :, None], 0.0), axis=0)
    spline_slope = jnp.sum(jnp.where(matches, x_spline[1][:, :, None], 0.0), axis=0)
    return (spline_value, spline_slope)


def spread_dipoles(vector, spline_value, spline_slope, yz_spline):
    atoms_here = spline_value.shape[0]
    planes = spline_value.shape[1]
    grid_lines = yz_spline.shape[2]
    lead_terms = (vector[0][:, None] * spline_slope)[:, :, None] * yz_spline[0][:, None, :]
    lead_terms = (
        lead_terms + (vector[1][:, None] * spline_value)[:, :, None] * yz_spline[1][:, None, :]
    )
    tail_terms = (vector[2][:, None] * spline_value)[:, :, None] * yz_spline[0][:, None, :]
    contract = (((0,), (0,)), ((), ()))
    charge = lax.dot_general(
        lead_terms.reshape(atoms_here, planes * grid_lines), yz_spline[2], contract, precision=EXACT
    )
    charge = charge + lax.dot_general(
        tail_terms.reshape(atoms_here, planes * grid_lines), yz_spline[3], contract, precision=EXACT
    )
    return charge.reshape(planes, grid_lines, grid_lines)


def gather_field(potential, spline_value, spline_slope, yz_spline):
    planes = potential.shape[0]
    grid_lines = potential.shape[1]
    atoms_here = spline_value.shape[0]
    flat_grid = potential.reshape(planes * grid_lines, grid_lines)
    contract = (((1,), (1,)), ((), ()))
    plain_sum = lax.dot_general(yz_spline[2], flat_grid, contract, precision=EXACT).reshape(
        atoms_here, planes, grid_lines
    )
    tilted_sum = lax.dot_general(yz_spline[3], flat_grid, contract, precision=EXACT).reshape(
        atoms_here, planes, grid_lines
    )
    first_comp = jnp.sum(
        spline_slope[:, :, None] * yz_spline[0][:, None, :] * plain_sum, axis=(1, 2)
    )
    second_comp = jnp.sum(
        spline_value[:, :, None] * yz_spline[1][:, None, :] * plain_sum, axis=(1, 2)
    )
    third_comp = jnp.sum(
        spline_value[:, :, None] * yz_spline[0][:, None, :] * tilted_sum, axis=(1, 2)
    )
    return jnp.stack([first_comp, second_comp, third_comp])


def mode_of(freq, size):
    half_size = size // 2
    mode_num = jnp.where(freq <= half_size, freq, freq - half_size)
    weight = jnp.where((freq == 0) | (freq == half_size), 1.0 / size, 2.0 / size)
    return (mode_num.astype(jnp.float32), weight.astype(jnp.float32))


def basis_rows(size, points):
    freq = jnp.arange(size, dtype=jnp.int32)
    half_size = size // 2
    mode_num = jnp.where(freq <= half_size, freq, freq - half_size)
    phase = mode_num[:, None] * points[None, :] % size
    angle = phase.astype(jnp.float32) * (2.0 * jnp.pi / size)
    return jnp.where((freq <= half_size)[:, None], jnp.cos(angle), jnp.sin(angle))


def kernel_block(x_modes, x_weights, y_modes, y_weights, z_modes, z_weights):
    mode_sq = (
        x_modes[:, None, None] * x_modes[:, None, None]
        + y_modes[None, :, None] * y_modes[None, :, None]
        + z_modes[None, None, :] * z_modes[None, None, :]
    )
    safe_sq = jnp.where(mode_sq > 0, mode_sq, 1.0)
    green = jnp.where(mode_sq > 0, RECIP_C * jnp.exp(-DAMP * safe_sq) / safe_sq, 0.0)
    return green * x_weights[:, None, None] * y_weights[None, :, None] * z_weights[None, None, :]


def forward_lines(charge, fourier_rows):
    along_z = jnp.einsum("pyz,kz->pyk", charge, fourier_rows, precision=EXACT)
    return jnp.einsum("jy,pyk->pjk", fourier_rows, along_z, precision=EXACT)


def inverse_lines(spectrum, fourier_rows):
    along_z = jnp.einsum("pjk,kz->pjz", spectrum, fourier_rows, precision=EXACT)
    return jnp.einsum("jy,pjz->pyz", fourier_rows, along_z, precision=EXACT)


def per_device_general(positions, field, inv_polar, x_spline, yz_spline, tile_list, tile_count):
    rank_count = lax.axis_size("gx")
    rank_index = lax.axis_index("gx")
    atoms_here = positions.shape[1]
    planes = GRID // rank_count
    extent = planes + 4
    halo_atoms = HALO_BLK * TILE
    slab_blocks = atoms_here // TILE
    local_plane = jnp.arange(atoms_here, dtype=jnp.int32) * planes // atoms_here
    spline_value, spline_slope = slab_weights(local_plane, x_spline, extent)
    ext_pos = extended(positions, (("gx", 1),), halo_atoms)
    shift_x = jnp.concatenate(
        [
            jnp.full((halo_atoms,), -1.0 * slab_blocks, jnp.float32),
            jnp.zeros((atoms_here,), jnp.float32),
            jnp.full((halo_atoms,), 1.0 * slab_blocks, jnp.float32),
        ]
    )
    ext_pos = ext_pos.at[0].add(shift_x)
    fourier_rows = basis_rows(GRID, jnp.arange(GRID, dtype=jnp.int32))
    ky_count = GRID // rank_count
    all_freq = jnp.arange(GRID, dtype=jnp.int32)
    ky_freq = rank_index * ky_count + jnp.arange(ky_count, dtype=jnp.int32)
    full_modes, full_weights = mode_of(all_freq, GRID)
    ky_modes, ky_weights = mode_of(ky_freq, GRID)
    kernel = kernel_block(full_modes, full_weights, ky_modes, ky_weights, full_modes, full_weights)
    kernel = kernel.reshape(GRID, ky_count * GRID)
    source_rows = jnp.arange(rank_count * extent, dtype=jnp.int32)
    points = (source_rows // extent * planes - 2 + source_rows % extent) % GRID
    across = basis_rows(GRID, points)

    def reciprocal(charge):
        spectrum = forward_lines(charge, fourier_rows)
        pencils = lax.all_to_all(spectrum, "gx", split_axis=1, concat_axis=0, tiled=True)
        rows_in = pencils.shape[0]
        flat_pencils = pencils.reshape(rows_in, ky_count * GRID)
        spectral_lines = jnp.dot(across, flat_pencils, precision=EXACT) * kernel
        returned_lines = lax.dot_general(
            across, spectral_lines, (((0,), (0,)), ((), ())), precision=EXACT
        )
        returned = lax.all_to_all(
            returned_lines.reshape(rows_in, ky_count, GRID),
            "gx",
            split_axis=0,
            concat_axis=1,
            tiled=True,
        )
        return inverse_lines(returned, fourier_rows)

    def apply(vector):
        ext_vec = extended(vector, (("gx", 1),), halo_atoms)
        near_field = pair_field(positions, ext_pos, ext_vec, tile_list, tile_count)
        charge = spread_dipoles(vector, spline_value, spline_slope, yz_spline)
        far_field = gather_field(reciprocal(charge), spline_value, spline_slope, yz_spline)
        return inv_polar[None, :] * vector + far_field - near_field

    def paired(residual, precond, applied):
        return lax.psum((jnp.sum(residual * precond), jnp.sum(applied * precond)), "gx")

    dipoles = jnp.zeros_like(field)
    residual = field
    precond = field / inv_polar[None, :]
    applied = apply(precond)
    rz_now, curvature = paired(residual, precond, applied)
    step_size = rz_now / curvature
    direction = precond
    applied_dir = applied
    for sweep_index in range(ITERS):
        dipoles = dipoles + step_size * direction
        residual = residual - step_size * applied_dir
        if sweep_index + 1 < ITERS:
            precond = residual / inv_polar[None, :]
            applied = apply(precond)
            rz_next, curvature = paired(residual, precond, applied)
            beta_ratio = rz_next / rz_now
            step_size = rz_next / (curvature - beta_ratio * rz_next / step_size)
            direction = precond + beta_ratio * direction
            applied_dir = applied + beta_ratio * applied_dir
            rz_now = rz_next
    return (dipoles, residual)


F32 = jnp.float32
BF16 = jnp.bfloat16
ROWS = 8
LINES = 2 * ROWS
IN_VMEM = pl.BlockSpec(memory_space=pltpu.VMEM)
IN_SMEM = pl.BlockSpec(memory_space=pltpu.SMEM)
IN_HBM = pl.BlockSpec(memory_space=pl.ANY)
REACH = ORDER - 1
SPAN = 2 * HALO_BLK + 1
PACKED = 6
NT = (((1,), (1,)), ((), ()))


def params(flops, vmem=None):
    return dict(
        cost_estimate=pl.CostEstimate(flops=flops, bytes_accessed=4 << 20, transcendentals=0),
        compiler_params=pltpu.CompilerParams(vmem_limit_bytes=vmem) if vmem else None,
    )


def halves(x):
    high = x.astype(BF16).astype(F32)
    return high, x - high


def bdot(a, b):
    return jnp.dot(a, b, preferred_element_type=F32)


def spline_values(u):
    w = 1.0 - u
    u2, w2 = u * u, w * w
    c = 1.0 / 24.0
    return [
        c * (w2 * w2),
        c * (11.0 + u * (-12.0 + u * (-6.0 + u * (12.0 - 4.0 * u)))),
        c * (11.0 + u * (12.0 + u * (-6.0 + u * (-12.0 + 6.0 * u)))),
        c * (1.0 + u * (4.0 + u * (6.0 + u * (4.0 - 4.0 * u)))),
        c * (u2 * u2),
    ]


def spline_slopes(u):
    w = 1.0 - u
    c = 1.0 / 6.0
    return [
        -c * (w * w * w),
        c * (-3.0 + u * (-3.0 + u * (9.0 - 4.0 * u))),
        c * (3.0 + u * (-3.0 + u * (-9.0 + 6.0 * u))),
        c * (1.0 + u * (3.0 + u * (3.0 - 4.0 * u))),
        c * (u * u * u),
    ]


def block_rows(ref, row):
    return jnp.concatenate(
        [ref[row : row + 1, b * TILE : (b + 1) * TILE] for b in range(ref.shape[1] // TILE)], axis=0
    )


def pack_kernel(field_ref, ip_ref, xs_ref, yz_ref, own_ref, inv_ref, out_ref):
    parts = out_ref.shape[0]
    blocks = field_ref.shape[1] // TILE
    grid = yz_ref.shape[2]
    inv = block_rows(ip_ref, 0)
    inv_ref[...] = inv
    tiles = [block_rows(field_ref, c) / inv for c in range(3)]
    for c in range(3):
        own_ref[c * blocks : (c + 1) * blocks, :] = tiles[c]
    tiles.append(sum(float(k) * block_rows(xs_ref.at[k], 0) for k in range(1, ORDER)) - 1.5)
    line = lax.broadcasted_iota(jnp.int32, (grid, TILE), 0)
    for axis in range(2):
        spots = []
        for b in range(blocks):
            here = slice(b * TILE, (b + 1) * TILE)
            value = yz_ref[2 * axis, here, :].T
            slope = yz_ref[2 * axis + 1, here, :].T
            used = jnp.where((value != 0.0) | (slope != 0.0), 1.0, 0.0)
            first = used * (1.0 - pltpu.roll(used, 1, 0))
            start = jnp.sum(first * line.astype(F32), axis=0, keepdims=True)
            offset = (line - start.astype(jnp.int32)) & (grid - 1)
            shift = jnp.sum(value * offset.astype(F32), axis=0, keepdims=True) - 1.5
            spots.append((start - float(grid // 2)) + shift)
        tiles.append(jnp.concatenate(spots, axis=0))
    for d in range(parts):
        for i, tile in enumerate(tiles):
            out_ref[d, i * blocks : (i + 1) * blocks, :] = tile


def pack_call(field, inv_row, xs, yz, parts):
    blocks = field.shape[1] // TILE
    return pl.pallas_call(
        pack_kernel,
        in_specs=[IN_VMEM] * 4,
        out_specs=[IN_VMEM] * 3,
        out_shape=[
            jax.ShapeDtypeStruct((3 * blocks, TILE), F32),
            jax.ShapeDtypeStruct((blocks, TILE), F32),
            jax.ShapeDtypeStruct((parts, PACKED * blocks, TILE), F32),
        ],
        name="pack",
        **params(1 << 26),
    )(field, inv_row, xs, yz)


def table_maker(atom_ref, rows_ref, turn_ref, tab_ref, yt_ref):
    slabs = atom_ref.shape[0]
    blocks = tab_ref.shape[0] // slabs
    kept, grid = rows_ref.shape
    high, low = halves(rows_ref[...])
    twice = jnp.concatenate([high, low], axis=0).astype(BF16)
    matrix = jnp.concatenate([twice, twice], axis=1)
    packed = (LINES, TILE)
    line = lax.broadcasted_iota(jnp.int32, (grid, TILE), 0).astype(F32).astype(BF16)
    lines = [line[c * LINES : (c + 1) * LINES] for c in range(grid // LINES)]
    turn = [jnp.broadcast_to(turn_ref[:, c : c + 1], packed) for c in range(2 * ORDER)]
    half = float(grid // 2)

    def spread_row(x, b):
        return jnp.broadcast_to(x[b : b + 1], packed).astype(BF16)

    def one_slab(slab):
        def located(i):
            place = atom_ref[slab, i * blocks : (i + 1) * blocks, :]
            start = jnp.floor(place)
            u = place - start
            return start, spline_values(u), spline_slopes(u)

        start, values, slopes = located(5)
        start = start.astype(jnp.int32) + grid // 2
        spots = [((start + k) & (grid - 1)).astype(F32) for k in range(ORDER)]
        pieces = [halves(x) for x in values], [halves(x) for x in slopes]
        for b in range(blocks):
            at = [spread_row(x, b) for x in spots]
            tables = []
            for part in range(2):
                columns = []
                for kind in range(2):
                    rows = [spread_row(x[part], b) for x in pieces[kind]]
                    column = []
                    for here in lines:
                        dense = jnp.zeros(packed, BF16)
                        for k in range(ORDER):
                            dense = jnp.where(here == at[k], rows[k], dense)
                        column.append(dense)
                    columns.append(jnp.concatenate(column, axis=0))
                tables.append(jnp.concatenate(columns, axis=1))
            both = bdot(matrix, jnp.concatenate(tables, axis=0))
            high, low = halves(both[:kept] + both[kept:])
            tab_ref[slab * blocks + b] = jnp.concatenate([high, low], axis=0).astype(BF16)
        start, values, slopes = located(4)
        mode, sine = turn[0], turn[1]
        for b in range(blocks):
            row = slice(b, b + 1)
            phase = mode * start[row]
            phase = phase - 2.0 * half * jnp.floor(phase * (0.5 / half) + 0.5)
            angle = phase * (jnp.pi / (4.0 * half))
            sq = angle * angle
            s = angle * (1.0 + sq * (-1.0 / 6 + sq * (1.0 / 120 + sq * (-1.0 / 5040 + sq / 362880))))
            c = 1.0 + sq * (-0.5 + sq * (1.0 / 24 + sq * (-1.0 / 720 + sq / 40320)))
            for _ in range(2):
                s, c = 2.0 * s * c, 1.0 - 2.0 * s * s
            lead = jnp.where(sine > 0.0, s, c)
            side = jnp.where(sine > 0.0, -c, s)
            for i, weights in enumerate((values, slopes)):
                even = weights[0][row] + sum(weights[k][row] * turn[1 + k] for k in range(1, ORDER))
                odd = sum(weights[k][row] * turn[ORDER + k] for k in range(1, ORDER))
                yt_ref[slab * blocks + b, i * LINES : (i + 1) * LINES, :] = lead * even - side * odd

    return one_slab


def near_tiles(refs, vec_ref, near_ref, col_ref):
    rank_ref, left_ref, pos_ref, right_ref = refs
    blocks = pos_ref.shape[1] // TILE
    total = vec_ref.shape[0] * blocks
    shift = 1.0 * blocks
    for j in range(blocks + 2 * HALO_BLK):
        i = j - HALO_BLK
        g = rank_ref[0] * blocks + i
        if i < 0:
            g = jnp.where(g < 0, g + total, g)
            source, i, move = left_ref, j, -shift
        elif i < blocks:
            source, move = pos_ref, 0.0
        else:
            g = jnp.where(g >= total, g - total, g)
            source, i, move = right_ref, i - blocks, shift
        rows = source[:, i * TILE : (i + 1) * TILE]
        near_ref[j, 0:1, :] = rows[0:1] + move
        near_ref[j, 1:3, :] = rows[1:3]
        src = lax.shift_right_logical(g, 3)
        block = g & (ROWS - 1)
        for c in range(3):
            near_ref[j, 3 + c : 4 + c, :] = vec_ref[src, pl.ds(c * blocks + block, 1), :]
        near_ref[j, 6:8, :] = jnp.zeros((2, TILE), F32)
    for b in range(blocks):
        col_ref[b * TILE : (b + 1) * TILE, :] = near_ref[HALO_BLK + b].T


def pair_part(part, size, wts_ref, near_ref, col_ref, sum_ref):
    first = part * size
    b = lax.shift_right_logical(first, 7)
    chunk = min(size, 32)
    shape = (chunk, TILE)
    lane = lax.broadcasted_iota(jnp.int32, shape, 1)
    ahead = lane - lax.broadcasted_iota(jnp.int32, shape, 0)
    for c in range(size // chunk):
        start = pl.multiple_of(first + c * chunk, chunk)
        home = col_ref[pl.ds(start, chunk), :]
        hx = jnp.broadcast_to(home[:, 0:1], shape)
        hy = jnp.broadcast_to(home[:, 1:2], shape)
        hz = jnp.broadcast_to(home[:, 2:3], shape)
        sx = sy = sz = jnp.zeros(shape, F32)
        for e in range(SPAN):
            near = near_ref[b + e]
            dx, dy, dz = hx - near[0:1], hy - near[1:2], hz - near[2:3]
            vx, vy, vz = near[3:4], near[4:5], near[5:6]
            inverse = lax.rsqrt(dx * dx + dy * dy + dz * dz + 1.0)
            square = inverse * inverse
            third = wts_ref[b * SPAN + e] * (inverse * square)
            if e == HALO_BLK:
                third = jnp.where(ahead == start - b * TILE, 0.0, third)
            fifth = (third * square) * (3.0 * (dx * vx + dy * vy + dz * vz))
            sx = sx + (third * vx - fifth * dx)
            sy = sy + (third * vy - fifth * dy)
            sz = sz + (third * vz - fifth * dz)
        sums = [jnp.sum(x, axis=1, keepdims=True) for x in (sx, sy, sz)]
        both = jnp.where(lane == 0, sums[0], jnp.where(lane == 1, sums[1], sums[2]))
        sum_ref[pl.ds(start, chunk), :] = both[:, :ROWS]


def moment_rows(energy, v0_ref, v1_ref, v2_ref, inv_ref, pair_ref):
    ip = jnp.concatenate([inv_ref[...]] * 3, axis=0)
    v0, v1, v2 = v0_ref[...], v1_ref[...], v2_ref[...]
    d1, d2 = ip * v1, ip * v2
    terms = [v0 * (ip * v0), v0 * d1, v1 * d1, v1 * d2, v2 * d2, -(v2 * pair_ref[...])]
    rows = [jnp.sum(term, axis=0, keepdims=True) for term in terms]
    rows[5] = rows[5] + energy
    blank = jnp.zeros((ROWS - len(rows), TILE), F32)
    return jnp.concatenate(rows + [blank], axis=0)


def field_kernel(mode, *refs):
    making, closing = mode
    v_ref, rows_ref, cols_ref, kern_hbm, *refs = refs
    if making:
        z_ref, turn_ref, out_ref, tab_hbm, yt_hbm, *refs = refs
        atom_ref = v_ref
    elif closing:
        atom_ref, tab_hbm, yt_hbm, wts_ref, *refs = refs
        places, known, refs = refs[:4], refs[4:8], refs[8:]
        out_ref, pair_ref, *refs = refs
    else:
        atom_ref, tab_hbm, yt_hbm, out_ref, *refs = refs
    tab, sem, yt_ref, yt_sem, kern_ref, kern_sem, grid_ref, *refs = refs
    parts = out_ref.shape[0]
    grid = rows_ref.shape[0]
    blocks = tab.shape[0] // parts
    width = LINES * ORDER
    kept = grid // 2

    def table_copies(s):
        part = pl.ds(s * blocks, blocks)
        ends = [(yt_hbm.at[part], yt_ref.at[part]), (tab_hbm.at[part], tab.at[part])]
        if making:
            ends = [(here, there) for there, here in ends]
        return [
            pltpu.make_async_copy(ends[0][0], ends[0][1], yt_sem.at[s]),
            pltpu.make_async_copy(ends[1][0], ends[1][1], sem.at[s]),
        ]

    kern_copy = pltpu.make_async_copy(kern_hbm, kern_ref, kern_sem)
    if not making:
        for s in range(parts):
            for copy in table_copies(s):
                copy.start()
    kern_copy.start()
    grid_ref[...] = jnp.zeros(grid_ref.shape, F32)
    if making:
        make_tables = table_maker(atom_ref, z_ref, turn_ref, tab, yt_ref)
    if closing:
        near_ref, col_ref, sum_ref = refs
        near_tiles(places, v_ref, near_ref, col_ref)
        pair_size = blocks * TILE // parts

    def plane(q):
        return pl.ds(pl.multiple_of(q * LINES, LINES), LINES)

    def x_weights(s):
        u = atom_ref[s, 3 * blocks : 4 * blocks, :]
        return spline_values(u), spline_slopes(u)

    def spread(s, carry):
        if making:
            make_tables(s)
        for copy in table_copies(s):
            copy.start() if making else copy.wait()
        value, slope = x_weights(s)
        vec = [v_ref[s, c * blocks : (c + 1) * blocks, :] for c in range(3)]
        a0 = [vec[0] * slope[k] for k in range(ORDER)]
        a1 = [vec[1] * value[k] for k in range(ORDER)]
        a2 = [vec[2] * value[k] for k in range(ORDER)]
        sums = [jnp.zeros((LINES, grid), F32) for _ in range(blocks + REACH)]
        for b in range(blocks):
            g = s * blocks + b
            row = slice(b, b + 1)
            yt, dyt = yt_ref[g, 0:LINES, :], yt_ref[g, LINES : 2 * LINES, :]
            lead = jnp.concatenate([a0[k][row] * yt + a1[k][row] * dyt for k in range(ORDER)], axis=0)
            tail = jnp.concatenate([a2[k][row] * yt for k in range(ORDER)], axis=0)
            high, low = halves(jnp.concatenate([lead, tail], axis=1))
            lhs = jnp.concatenate([high, low], axis=0).astype(BF16)
            out = lax.dot_general(lhs, tab[g], NT, preferred_element_type=F32)
            out = out[:width] + out[width:]
            for k in range(ORDER):
                sums[b + k] = sums[b + k] + out[k * LINES : (k + 1) * LINES]
        for j, tile in enumerate(sums):
            grid_ref[plane(s * blocks + j), :] += tile
        return carry

    lax.fori_loop(0, parts, spread, 0)
    side = REACH // 2
    left, right = slice(0, side * LINES), slice((side + grid) * LINES, (2 * side + grid) * LINES)
    first = slice(side * LINES, 2 * side * LINES)
    last = slice(grid * LINES, (side + grid) * LINES)
    grid_ref[last, :] += grid_ref[left, :]
    grid_ref[first, :] += grid_ref[right, :]

    def product(matrix, x):
        mh, ml = halves(matrix)
        xh, xl = halves(x)
        rhs = jnp.concatenate([xh, xl], axis=0).astype(BF16)
        mh, ml = mh.astype(BF16), ml.astype(BF16)
        return bdot(jnp.concatenate([mh, mh], axis=1), rhs) + bdot(
            jnp.concatenate([ml, ml], axis=1), rhs
        )

    def lines(j):
        return pl.ds(side * LINES + j, grid, stride=LINES)

    lower = lax.broadcasted_iota(jnp.int32, (grid, grid), 1) < kept

    def folded(j):
        x = grid_ref[lines(j), :]
        return x + pltpu.roll(x, kept, 1)

    charge = jnp.concatenate(
        [jnp.where(lower, folded(j), folded(j + ROWS)) for j in range(ROWS)], axis=1
    )
    spectrum = product(rows_ref[...], charge)
    kern_copy.wait()
    weighted = spectrum * kern_ref[...]
    potential = product(cols_ref[...], weighted)
    for j in range(ROWS):
        x = potential[:, j * grid : (j + 1) * grid]
        y = pltpu.roll(x, kept, 1)
        grid_ref[lines(j), :] = jnp.where(lower, x, y)
        grid_ref[lines(j + ROWS), :] = jnp.where(lower, y, x)
    grid_ref[left, :] = grid_ref[last, :]
    grid_ref[right, :] = grid_ref[first, :]
    if closing:
        energy = jnp.sum(spectrum * weighted, axis=0, keepdims=True)
        energy = sum(energy[:, j * grid : (j + 1) * grid] for j in range(ROWS))

    def gather(s, carry):
        if closing:
            pair_part(s, pair_size, wts_ref, near_ref, col_ref, sum_ref)
        value, slope = x_weights(s)
        pieces = [halves(grid_ref[plane(s * blocks + q), :]) for q in range(blocks + REACH)]
        fields = ([], [], [])
        for b in range(blocks):
            g = s * blocks + b
            row = slice(b, b + 1)
            yt, dyt = yt_ref[g, 0:LINES, :], yt_ref[g, LINES : 2 * LINES, :]
            near = pieces[b : b + ORDER]
            high = jnp.concatenate([x[0] for x in near], axis=0).astype(BF16)
            low = jnp.concatenate([x[1] for x in near], axis=0).astype(BF16)
            table = tab[g]
            out = bdot(
                jnp.concatenate([high, low], axis=1),
                jnp.concatenate([table, table[:kept], jnp.zeros_like(table[:kept])], axis=0),
            )
            tiles = [out[k * LINES : (k + 1) * LINES] for k in range(ORDER)]
            f0 = sum(slope[k][row] * tiles[k][:, :TILE] for k in range(ORDER))
            f1 = sum(value[k][row] * tiles[k][:, :TILE] for k in range(ORDER))
            f2 = sum(value[k][row] * tiles[k][:, TILE:] for k in range(ORDER))
            for i, part in enumerate((yt * f0, dyt * f1, yt * f2)):
                fields[i].append(jnp.sum(part, axis=0, keepdims=True))
        for i in range(3):
            out_ref[s, i * blocks : (i + 1) * blocks, :] = jnp.concatenate(fields[i], axis=0)
        return carry

    lax.fori_loop(0, parts, gather, 0)
    if making:
        for s in range(parts):
            for copy in table_copies(s):
                copy.wait()
    if closing:
        for b in range(blocks):
            turned = PAIR_C * sum_ref[b * TILE : (b + 1) * TILE, :].T
            for c in range(3):
                pair_ref[c * blocks + b : c * blocks + b + 1, :] = turned[c : c + 1]
        sums = moment_rows(energy, *known, pair_ref)
        for d in range(parts):
            out_ref[d, 3 * blocks :, :] = sums


def field_call(vec, rows, cols, kern, first=(), tables=(), final=()):
    parts = vec.shape[0]
    grid = rows.shape[0]
    blocks = grid // parts
    mode = (len(first) > 0, len(final) > 0)
    tab_shape = jax.ShapeDtypeStruct((grid, grid, 2 * TILE), BF16)
    yt_shape = jax.ShapeDtypeStruct((grid, 2 * LINES, TILE), F32)
    args = [vec, rows, cols, kern, *first, *tables, *final]
    specs = [IN_VMEM] * 3 + [IN_HBM] + [IN_VMEM] * len(first)
    if tables:
        specs += [IN_VMEM, IN_HBM, IN_HBM]
    if final:
        specs += [IN_SMEM] * 2 + [IN_VMEM] * (len(final) - 2)
    out_rows = 3 * blocks + (ROWS if final else 0)
    shapes = [jax.ShapeDtypeStruct((parts, out_rows, TILE), F32)]
    out_specs = [IN_VMEM]
    scratch = [
        pltpu.VMEM(tab_shape.shape, BF16),
        pltpu.SemaphoreType.DMA((parts,)),
        pltpu.VMEM(yt_shape.shape, F32),
        pltpu.SemaphoreType.DMA((parts,)),
        pltpu.VMEM(kern.shape, F32),
        pltpu.SemaphoreType.DMA(()),
        pltpu.VMEM(((grid + REACH) * LINES, grid), F32),
    ]
    if first:
        shapes += [tab_shape, yt_shape]
        out_specs += [IN_HBM, IN_HBM]
    if final:
        shapes.append(jax.ShapeDtypeStruct((3 * blocks, TILE), F32))
        out_specs.append(IN_VMEM)
        scratch += [
            pltpu.VMEM((blocks + 2 * HALO_BLK, ROWS, TILE), F32),
            pltpu.VMEM((blocks * TILE, ROWS), F32),
            pltpu.VMEM((blocks * TILE, ROWS), F32),
        ]
    return pl.pallas_call(
        lambda *refs: field_kernel(mode, *refs),
        in_specs=specs,
        out_specs=out_specs,
        out_shape=shapes,
        scratch_shapes=scratch,
        name="field",
        **params(1 << 31, 56 << 20),
    )(*args)


def pair_kernel(list_ref, count_ref, rank_ref, left_ref, pos_ref, right_ref, vec_ref, out_ref, acc_ref, near_ref, col_ref):
    blocks = pos_ref.shape[1] // TILE
    near_tiles((rank_ref, left_ref, pos_ref, right_ref), vec_ref, near_ref, col_ref)
    chunk = TILE // 2
    shape = (chunk, TILE)
    ahead = lax.broadcasted_iota(jnp.int32, shape, 1) - lax.broadcasted_iota(jnp.int32, shape, 0)

    def one_block(b, carry):
        for c in range(TILE // chunk):
            home = col_ref[pl.ds(pl.multiple_of(b * TILE + c * chunk, chunk), chunk), :]
            hx = jnp.broadcast_to(home[:, 0:1], shape)
            hy = jnp.broadcast_to(home[:, 1:2], shape)
            hz = jnp.broadcast_to(home[:, 2:3], shape)

            def one_tile(k, sums):
                sx, sy, sz = sums
                j = list_ref[b, k]
                near = near_ref[j]
                dx, dy, dz = hx - near[0:1], hy - near[1:2], hz - near[2:3]
                vx, vy, vz = near[3:4], near[4:5], near[5:6]
                inverse = lax.rsqrt(dx * dx + dy * dy + dz * dz + 1.0)
                square = inverse * inverse
                itself = ahead == c * chunk - (j - b - HALO_BLK) * TILE
                third = jnp.where(itself, 0.0, inverse * square)
                fifth = (third * square) * (3.0 * (dx * vx + dy * vy + dz * vz))
                return (
                    sx + (third * vx - fifth * dx),
                    sy + (third * vy - fifth * dy),
                    sz + (third * vz - fifth * dz),
                )

            zero = jnp.zeros(shape, F32)
            sums = lax.fori_loop(0, count_ref[b], one_tile, (zero, zero, zero))
            for i in range(3):
                acc_ref[i, c * chunk : (c + 1) * chunk, :] = sums[i]
        for i in range(3):
            out_ref[pl.ds(i * blocks + b, 1), :] = PAIR_C * jnp.sum(acc_ref[i].T, axis=0, keepdims=True)
        return carry

    lax.fori_loop(0, blocks, one_block, 0)


def pair_call(tiles, counts, places, vec):
    rank, left, pos, right = places
    blocks = pos.shape[1] // TILE
    return pl.pallas_call(
        pair_kernel,
        in_specs=[IN_SMEM] * 3 + [IN_VMEM] * 4,
        out_specs=IN_VMEM,
        out_shape=jax.ShapeDtypeStruct((3 * blocks, TILE), F32),
        scratch_shapes=[
            pltpu.VMEM((3, TILE, TILE), F32),
            pltpu.VMEM((blocks + 2 * HALO_BLK, ROWS, TILE), F32),
            pltpu.VMEM((blocks * TILE, ROWS), F32),
        ],
        name="pair",
        **params(1 << 30),
    )(tiles, counts, rank, left, pos, right, vec)


def update_kernel(ret_ref, pair_ref, inv_ref, own_ref, out_ref):
    blocks = inv_ref.shape[0]
    far = jnp.sum(ret_ref[...], axis=0) - pair_ref[...]
    inv = inv_ref[...]
    vec = jnp.concatenate([far[c * blocks : (c + 1) * blocks] / inv for c in range(3)], axis=0)
    own_ref[...] = vec
    for d in range(out_ref.shape[0]):
        out_ref[d] = vec


def update_call(returned, pair, inv):
    parts = returned.shape[0]
    return pl.pallas_call(
        update_kernel,
        in_specs=[IN_VMEM] * 3,
        out_specs=[IN_VMEM] * 2,
        out_shape=[
            jax.ShapeDtypeStruct(pair.shape, F32),
            jax.ShapeDtypeStruct((parts,) + pair.shape, F32),
        ],
        name="update",
        **params(1 << 24),
    )(returned, pair, inv)


def finish_kernel(ret_ref, pair_ref, v0_ref, v1_ref, v2_ref, inv_ref, dip_ref, res_ref):
    blocks = inv_ref.shape[0]
    summed = jnp.sum(ret_ref[...], axis=0)
    total = jnp.sum(summed[3 * blocks :], axis=1, keepdims=True)
    h = summed[: 3 * blocks] - pair_ref[...]
    m = [total[k : k + 1, 0:1] for k in range(6)]
    s = [lax.rsqrt(m[2 * i]) for i in range(3)]
    g = [[m[i + j] * s[i] * s[j] for j in range(3)] for i in range(3)]
    b = [-m[i + 3] * s[i] for i in range(3)]
    l10 = g[1][0] / g[0][0]
    l20 = g[2][0] / g[0][0]
    p11 = g[1][1] - l10 * g[0][1]
    p12 = g[1][2] - l10 * g[0][2]
    l21 = p12 / p11
    p22 = g[2][2] - l20 * g[0][2] - l21 * p12
    b1 = b[1] - l10 * b[0]
    b2 = b[2] - l20 * b[0] - l21 * b1
    y2 = b2 / p22
    y1 = (b1 - p12 * y2) / p11
    y0 = (b[0] - g[0][1] * y1 - g[0][2] * y2) / g[0][0]
    a0, a1, a2 = s[0] * y0, s[1] * y1, s[2] * y2
    scale = 1.0 / (a0 - a1 + a2 - 1.0)
    a0, a1, a2, a3 = a0 * scale, a1 * scale, a2 * scale, scale
    c2 = -a3
    c1 = a3 - a2
    c0 = a2 - a3 - a1
    ip = jnp.concatenate([inv_ref[...]] * 3, axis=0)
    v0, v1, v2 = v0_ref[...], v1_ref[...], v2_ref[...]
    dip = c0 * v0 + c1 * v1 + c2 * v2
    res = ip * (a0 * v0 + a1 * v1 + a2 * v2) + a3 * h
    for c in range(3):
        for b in range(blocks):
            row = slice(c * blocks + b, c * blocks + b + 1)
            here = slice(b * TILE, (b + 1) * TILE)
            dip_ref[c : c + 1, here] = dip[row]
            res_ref[c : c + 1, here] = res[row]


def finish_call(returned, pair, vectors, inv):
    atoms = inv.shape[0] * TILE
    return pl.pallas_call(
        finish_kernel,
        in_specs=[IN_VMEM] * 6,
        out_specs=[IN_VMEM] * 2,
        out_shape=[jax.ShapeDtypeStruct((3, atoms), F32)] * 2,
        name="finish",
        **params(1 << 24),
    )(returned, pair, *vectors, inv)


def fourier_matrix(size):
    freq = np.arange(size)
    mode = np.where(freq <= size // 2, freq, freq - size // 2)
    angle = (mode[:, None] * np.arange(size)[None, :] % size) * (2.0 * np.pi / size)
    rows = np.where((freq <= size // 2)[:, None], np.cos(angle), np.sin(angle))
    return rows.astype(np.float32)


def kernel_lines(x_axis, y_axis, z_axis):
    mode_sq = x_axis[0] * x_axis[0] + y_axis[0] * y_axis[0] + z_axis[0] * z_axis[0]
    safe_sq = jnp.where(mode_sq > 0, mode_sq, 1.0)
    green = jnp.where(mode_sq > 0, RECIP_C * jnp.exp(-DAMP * safe_sq) / safe_sq, 0.0)
    return green * x_axis[1] * y_axis[1] * z_axis[1]


def swap(x):
    return lax.all_to_all(x, "gx", split_axis=0, concat_axis=0, tiled=True)


def per_device_modes(positions, field, inv_polar, x_spline, yz_spline, tile_list, tile_count):
    parts = lax.axis_size("gx")
    rank = lax.axis_index("gx")
    atoms = positions.shape[1]
    halo = HALO_BLK * TILE
    blocks = atoms // TILE
    up = [(i, (i + 1) % parts) for i in range(parts)]
    down = [(j, i) for i, j in up]

    own, inv, packed = pack_call(
        field, inv_polar[None, :], x_spline.transpose(1, 0, 2), yz_spline, parts
    )
    everyone = swap(packed)
    edges, everyone = lax.optimization_barrier((positions, everyone))
    left = lax.ppermute(edges[:, atoms - halo :], "gx", up)
    right = lax.ppermute(edges[:, :halo], "gx", down)

    offsets = jnp.arange(SPAN, dtype=jnp.int32)
    block_ids = jnp.arange(blocks, dtype=jnp.int32)
    live = jnp.arange(tile_list.shape[1], dtype=jnp.int32)[None, :] < tile_count[:, None]
    hit = tile_list[:, :, None] == block_ids[:, None, None] + offsets[None, None, :]
    wts = jnp.sum((hit & live[:, :, None]).astype(F32), axis=1).reshape(-1)

    matrix = fourier_matrix(GRID)
    rows, cols = jnp.asarray(matrix), jnp.asarray(matrix.T)
    all_freq = jnp.arange(GRID, dtype=jnp.int32)
    kept = GRID // 2
    ky_freq = rank // 2 * LINES + jnp.arange(LINES, dtype=jnp.int32)
    kz_freq = rank % 2 * kept + jnp.arange(kept, dtype=jnp.int32)
    z_rows = lax.dynamic_slice_in_dim(rows, rank % 2 * kept, kept, 0)
    full_modes, full_weights = mode_of(all_freq, GRID)
    ky_modes, ky_weights = mode_of(ky_freq, GRID)
    kz_modes, kz_weights = mode_of(kz_freq, GRID)

    def paired_lines(x):
        x = x.reshape(1, 2, ROWS, 1)
        x = jnp.broadcast_to(x.transpose(0, 2, 1, 3), (1, ROWS, 2, kept))
        return x.reshape(1, ROWS * GRID)

    def repeated(x):
        return jnp.tile(x[None, :], (1, LINES))

    kern = kernel_lines(
        (full_modes[:, None], full_weights[:, None]),
        (paired_lines(ky_modes), paired_lines(ky_weights)),
        (repeated(kz_modes), repeated(kz_weights)),
    )
    steps = jnp.arange(1, ORDER).astype(F32)
    angle = steps[:, None] * ky_modes[None, :] * (2.0 * jnp.pi / GRID)
    sine = (ky_freq > GRID // 2).astype(F32)
    turns = jnp.concatenate([ky_modes[None], sine[None], jnp.cos(angle), jnp.sin(angle)])
    turns = jnp.pad(turns.T, ((0, 0), (0, TILE - turns.shape[0])))

    partial, table, yt = field_call(everyone, rows, cols, kern, first=(z_rows, turns))
    tables = (everyone, table, yt)
    places = (rank[None].astype(jnp.int32), left, positions, right)
    vec, vectors = everyone, [own]
    for step in range(ITERS):
        last = step + 1 == ITERS
        if last:
            final = (wts, *places, *vectors, inv)
            partial, pair = field_call(vec, rows, cols, kern, tables=tables, final=final)
        elif step > 0:
            (partial,) = field_call(vec, rows, cols, kern, tables=tables)
        returned = swap(partial)
        if not last:
            pair = pair_call(tile_list, tile_count, places, vec)
            own, packed = update_call(returned, pair, inv)
            vectors.append(own)
            vec = swap(packed)
    dipoles, residual = finish_call(returned, pair, vectors, inv)
    return (dipoles, residual)


def per_device(positions, *others):
    parts = lax.axis_size("gx")
    atoms = positions.shape[1]
    planes = GRID // parts
    modes = (
        parts * ROWS == GRID
        and atoms == planes * TILE
        and planes == ROWS
        and atoms >= HALO_BLK * TILE
        and ORDER == 5
        and atoms % parts == 0
        and (atoms // parts) % 32 == 0
        and TILE % (atoms // parts) == 0
        and ITERS == 3
    )
    run = per_device_modes if modes else per_device_general
    return run(positions, *others)


def solution(mesh):
    placed = (
        P(None, ("rep", "gx")),
        P(None, ("rep", "gx")),
        P(("rep", "gx")),
        P(None, None, ("rep", "gx")),
        P(None, ("rep", "gx"), None),
        P(("rep", "gx"), None),
        P(("rep", "gx")),
    )
    return jax.shard_map(
        per_device,
        mesh=mesh,
        in_specs=placed,
        out_specs=(P(None, ("rep", "gx")), P(None, ("rep", "gx"))),
        check_vma=False,
    )
```

```python
import jax
import numpy as np
import jax.numpy as jnp
from jax import lax
from jax.experimental import pallas as pl
from jax.experimental.pallas import tpu as pltpu
from jax.sharding import PartitionSpec as P

GRID = 128
ORDER = 5
TILE = 128
HALO_BLK = 3
ITERS = 3


PAIR_C = 0.025
RECIP_C = 8192.0
DAMP = 0.0008
EXACT = lax.Precision.HIGHEST


def extended(x, sides, width):
    for axis, dim in sides:
        devices, length = (lax.axis_size(axis), x.shape[dim])
        up = [(i, (i + 1) % devices) for i in range(devices)]
        down = [(j, i) for i, j in up]
        last = lax.slice_in_dim(x, length - width, length, axis=dim)
        first = lax.slice_in_dim(x, 0, width, axis=dim)
        before = lax.ppermute(last, axis, up)
        after = lax.ppermute(first, axis, down)
        x = jnp.concatenate([before, x, after], axis=dim)
    return x


def pair_field(home_pos, ext_pos, ext_vec, tile_rows, live_counts):
    slab_blocks = home_pos.shape[1] // TILE
    ext_blocks = ext_pos.shape[1] // TILE
    home_blocks = home_pos.reshape(3, slab_blocks, TILE).transpose(1, 0, 2)
    pos_blocks = ext_pos.reshape(3, ext_blocks, TILE)
    vec_blocks = ext_vec.reshape(3, ext_blocks, TILE)
    slot_index = jnp.arange(tile_rows.shape[1], dtype=jnp.int32)
    self_pair = jnp.eye(TILE, dtype=bool)

    def one_block(carried, scan_item):
        home_block, tile_row, live_count, block_index = scan_item
        near_pos = jnp.take(pos_blocks, tile_row, axis=1)
        near_vec = jnp.take(vec_blocks, tile_row, axis=1)
        offsets = home_block[:, None, :, None] - near_pos[:, :, None, :]
        distance_sq = jnp.sum(offsets * offsets, axis=0) + 1.0
        inverse = lax.rsqrt(distance_sq)
        third_power = inverse * inverse * inverse
        fifth_power = third_power * inverse * inverse
        same_block = (tile_row == block_index + HALO_BLK)[:, None, None]
        live_mask = (slot_index < live_count)[:, None, None] & ~(same_block & self_pair[None])
        third_power = jnp.where(live_mask, third_power, 0.0)
        fifth_power = jnp.where(live_mask, fifth_power, 0.0)
        projection = jnp.sum(offsets * near_vec[:, :, None, :], axis=0)
        field_sum = jnp.sum(
            third_power[None] * near_vec[:, :, None, :]
            - 3.0 * (fifth_power * projection)[None] * offsets,
            axis=(1, 3),
        )
        return (carried, PAIR_C * field_sum)

    block_ids = jnp.arange(slab_blocks, dtype=jnp.int32)
    _, blocks_out = lax.scan(
        one_block, jnp.zeros((), jnp.float32), (home_blocks, tile_rows, live_counts, block_ids)
    )
    return blocks_out.transpose(1, 0, 2).reshape(3, slab_blocks * TILE)


def slab_weights(local_plane, x_spline, planes):
    spline_steps = jnp.arange(ORDER, dtype=jnp.int32)
    plane_index = jnp.arange(planes, dtype=jnp.int32)
    matches = local_plane[None, :, None] + spline_steps[:, None, None] == plane_index[None, None, :]
    spline_value = jnp.sum(jnp.where(matches, x_spline[0][:, :, None], 0.0), axis=0)
    spline_slope = jnp.sum(jnp.where(matches, x_spline[1][:, :, None], 0.0), axis=0)
    return (spline_value, spline_slope)


def spread_dipoles(vector, spline_value, spline_slope, yz_spline):
    atoms_here = spline_value.shape[0]
    planes = spline_value.shape[1]
    grid_lines = yz_spline.shape[2]
    lead_terms = (vector[0][:, None] * spline_slope)[:, :, None] * yz_spline[0][:, None, :]
    lead_terms = (
        lead_terms + (vector[1][:, None] * spline_value)[:, :, None] * yz_spline[1][:, None, :]
    )
    tail_terms = (vector[2][:, None] * spline_value)[:, :, None] * yz_spline[0][:, None, :]
    contract = (((0,), (0,)), ((), ()))
    charge = lax.dot_general(
        lead_terms.reshape(atoms_here, planes * grid_lines), yz_spline[2], contract, precision=EXACT
    )
    charge = charge + lax.dot_general(
        tail_terms.reshape(atoms_here, planes * grid_lines), yz_spline[3], contract, precision=EXACT
    )
    return charge.reshape(planes, grid_lines, grid_lines)


def gather_field(potential, spline_value, spline_slope, yz_spline):
    planes = potential.shape[0]
    grid_lines = potential.shape[1]
    atoms_here = spline_value.shape[0]
    flat_grid = potential.reshape(planes * grid_lines, grid_lines)
    contract = (((1,), (1,)), ((), ()))
    plain_sum = lax.dot_general(yz_spline[2], flat_grid, contract, precision=EXACT).reshape(
        atoms_here, planes, grid_lines
    )
    tilted_sum = lax.dot_general(yz_spline[3], flat_grid, contract, precision=EXACT).reshape(
        atoms_here, planes, grid_lines
    )
    first_comp = jnp.sum(
        spline_slope[:, :, None] * yz_spline[0][:, None, :] * plain_sum, axis=(1, 2)
    )
    second_comp = jnp.sum(
        spline_value[:, :, None] * yz_spline[1][:, None, :] * plain_sum, axis=(1, 2)
    )
    third_comp = jnp.sum(
        spline_value[:, :, None] * yz_spline[0][:, None, :] * tilted_sum, axis=(1, 2)
    )
    return jnp.stack([first_comp, second_comp, third_comp])


def mode_of(freq, size):
    half_size = size // 2
    mode_num = jnp.where(freq <= half_size, freq, freq - half_size)
    weight = jnp.where((freq == 0) | (freq == half_size), 1.0 / size, 2.0 / size)
    return (mode_num.astype(jnp.float32), weight.astype(jnp.float32))


def basis_rows(size, points):
    freq = jnp.arange(size, dtype=jnp.int32)
    half_size = size // 2
    mode_num = jnp.where(freq <= half_size, freq, freq - half_size)
    phase = mode_num[:, None] * points[None, :] % size
    angle = phase.astype(jnp.float32) * (2.0 * jnp.pi / size)
    return jnp.where((freq <= half_size)[:, None], jnp.cos(angle), jnp.sin(angle))


def kernel_block(x_modes, x_weights, y_modes, y_weights, z_modes, z_weights):
    mode_sq = (
        x_modes[:, None, None] * x_modes[:, None, None]
        + y_modes[None, :, None] * y_modes[None, :, None]
        + z_modes[None, None, :] * z_modes[None, None, :]
    )
    safe_sq = jnp.where(mode_sq > 0, mode_sq, 1.0)
    green = jnp.where(mode_sq > 0, RECIP_C * jnp.exp(-DAMP * safe_sq) / safe_sq, 0.0)
    return green * x_weights[:, None, None] * y_weights[None, :, None] * z_weights[None, None, :]


def forward_lines(charge, fourier_rows):
    along_z = jnp.einsum("pyz,kz->pyk", charge, fourier_rows, precision=EXACT)
    return jnp.einsum("jy,pyk->pjk", fourier_rows, along_z, precision=EXACT)


def inverse_lines(spectrum, fourier_rows):
    along_z = jnp.einsum("pjk,kz->pjz", spectrum, fourier_rows, precision=EXACT)
    return jnp.einsum("jy,pjz->pyz", fourier_rows, along_z, precision=EXACT)


def per_device_general(positions, field, inv_polar, x_spline, yz_spline, tile_list, tile_count):
    rank_count = lax.axis_size("gx")
    rank_index = lax.axis_index("gx")
    atoms_here = positions.shape[1]
    planes = GRID // rank_count
    extent = planes + 4
    halo_atoms = HALO_BLK * TILE
    slab_blocks = atoms_here // TILE
    local_plane = jnp.arange(atoms_here, dtype=jnp.int32) * planes // atoms_here
    spline_value, spline_slope = slab_weights(local_plane, x_spline, extent)
    ext_pos = extended(positions, (("gx", 1),), halo_atoms)
    shift_x = jnp.concatenate(
        [
            jnp.full((halo_atoms,), -1.0 * slab_blocks, jnp.float32),
            jnp.zeros((atoms_here,), jnp.float32),
            jnp.full((halo_atoms,), 1.0 * slab_blocks, jnp.float32),
        ]
    )
    ext_pos = ext_pos.at[0].add(shift_x)
    fourier_rows = basis_rows(GRID, jnp.arange(GRID, dtype=jnp.int32))
    ky_count = GRID // rank_count
    all_freq = jnp.arange(GRID, dtype=jnp.int32)
    ky_freq = rank_index * ky_count + jnp.arange(ky_count, dtype=jnp.int32)
    full_modes, full_weights = mode_of(all_freq, GRID)
    ky_modes, ky_weights = mode_of(ky_freq, GRID)
    kernel = kernel_block(full_modes, full_weights, ky_modes, ky_weights, full_modes, full_weights)
    kernel = kernel.reshape(GRID, ky_count * GRID)
    source_rows = jnp.arange(rank_count * extent, dtype=jnp.int32)
    points = (source_rows // extent * planes - 2 + source_rows % extent) % GRID
    across = basis_rows(GRID, points)

    def reciprocal(charge):
        spectrum = forward_lines(charge, fourier_rows)
        pencils = lax.all_to_all(spectrum, "gx", split_axis=1, concat_axis=0, tiled=True)
        rows_in = pencils.shape[0]
        flat_pencils = pencils.reshape(rows_in, ky_count * GRID)
        spectral_lines = jnp.dot(across, flat_pencils, precision=EXACT) * kernel
        returned_lines = lax.dot_general(
            across, spectral_lines, (((0,), (0,)), ((), ())), precision=EXACT
        )
        returned = lax.all_to_all(
            returned_lines.reshape(rows_in, ky_count, GRID),
            "gx",
            split_axis=0,
            concat_axis=1,
            tiled=True,
        )
        return inverse_lines(returned, fourier_rows)

    def apply(vector):
        ext_vec = extended(vector, (("gx", 1),), halo_atoms)
        near_field = pair_field(positions, ext_pos, ext_vec, tile_list, tile_count)
        charge = spread_dipoles(vector, spline_value, spline_slope, yz_spline)
        far_field = gather_field(reciprocal(charge), spline_value, spline_slope, yz_spline)
        return inv_polar[None, :] * vector + far_field - near_field

    def paired(residual, precond, applied):
        return lax.psum((jnp.sum(residual * precond), jnp.sum(applied * precond)), "gx")

    dipoles = jnp.zeros_like(field)
    residual = field
    precond = field / inv_polar[None, :]
    applied = apply(precond)
    rz_now, curvature = paired(residual, precond, applied)
    step_size = rz_now / curvature
    direction = precond
    applied_dir = applied
    for sweep_index in range(ITERS):
        dipoles = dipoles + step_size * direction
        residual = residual - step_size * applied_dir
        if sweep_index + 1 < ITERS:
            precond = residual / inv_polar[None, :]
            applied = apply(precond)
            rz_next, curvature = paired(residual, precond, applied)
            beta_ratio = rz_next / rz_now
            step_size = rz_next / (curvature - beta_ratio * rz_next / step_size)
            direction = precond + beta_ratio * direction
            applied_dir = applied + beta_ratio * applied_dir
            rz_now = rz_next
    return (dipoles, residual)


F32 = jnp.float32
BF16 = jnp.bfloat16
ROWS = 8
LINES = 2 * ROWS
IN_VMEM = pl.BlockSpec(memory_space=pltpu.VMEM)
IN_SMEM = pl.BlockSpec(memory_space=pltpu.SMEM)
IN_HBM = pl.BlockSpec(memory_space=pl.ANY)
REACH = ORDER - 1
SPAN = 2 * HALO_BLK + 1
PACKED = 6
NT = (((1,), (1,)), ((), ()))


def near(x):
    return pltpu.with_memory_space_constraint(x, pltpu.VMEM)


def params(flops, vmem=None):
    return dict(
        cost_estimate=pl.CostEstimate(flops=flops, bytes_accessed=4 << 20, transcendentals=0),
        compiler_params=pltpu.CompilerParams(vmem_limit_bytes=vmem) if vmem else None,
    )


def halves(x):
    high = x.astype(BF16).astype(F32)
    return high, x - high


def bdot(a, b):
    return jnp.dot(a, b, preferred_element_type=F32)


def spline_values(u):
    w = 1.0 - u
    u2, w2 = u * u, w * w
    c = 1.0 / 24.0
    return [
        c * (w2 * w2),
        c * (11.0 + u * (-12.0 + u * (-6.0 + u * (12.0 - 4.0 * u)))),
        c * (11.0 + u * (12.0 + u * (-6.0 + u * (-12.0 + 6.0 * u)))),
        c * (1.0 + u * (4.0 + u * (6.0 + u * (4.0 - 4.0 * u)))),
        c * (u2 * u2),
    ]


def spline_slopes(u):
    w = 1.0 - u
    c = 1.0 / 6.0
    return [
        -c * (w * w * w),
        c * (-3.0 + u * (-3.0 + u * (9.0 - 4.0 * u))),
        c * (3.0 + u * (-3.0 + u * (-9.0 + 6.0 * u))),
        c * (1.0 + u * (3.0 + u * (3.0 - 4.0 * u))),
        c * (u * u * u),
    ]


def block_rows(ref, row):
    return jnp.concatenate(
        [ref[row : row + 1, b * TILE : (b + 1) * TILE] for b in range(ref.shape[1] // TILE)], axis=0
    )


def pack_kernel(field_ref, ip_ref, xs_ref, yz_ref, own_ref, inv_ref, out_ref):
    parts = out_ref.shape[0]
    blocks = field_ref.shape[1] // TILE
    grid = yz_ref.shape[2]
    inv = block_rows(ip_ref, 0)
    inv_ref[...] = inv
    tiles = [block_rows(field_ref, c) / inv for c in range(3)]
    for c in range(3):
        own_ref[c * blocks : (c + 1) * blocks, :] = tiles[c]
    tiles.append(sum(float(k) * block_rows(xs_ref.at[k], 0) for k in range(1, ORDER)) - 1.5)
    line = lax.broadcasted_iota(jnp.int32, (grid, TILE), 0)
    for axis in range(2):
        spots = []
        for b in range(blocks):
            here = slice(b * TILE, (b + 1) * TILE)
            value = yz_ref[2 * axis, here, :].T
            slope = yz_ref[2 * axis + 1, here, :].T
            used = jnp.where((value != 0.0) | (slope != 0.0), 1.0, 0.0)
            first = used * (1.0 - pltpu.roll(used, 1, 0))
            start = jnp.sum(first * line.astype(F32), axis=0, keepdims=True)
            offset = (line - start.astype(jnp.int32)) & (grid - 1)
            shift = jnp.sum(value * offset.astype(F32), axis=0, keepdims=True) - 1.5
            spots.append((start - float(grid // 2)) + shift)
        tiles.append(jnp.concatenate(spots, axis=0))
    for d in range(parts):
        for i, tile in enumerate(tiles):
            out_ref[d, i * blocks : (i + 1) * blocks, :] = tile


def pack_call(field, inv_row, xs, yz, parts):
    blocks = field.shape[1] // TILE
    return pl.pallas_call(
        pack_kernel,
        in_specs=[IN_VMEM] * 4,
        out_specs=[IN_VMEM] * 3,
        out_shape=[
            pltpu.VMEM((3 * blocks, TILE), F32),
            pltpu.VMEM((blocks, TILE), F32),
            pltpu.VMEM((parts, PACKED * blocks, TILE), F32),
        ],
        name="pack",
        **params(1 << 26),
    )(field, inv_row, xs, yz)


def table_maker(atom_ref, rows_ref, turn_ref, tab_ref, yt_ref):
    slabs = atom_ref.shape[0]
    blocks = tab_ref.shape[0] // slabs
    kept, grid = rows_ref.shape
    high, low = halves(rows_ref[...])
    twice = jnp.concatenate([high, low], axis=0).astype(BF16)
    matrix = jnp.concatenate([twice, twice], axis=1)
    packed = (LINES, TILE)
    line = lax.broadcasted_iota(jnp.int32, (grid, TILE), 0).astype(F32).astype(BF16)
    lines = [line[c * LINES : (c + 1) * LINES] for c in range(grid // LINES)]
    turn = [jnp.broadcast_to(turn_ref[:, c : c + 1], packed) for c in range(2 * ORDER)]
    half = float(grid // 2)

    def spread_row(x, b):
        return jnp.broadcast_to(x[b : b + 1], packed).astype(BF16)

    def one_slab(slab):
        def located(i):
            place = atom_ref[slab, i * blocks : (i + 1) * blocks, :]
            start = jnp.floor(place)
            u = place - start
            return start, spline_values(u), spline_slopes(u)

        start, values, slopes = located(5)
        start = start.astype(jnp.int32) + grid // 2
        spots = [((start + k) & (grid - 1)).astype(F32) for k in range(ORDER)]
        pieces = [halves(x) for x in values], [halves(x) for x in slopes]
        for b in range(blocks):
            at = [spread_row(x, b) for x in spots]
            tables = []
            for part in range(2):
                columns = []
                for kind in range(2):
                    rows = [spread_row(x[part], b) for x in pieces[kind]]
                    column = []
                    for here in lines:
                        dense = jnp.zeros(packed, BF16)
                        for k in range(ORDER):
                            dense = jnp.where(here == at[k], rows[k], dense)
                        column.append(dense)
                    columns.append(jnp.concatenate(column, axis=0))
                tables.append(jnp.concatenate(columns, axis=1))
            both = bdot(matrix, jnp.concatenate(tables, axis=0))
            high, low = halves(both[:kept] + both[kept:])
            tab_ref[slab * blocks + b] = jnp.concatenate([high, low], axis=0).astype(BF16)
        start, values, slopes = located(4)
        mode, sine = turn[0], turn[1]
        for b in range(blocks):
            row = slice(b, b + 1)
            phase = mode * start[row]
            phase = phase - 2.0 * half * jnp.floor(phase * (0.5 / half) + 0.5)
            angle = phase * (jnp.pi / (4.0 * half))
            sq = angle * angle
            s = angle * (1.0 + sq * (-1.0 / 6 + sq * (1.0 / 120 + sq * (-1.0 / 5040 + sq / 362880))))
            c = 1.0 + sq * (-0.5 + sq * (1.0 / 24 + sq * (-1.0 / 720 + sq / 40320)))
            for _ in range(2):
                s, c = 2.0 * s * c, 1.0 - 2.0 * s * s
            lead = jnp.where(sine > 0.0, s, c)
            side = jnp.where(sine > 0.0, -c, s)
            for i, weights in enumerate((values, slopes)):
                even = weights[0][row] + sum(weights[k][row] * turn[1 + k] for k in range(1, ORDER))
                odd = sum(weights[k][row] * turn[ORDER + k] for k in range(1, ORDER))
                yt_ref[slab * blocks + b, i * LINES : (i + 1) * LINES, :] = lead * even - side * odd

    return one_slab


def near_tiles(refs, vec_ref, near_ref, col_ref):
    rank_ref, left_ref, pos_ref, right_ref = refs
    blocks = pos_ref.shape[1] // TILE
    total = vec_ref.shape[0] * blocks
    shift = 1.0 * blocks
    for j in range(blocks + 2 * HALO_BLK):
        i = j - HALO_BLK
        g = rank_ref[0] * blocks + i
        if i < 0:
            g = jnp.where(g < 0, g + total, g)
            source, i, move = left_ref, j, -shift
        elif i < blocks:
            source, move = pos_ref, 0.0
        else:
            g = jnp.where(g >= total, g - total, g)
            source, i, move = right_ref, i - blocks, shift
        rows = source[:, i * TILE : (i + 1) * TILE]
        near_ref[j, 0:1, :] = rows[0:1] + move
        near_ref[j, 1:3, :] = rows[1:3]
        src = lax.shift_right_logical(g, 3)
        block = g & (ROWS - 1)
        for c in range(3):
            near_ref[j, 3 + c : 4 + c, :] = vec_ref[src, pl.ds(c * blocks + block, 1), :]
        near_ref[j, 6:8, :] = jnp.zeros((2, TILE), F32)
    for b in range(blocks):
        col_ref[b * TILE : (b + 1) * TILE, :] = near_ref[HALO_BLK + b].T


def pair_part(part, size, wts_ref, near_ref, col_ref, sum_ref):
    first = part * size
    b = lax.shift_right_logical(first, 7)
    chunk = min(size, 32)
    shape = (chunk, TILE)
    lane = lax.broadcasted_iota(jnp.int32, shape, 1)
    ahead = lane - lax.broadcasted_iota(jnp.int32, shape, 0)
    for c in range(size // chunk):
        start = pl.multiple_of(first + c * chunk, chunk)
        home = col_ref[pl.ds(start, chunk), :]
        hx = jnp.broadcast_to(home[:, 0:1], shape)
        hy = jnp.broadcast_to(home[:, 1:2], shape)
        hz = jnp.broadcast_to(home[:, 2:3], shape)
        sx = sy = sz = jnp.zeros(shape, F32)
        for e in range(SPAN):
            tile = near_ref[b + e]
            dx, dy, dz = hx - tile[0:1], hy - tile[1:2], hz - tile[2:3]
            vx, vy, vz = tile[3:4], tile[4:5], tile[5:6]
            inverse = lax.rsqrt(dx * dx + dy * dy + dz * dz + 1.0)
            square = inverse * inverse
            third = wts_ref[b * SPAN + e] * (inverse * square)
            if e == HALO_BLK:
                third = jnp.where(ahead == start - b * TILE, 0.0, third)
            fifth = (third * square) * (3.0 * (dx * vx + dy * vy + dz * vz))
            sx = sx + (third * vx - fifth * dx)
            sy = sy + (third * vy - fifth * dy)
            sz = sz + (third * vz - fifth * dz)
        sums = [jnp.sum(x, axis=1, keepdims=True) for x in (sx, sy, sz)]
        both = jnp.where(lane == 0, sums[0], jnp.where(lane == 1, sums[1], sums[2]))
        sum_ref[pl.ds(start, chunk), :] = both[:, :ROWS]


def moment_rows(energy, v0_ref, v1_ref, v2_ref, inv_ref, pair_ref):
    ip = jnp.concatenate([inv_ref[...]] * 3, axis=0)
    v0, v1, v2 = v0_ref[...], v1_ref[...], v2_ref[...]
    d1, d2 = ip * v1, ip * v2
    terms = [v0 * (ip * v0), v0 * d1, v1 * d1, v1 * d2, v2 * d2, -(v2 * pair_ref[...])]
    rows = [jnp.sum(term, axis=0, keepdims=True) for term in terms]
    rows[5] = rows[5] + energy
    blank = jnp.zeros((ROWS - len(rows), TILE), F32)
    return jnp.concatenate(rows + [blank], axis=0)


def field_kernel(mode, *refs):
    making, closing = mode
    v_ref, rows_ref, cols_ref, kern_hbm, *refs = refs
    if making:
        z_ref, turn_ref, out_ref, tab_hbm, yt_hbm, *refs = refs
        atom_ref = v_ref
    elif closing:
        atom_ref, tab_hbm, yt_hbm, wts_ref, *refs = refs
        places, known, refs = refs[:4], refs[4:8], refs[8:]
        out_ref, pair_ref, *refs = refs
    else:
        atom_ref, tab_hbm, yt_hbm, out_ref, *refs = refs
    tab, sem, yt_ref, yt_sem, kern_ref, kern_sem, grid_ref, *refs = refs
    parts = out_ref.shape[0]
    grid = rows_ref.shape[0]
    blocks = tab.shape[0] // parts
    width = LINES * ORDER
    kept = grid // 2

    def table_copies(s):
        part = pl.ds(s * blocks, blocks)
        ends = [(yt_hbm.at[part], yt_ref.at[part]), (tab_hbm.at[part], tab.at[part])]
        if making:
            ends = [(here, there) for there, here in ends]
        return [
            pltpu.make_async_copy(ends[0][0], ends[0][1], yt_sem.at[s]),
            pltpu.make_async_copy(ends[1][0], ends[1][1], sem.at[s]),
        ]

    kern_copy = pltpu.make_async_copy(kern_hbm, kern_ref, kern_sem)
    if not making:
        for s in range(parts):
            for copy in table_copies(s):
                copy.start()
    kern_copy.start()
    grid_ref[...] = jnp.zeros(grid_ref.shape, F32)
    if making:
        make_tables = table_maker(atom_ref, z_ref, turn_ref, tab, yt_ref)
    if closing:
        near_ref, col_ref, sum_ref = refs
        near_tiles(places, v_ref, near_ref, col_ref)
        pair_size = blocks * TILE // parts

    def plane(q):
        return pl.ds(pl.multiple_of(q * LINES, LINES), LINES)

    def x_weights(s):
        u = atom_ref[s, 3 * blocks : 4 * blocks, :]
        return spline_values(u), spline_slopes(u)

    def spread(s, carry):
        if making:
            make_tables(s)
        for copy in table_copies(s):
            copy.start() if making else copy.wait()
        value, slope = x_weights(s)
        vec = [v_ref[s, c * blocks : (c + 1) * blocks, :] for c in range(3)]
        a0 = [vec[0] * slope[k] for k in range(ORDER)]
        a1 = [vec[1] * value[k] for k in range(ORDER)]
        a2 = [vec[2] * value[k] for k in range(ORDER)]
        sums = [jnp.zeros((LINES, grid), F32) for _ in range(blocks + REACH)]
        for b in range(blocks):
            g = s * blocks + b
            row = slice(b, b + 1)
            yt, dyt = yt_ref[g, 0:LINES, :], yt_ref[g, LINES : 2 * LINES, :]
            lead = jnp.concatenate([a0[k][row] * yt + a1[k][row] * dyt for k in range(ORDER)], axis=0)
            tail = jnp.concatenate([a2[k][row] * yt for k in range(ORDER)], axis=0)
            high, low = halves(jnp.concatenate([lead, tail], axis=1))
            lhs = jnp.concatenate([high, low], axis=0).astype(BF16)
            out = lax.dot_general(lhs, tab[g], NT, preferred_element_type=F32)
            out = out[:width] + out[width:]
            for k in range(ORDER):
                sums[b + k] = sums[b + k] + out[k * LINES : (k + 1) * LINES]
        for j, tile in enumerate(sums):
            grid_ref[plane(s * blocks + j), :] += tile
        return carry

    lax.fori_loop(0, parts, spread, 0)
    side = REACH // 2
    left, right = slice(0, side * LINES), slice((side + grid) * LINES, (2 * side + grid) * LINES)
    first = slice(side * LINES, 2 * side * LINES)
    last = slice(grid * LINES, (side + grid) * LINES)
    grid_ref[last, :] += grid_ref[left, :]
    grid_ref[first, :] += grid_ref[right, :]

    def product(matrix, x):
        mh, ml = halves(matrix)
        xh, xl = halves(x)
        rhs = jnp.concatenate([xh, xl], axis=0).astype(BF16)
        mh, ml = mh.astype(BF16), ml.astype(BF16)
        return bdot(jnp.concatenate([mh, mh], axis=1), rhs) + bdot(
            jnp.concatenate([ml, ml], axis=1), rhs
        )

    def lines(j):
        return pl.ds(side * LINES + j, grid, stride=LINES)

    lower = lax.broadcasted_iota(jnp.int32, (grid, grid), 1) < kept

    def folded(j):
        x = grid_ref[lines(j), :]
        return x + pltpu.roll(x, kept, 1)

    charge = jnp.concatenate(
        [jnp.where(lower, folded(j), folded(j + ROWS)) for j in range(ROWS)], axis=1
    )
    spectrum = product(rows_ref[...], charge)
    kern_copy.wait()
    weighted = spectrum * kern_ref[...]
    potential = product(cols_ref[...], weighted)
    for j in range(ROWS):
        x = potential[:, j * grid : (j + 1) * grid]
        y = pltpu.roll(x, kept, 1)
        grid_ref[lines(j), :] = jnp.where(lower, x, y)
        grid_ref[lines(j + ROWS), :] = jnp.where(lower, y, x)
    grid_ref[left, :] = grid_ref[last, :]
    grid_ref[right, :] = grid_ref[first, :]
    if closing:
        energy = jnp.sum(spectrum * weighted, axis=0, keepdims=True)
        energy = sum(energy[:, j * grid : (j + 1) * grid] for j in range(ROWS))

    def gather(s, carry):
        if closing:
            pair_part(s, pair_size, wts_ref, near_ref, col_ref, sum_ref)
        value, slope = x_weights(s)
        pieces = [halves(grid_ref[plane(s * blocks + q), :]) for q in range(blocks + REACH)]
        fields = ([], [], [])
        for b in range(blocks):
            g = s * blocks + b
            row = slice(b, b + 1)
            yt, dyt = yt_ref[g, 0:LINES, :], yt_ref[g, LINES : 2 * LINES, :]
            near = pieces[b : b + ORDER]
            high = jnp.concatenate([x[0] for x in near], axis=0).astype(BF16)
            low = jnp.concatenate([x[1] for x in near], axis=0).astype(BF16)
            table = tab[g]
            out = bdot(
                jnp.concatenate([high, low], axis=1),
                jnp.concatenate([table, table[:kept], jnp.zeros_like(table[:kept])], axis=0),
            )
            tiles = [out[k * LINES : (k + 1) * LINES] for k in range(ORDER)]
            f0 = sum(slope[k][row] * tiles[k][:, :TILE] for k in range(ORDER))
            f1 = sum(value[k][row] * tiles[k][:, :TILE] for k in range(ORDER))
            f2 = sum(value[k][row] * tiles[k][:, TILE:] for k in range(ORDER))
            for i, part in enumerate((yt * f0, dyt * f1, yt * f2)):
                fields[i].append(jnp.sum(part, axis=0, keepdims=True))
        for i in range(3):
            out_ref[s, i * blocks : (i + 1) * blocks, :] = jnp.concatenate(fields[i], axis=0)
        return carry

    lax.fori_loop(0, parts, gather, 0)
    if making:
        for s in range(parts):
            for copy in table_copies(s):
                copy.wait()
    if closing:
        for b in range(blocks):
            turned = PAIR_C * sum_ref[b * TILE : (b + 1) * TILE, :].T
            for c in range(3):
                pair_ref[c * blocks + b : c * blocks + b + 1, :] = turned[c : c + 1]
        sums = moment_rows(energy, *known, pair_ref)
        for d in range(parts):
            out_ref[d, 3 * blocks :, :] = sums


def field_call(vec, rows, cols, kern, first=(), tables=(), final=()):
    parts = vec.shape[0]
    grid = rows.shape[0]
    blocks = grid // parts
    mode = (len(first) > 0, len(final) > 0)
    tab_shape = jax.ShapeDtypeStruct((grid, grid, 2 * TILE), BF16)
    yt_shape = jax.ShapeDtypeStruct((grid, 2 * LINES, TILE), F32)
    tables = [near(tables[0]), *tables[1:]] if tables else []
    args = [near(vec), rows, cols, kern, *first, *tables, *final[:5], *map(near, final[5:])]
    specs = [IN_VMEM] * 3 + [IN_HBM] + [IN_VMEM] * len(first)
    if tables:
        specs += [IN_VMEM, IN_HBM, IN_HBM]
    if final:
        specs += [IN_SMEM] * 2 + [IN_VMEM] * (len(final) - 2)
    out_rows = 3 * blocks + (ROWS if final else 0)
    shapes = [pltpu.VMEM((parts, out_rows, TILE), F32)]
    out_specs = [IN_VMEM]
    scratch = [
        pltpu.VMEM(tab_shape.shape, BF16),
        pltpu.SemaphoreType.DMA((parts,)),
        pltpu.VMEM(yt_shape.shape, F32),
        pltpu.SemaphoreType.DMA((parts,)),
        pltpu.VMEM(kern.shape, F32),
        pltpu.SemaphoreType.DMA(()),
        pltpu.VMEM(((grid + REACH) * LINES, grid), F32),
    ]
    if first:
        shapes += [tab_shape, yt_shape]
        out_specs += [IN_HBM, IN_HBM]
    if final:
        shapes.append(pltpu.VMEM((3 * blocks, TILE), F32))
        out_specs.append(IN_VMEM)
        scratch += [
            pltpu.VMEM((blocks + 2 * HALO_BLK, ROWS, TILE), F32),
            pltpu.VMEM((blocks * TILE, ROWS), F32),
            pltpu.VMEM((blocks * TILE, ROWS), F32),
        ]
    return pl.pallas_call(
        lambda *refs: field_kernel(mode, *refs),
        in_specs=specs,
        out_specs=out_specs,
        out_shape=shapes,
        scratch_shapes=scratch,
        name="field",
        **params(1 << 31, 56 << 20),
    )(*args)


def pair_kernel(list_ref, count_ref, rank_ref, left_ref, pos_ref, right_ref, vec_ref, out_ref, acc_ref, near_ref, col_ref):
    blocks = pos_ref.shape[1] // TILE
    near_tiles((rank_ref, left_ref, pos_ref, right_ref), vec_ref, near_ref, col_ref)
    chunk = TILE // 2
    shape = (chunk, TILE)
    ahead = lax.broadcasted_iota(jnp.int32, shape, 1) - lax.broadcasted_iota(jnp.int32, shape, 0)

    def one_block(b, carry):
        for c in range(TILE // chunk):
            home = col_ref[pl.ds(pl.multiple_of(b * TILE + c * chunk, chunk), chunk), :]
            hx = jnp.broadcast_to(home[:, 0:1], shape)
            hy = jnp.broadcast_to(home[:, 1:2], shape)
            hz = jnp.broadcast_to(home[:, 2:3], shape)

            def one_tile(k, sums):
                sx, sy, sz = sums
                j = list_ref[b, k]
                tile = near_ref[j]
                dx, dy, dz = hx - tile[0:1], hy - tile[1:2], hz - tile[2:3]
                vx, vy, vz = tile[3:4], tile[4:5], tile[5:6]
                inverse = lax.rsqrt(dx * dx + dy * dy + dz * dz + 1.0)
                square = inverse * inverse
                itself = ahead == c * chunk - (j - b - HALO_BLK) * TILE
                third = jnp.where(itself, 0.0, inverse * square)
                fifth = (third * square) * (3.0 * (dx * vx + dy * vy + dz * vz))
                return (
                    sx + (third * vx - fifth * dx),
                    sy + (third * vy - fifth * dy),
                    sz + (third * vz - fifth * dz),
                )

            zero = jnp.zeros(shape, F32)
            sums = lax.fori_loop(0, count_ref[b], one_tile, (zero, zero, zero))
            for i in range(3):
                acc_ref[i, c * chunk : (c + 1) * chunk, :] = sums[i]
        for i in range(3):
            out_ref[pl.ds(i * blocks + b, 1), :] = PAIR_C * jnp.sum(acc_ref[i].T, axis=0, keepdims=True)
        return carry

    lax.fori_loop(0, blocks, one_block, 0)


def pair_call(tiles, counts, places, vec):
    rank, left, pos, right = places
    blocks = pos.shape[1] // TILE
    return pl.pallas_call(
        pair_kernel,
        in_specs=[IN_SMEM] * 3 + [IN_VMEM] * 4,
        out_specs=IN_VMEM,
        out_shape=pltpu.VMEM((3 * blocks, TILE), F32),
        scratch_shapes=[
            pltpu.VMEM((3, TILE, TILE), F32),
            pltpu.VMEM((blocks + 2 * HALO_BLK, ROWS, TILE), F32),
            pltpu.VMEM((blocks * TILE, ROWS), F32),
        ],
        name="pair",
        **params(1 << 30),
    )(tiles, counts, rank, left, pos, right, near(vec))


def update_kernel(ret_ref, pair_ref, inv_ref, own_ref, out_ref):
    blocks = inv_ref.shape[0]
    far = jnp.sum(ret_ref[...], axis=0) - pair_ref[...]
    inv = inv_ref[...]
    vec = jnp.concatenate([far[c * blocks : (c + 1) * blocks] / inv for c in range(3)], axis=0)
    own_ref[...] = vec
    for d in range(out_ref.shape[0]):
        out_ref[d] = vec


def update_call(returned, pair, inv):
    parts = returned.shape[0]
    return pl.pallas_call(
        update_kernel,
        in_specs=[IN_VMEM] * 3,
        out_specs=[IN_VMEM] * 2,
        out_shape=[
            pltpu.VMEM(pair.shape, F32),
            pltpu.VMEM((parts,) + pair.shape, F32),
        ],
        name="update",
        **params(1 << 24),
    )(near(returned), near(pair), near(inv))


def finish_kernel(ret_ref, pair_ref, v0_ref, v1_ref, v2_ref, inv_ref, dip_ref, res_ref):
    blocks = inv_ref.shape[0]
    summed = jnp.sum(ret_ref[...], axis=0)
    total = jnp.sum(summed[3 * blocks :], axis=1, keepdims=True)
    h = summed[: 3 * blocks] - pair_ref[...]
    m = [total[k : k + 1, 0:1] for k in range(6)]
    s = [lax.rsqrt(m[2 * i]) for i in range(3)]
    g = [[m[i + j] * s[i] * s[j] for j in range(3)] for i in range(3)]
    b = [-m[i + 3] * s[i] for i in range(3)]
    l10 = g[1][0] / g[0][0]
    l20 = g[2][0] / g[0][0]
    p11 = g[1][1] - l10 * g[0][1]
    p12 = g[1][2] - l10 * g[0][2]
    l21 = p12 / p11
    p22 = g[2][2] - l20 * g[0][2] - l21 * p12
    b1 = b[1] - l10 * b[0]
    b2 = b[2] - l20 * b[0] - l21 * b1
    y2 = b2 / p22
    y1 = (b1 - p12 * y2) / p11
    y0 = (b[0] - g[0][1] * y1 - g[0][2] * y2) / g[0][0]
    a0, a1, a2 = s[0] * y0, s[1] * y1, s[2] * y2
    scale = 1.0 / (a0 - a1 + a2 - 1.0)
    a0, a1, a2, a3 = a0 * scale, a1 * scale, a2 * scale, scale
    c2 = -a3
    c1 = a3 - a2
    c0 = a2 - a3 - a1
    ip = jnp.concatenate([inv_ref[...]] * 3, axis=0)
    v0, v1, v2 = v0_ref[...], v1_ref[...], v2_ref[...]
    dip = c0 * v0 + c1 * v1 + c2 * v2
    res = ip * (a0 * v0 + a1 * v1 + a2 * v2) + a3 * h
    for c in range(3):
        for b in range(blocks):
            row = slice(c * blocks + b, c * blocks + b + 1)
            here = slice(b * TILE, (b + 1) * TILE)
            dip_ref[c : c + 1, here] = dip[row]
            res_ref[c : c + 1, here] = res[row]


def finish_call(returned, pair, vectors, inv):
    atoms = inv.shape[0] * TILE
    return pl.pallas_call(
        finish_kernel,
        in_specs=[IN_VMEM] * 6,
        out_specs=[IN_VMEM] * 2,
        out_shape=[jax.ShapeDtypeStruct((3, atoms), F32)] * 2,
        name="finish",
        **params(1 << 24),
    )(*map(near, (returned, pair, *vectors, inv)))


def fourier_matrix(size):
    freq = np.arange(size)
    mode = np.where(freq <= size // 2, freq, freq - size // 2)
    angle = (mode[:, None] * np.arange(size)[None, :] % size) * (2.0 * np.pi / size)
    rows = np.where((freq <= size // 2)[:, None], np.cos(angle), np.sin(angle))
    return rows.astype(np.float32)


def kernel_lines(x_axis, y_axis, z_axis):
    mode_sq = x_axis[0] * x_axis[0] + y_axis[0] * y_axis[0] + z_axis[0] * z_axis[0]
    safe_sq = jnp.where(mode_sq > 0, mode_sq, 1.0)
    green = jnp.where(mode_sq > 0, RECIP_C * jnp.exp(-DAMP * safe_sq) / safe_sq, 0.0)
    return green * x_axis[1] * y_axis[1] * z_axis[1]


def swap(x):
    return lax.all_to_all(x, "gx", split_axis=0, concat_axis=0, tiled=True)


def per_device_modes(positions, field, inv_polar, x_spline, yz_spline, tile_list, tile_count):
    parts = lax.axis_size("gx")
    rank = lax.axis_index("gx")
    atoms = positions.shape[1]
    halo = HALO_BLK * TILE
    blocks = atoms // TILE
    up = [(i, (i + 1) % parts) for i in range(parts)]
    down = [(j, i) for i, j in up]

    own, inv, packed = pack_call(
        field, inv_polar[None, :], x_spline.transpose(1, 0, 2), yz_spline, parts
    )
    everyone = swap(packed)
    edges, everyone = lax.optimization_barrier((positions, everyone))
    left = lax.ppermute(edges[:, atoms - halo :], "gx", up)
    right = lax.ppermute(edges[:, :halo], "gx", down)

    offsets = jnp.arange(SPAN, dtype=jnp.int32)
    block_ids = jnp.arange(blocks, dtype=jnp.int32)
    live = jnp.arange(tile_list.shape[1], dtype=jnp.int32)[None, :] < tile_count[:, None]
    hit = tile_list[:, :, None] == block_ids[:, None, None] + offsets[None, None, :]
    wts = jnp.sum((hit & live[:, :, None]).astype(F32), axis=1).reshape(-1)

    matrix = fourier_matrix(GRID)
    rows, cols = jnp.asarray(matrix), jnp.asarray(matrix.T)
    all_freq = jnp.arange(GRID, dtype=jnp.int32)
    kept = GRID // 2
    ky_freq = rank // 2 * LINES + jnp.arange(LINES, dtype=jnp.int32)
    kz_freq = rank % 2 * kept + jnp.arange(kept, dtype=jnp.int32)
    z_rows = lax.dynamic_slice_in_dim(rows, rank % 2 * kept, kept, 0)
    full_modes, full_weights = mode_of(all_freq, GRID)
    ky_modes, ky_weights = mode_of(ky_freq, GRID)
    kz_modes, kz_weights = mode_of(kz_freq, GRID)

    def paired_lines(x):
        x = x.reshape(1, 2, ROWS, 1)
        x = jnp.broadcast_to(x.transpose(0, 2, 1, 3), (1, ROWS, 2, kept))
        return x.reshape(1, ROWS * GRID)

    def repeated(x):
        return jnp.tile(x[None, :], (1, LINES))

    kern = kernel_lines(
        (full_modes[:, None], full_weights[:, None]),
        (paired_lines(ky_modes), paired_lines(ky_weights)),
        (repeated(kz_modes), repeated(kz_weights)),
    )
    steps = jnp.arange(1, ORDER).astype(F32)
    angle = steps[:, None] * ky_modes[None, :] * (2.0 * jnp.pi / GRID)
    sine = (ky_freq > GRID // 2).astype(F32)
    turns = jnp.concatenate([ky_modes[None], sine[None], jnp.cos(angle), jnp.sin(angle)])
    turns = jnp.pad(turns.T, ((0, 0), (0, TILE - turns.shape[0])))

    partial, table, yt = field_call(everyone, rows, cols, kern, first=(z_rows, turns))
    tables = (everyone, table, yt)
    places = (rank[None].astype(jnp.int32), left, positions, right)
    vec, vectors = everyone, [own]
    for step in range(ITERS):
        last = step + 1 == ITERS
        if last:
            final = (wts, *places, *vectors, inv)
            partial, pair = field_call(vec, rows, cols, kern, tables=tables, final=final)
        elif step > 0:
            (partial,) = field_call(vec, rows, cols, kern, tables=tables)
        returned = swap(partial)
        if not last:
            pair = pair_call(tile_list, tile_count, places, vec)
            own, packed = update_call(returned, pair, inv)
            vectors.append(own)
            vec = swap(packed)
    dipoles, residual = finish_call(returned, pair, vectors, inv)
    return (dipoles, residual)


def per_device(positions, *others):
    parts = lax.axis_size("gx")
    atoms = positions.shape[1]
    planes = GRID // parts
    modes = (
        parts * ROWS == GRID
        and atoms == planes * TILE
        and planes == ROWS
        and atoms >= HALO_BLK * TILE
        and ORDER == 5
        and atoms % parts == 0
        and (atoms // parts) % 32 == 0
        and TILE % (atoms // parts) == 0
        and ITERS == 3
    )
    run = per_device_modes if modes else per_device_general
    return run(positions, *others)


def solution(mesh):
    placed = (
        P(None, ("rep", "gx")),
        P(None, ("rep", "gx")),
        P(("rep", "gx")),
        P(None, None, ("rep", "gx")),
        P(None, ("rep", "gx"), None),
        P(("rep", "gx"), None),
        P(("rep", "gx")),
    )
    return jax.shard_map(
        per_device,
        mesh=mesh,
        in_specs=placed,
        out_specs=(P(None, ("rep", "gx")), P(None, ("rep", "gx"))),
        check_vma=False,
    )
```

```python
import jax
import numpy as np
import jax.numpy as jnp
from jax import lax
from jax.experimental import pallas as pl
from jax.experimental.pallas import tpu as pltpu
from jax.sharding import PartitionSpec as P

GRID = 128
ORDER = 5
TILE = 128
HALO_BLK = 3
ITERS = 3


PAIR_C = 0.025
RECIP_C = 8192.0
DAMP = 0.0008
EXACT = lax.Precision.HIGHEST


def extended(x, sides, width):
    for axis, dim in sides:
        devices, length = (lax.axis_size(axis), x.shape[dim])
        up = [(i, (i + 1) % devices) for i in range(devices)]
        down = [(j, i) for i, j in up]
        last = lax.slice_in_dim(x, length - width, length, axis=dim)
        first = lax.slice_in_dim(x, 0, width, axis=dim)
        before = lax.ppermute(last, axis, up)
        after = lax.ppermute(first, axis, down)
        x = jnp.concatenate([before, x, after], axis=dim)
    return x


def pair_field(home_pos, ext_pos, ext_vec, tile_rows, live_counts):
    slab_blocks = home_pos.shape[1] // TILE
    ext_blocks = ext_pos.shape[1] // TILE
    home_blocks = home_pos.reshape(3, slab_blocks, TILE).transpose(1, 0, 2)
    pos_blocks = ext_pos.reshape(3, ext_blocks, TILE)
    vec_blocks = ext_vec.reshape(3, ext_blocks, TILE)
    slot_index = jnp.arange(tile_rows.shape[1], dtype=jnp.int32)
    self_pair = jnp.eye(TILE, dtype=bool)

    def one_block(carried, scan_item):
        home_block, tile_row, live_count, block_index = scan_item
        near_pos = jnp.take(pos_blocks, tile_row, axis=1)
        near_vec = jnp.take(vec_blocks, tile_row, axis=1)
        offsets = home_block[:, None, :, None] - near_pos[:, :, None, :]
        distance_sq = jnp.sum(offsets * offsets, axis=0) + 1.0
        inverse = lax.rsqrt(distance_sq)
        third_power = inverse * inverse * inverse
        fifth_power = third_power * inverse * inverse
        same_block = (tile_row == block_index + HALO_BLK)[:, None, None]
        live_mask = (slot_index < live_count)[:, None, None] & ~(same_block & self_pair[None])
        third_power = jnp.where(live_mask, third_power, 0.0)
        fifth_power = jnp.where(live_mask, fifth_power, 0.0)
        projection = jnp.sum(offsets * near_vec[:, :, None, :], axis=0)
        field_sum = jnp.sum(
            third_power[None] * near_vec[:, :, None, :]
            - 3.0 * (fifth_power * projection)[None] * offsets,
            axis=(1, 3),
        )
        return (carried, PAIR_C * field_sum)

    block_ids = jnp.arange(slab_blocks, dtype=jnp.int32)
    _, blocks_out = lax.scan(
        one_block, jnp.zeros((), jnp.float32), (home_blocks, tile_rows, live_counts, block_ids)
    )
    return blocks_out.transpose(1, 0, 2).reshape(3, slab_blocks * TILE)


def slab_weights(local_plane, x_spline, planes):
    spline_steps = jnp.arange(ORDER, dtype=jnp.int32)
    plane_index = jnp.arange(planes, dtype=jnp.int32)
    matches = local_plane[None, :, None] + spline_steps[:, None, None] == plane_index[None, None, :]
    spline_value = jnp.sum(jnp.where(matches, x_spline[0][:, :, None], 0.0), axis=0)
    spline_slope = jnp.sum(jnp.where(matches, x_spline[1][:, :, None], 0.0), axis=0)
    return (spline_value, spline_slope)


def spread_dipoles(vector, spline_value, spline_slope, yz_spline):
    atoms_here = spline_value.shape[0]
    planes = spline_value.shape[1]
    grid_lines = yz_spline.shape[2]
    lead_terms = (vector[0][:, None] * spline_slope)[:, :, None] * yz_spline[0][:, None, :]
    lead_terms = (
        lead_terms + (vector[1][:, None] * spline_value)[:, :, None] * yz_spline[1][:, None, :]
    )
    tail_terms = (vector[2][:, None] * spline_value)[:, :, None] * yz_spline[0][:, None, :]
    contract = (((0,), (0,)), ((), ()))
    charge = lax.dot_general(
        lead_terms.reshape(atoms_here, planes * grid_lines), yz_spline[2], contract, precision=EXACT
    )
    charge = charge + lax.dot_general(
        tail_terms.reshape(atoms_here, planes * grid_lines), yz_spline[3], contract, precision=EXACT
    )
    return charge.reshape(planes, grid_lines, grid_lines)


def gather_field(potential, spline_value, spline_slope, yz_spline):
    planes = potential.shape[0]
    grid_lines = potential.shape[1]
    atoms_here = spline_value.shape[0]
    flat_grid = potential.reshape(planes * grid_lines, grid_lines)
    contract = (((1,), (1,)), ((), ()))
    plain_sum = lax.dot_general(yz_spline[2], flat_grid, contract, precision=EXACT).reshape(
        atoms_here, planes, grid_lines
    )
    tilted_sum = lax.dot_general(yz_spline[3], flat_grid, contract, precision=EXACT).reshape(
        atoms_here, planes, grid_lines
    )
    first_comp = jnp.sum(
        spline_slope[:, :, None] * yz_spline[0][:, None, :] * plain_sum, axis=(1, 2)
    )
    second_comp = jnp.sum(
        spline_value[:, :, None] * yz_spline[1][:, None, :] * plain_sum, axis=(1, 2)
    )
    third_comp = jnp.sum(
        spline_value[:, :, None] * yz_spline[0][:, None, :] * tilted_sum, axis=(1, 2)
    )
    return jnp.stack([first_comp, second_comp, third_comp])


def mode_of(freq, size):
    half_size = size // 2
    mode_num = jnp.where(freq <= half_size, freq, freq - half_size)
    weight = jnp.where((freq == 0) | (freq == half_size), 1.0 / size, 2.0 / size)
    return (mode_num.astype(jnp.float32), weight.astype(jnp.float32))


def basis_rows(size, points):
    freq = jnp.arange(size, dtype=jnp.int32)
    half_size = size // 2
    mode_num = jnp.where(freq <= half_size, freq, freq - half_size)
    phase = mode_num[:, None] * points[None, :] % size
    angle = phase.astype(jnp.float32) * (2.0 * jnp.pi / size)
    return jnp.where((freq <= half_size)[:, None], jnp.cos(angle), jnp.sin(angle))


def kernel_block(x_modes, x_weights, y_modes, y_weights, z_modes, z_weights):
    mode_sq = (
        x_modes[:, None, None] * x_modes[:, None, None]
        + y_modes[None, :, None] * y_modes[None, :, None]
        + z_modes[None, None, :] * z_modes[None, None, :]
    )
    safe_sq = jnp.where(mode_sq > 0, mode_sq, 1.0)
    green = jnp.where(mode_sq > 0, RECIP_C * jnp.exp(-DAMP * safe_sq) / safe_sq, 0.0)
    return green * x_weights[:, None, None] * y_weights[None, :, None] * z_weights[None, None, :]


def forward_lines(charge, fourier_rows):
    along_z = jnp.einsum("pyz,kz->pyk", charge, fourier_rows, precision=EXACT)
    return jnp.einsum("jy,pyk->pjk", fourier_rows, along_z, precision=EXACT)


def inverse_lines(spectrum, fourier_rows):
    along_z = jnp.einsum("pjk,kz->pjz", spectrum, fourier_rows, precision=EXACT)
    return jnp.einsum("jy,pjz->pyz", fourier_rows, along_z, precision=EXACT)


def per_device_general(positions, field, inv_polar, x_spline, yz_spline, tile_list, tile_count):
    rank_count = lax.axis_size("gx")
    rank_index = lax.axis_index("gx")
    atoms_here = positions.shape[1]
    planes = GRID // rank_count
    extent = planes + 4
    halo_atoms = HALO_BLK * TILE
    slab_blocks = atoms_here // TILE
    local_plane = jnp.arange(atoms_here, dtype=jnp.int32) * planes // atoms_here
    spline_value, spline_slope = slab_weights(local_plane, x_spline, extent)
    ext_pos = extended(positions, (("gx", 1),), halo_atoms)
    shift_x = jnp.concatenate(
        [
            jnp.full((halo_atoms,), -1.0 * slab_blocks, jnp.float32),
            jnp.zeros((atoms_here,), jnp.float32),
            jnp.full((halo_atoms,), 1.0 * slab_blocks, jnp.float32),
        ]
    )
    ext_pos = ext_pos.at[0].add(shift_x)
    fourier_rows = basis_rows(GRID, jnp.arange(GRID, dtype=jnp.int32))
    ky_count = GRID // rank_count
    all_freq = jnp.arange(GRID, dtype=jnp.int32)
    ky_freq = rank_index * ky_count + jnp.arange(ky_count, dtype=jnp.int32)
    full_modes, full_weights = mode_of(all_freq, GRID)
    ky_modes, ky_weights = mode_of(ky_freq, GRID)
    kernel = kernel_block(full_modes, full_weights, ky_modes, ky_weights, full_modes, full_weights)
    kernel = kernel.reshape(GRID, ky_count * GRID)
    source_rows = jnp.arange(rank_count * extent, dtype=jnp.int32)
    points = (source_rows // extent * planes - 2 + source_rows % extent) % GRID
    across = basis_rows(GRID, points)

    def reciprocal(charge):
        spectrum = forward_lines(charge, fourier_rows)
        pencils = lax.all_to_all(spectrum, "gx", split_axis=1, concat_axis=0, tiled=True)
        rows_in = pencils.shape[0]
        flat_pencils = pencils.reshape(rows_in, ky_count * GRID)
        spectral_lines = jnp.dot(across, flat_pencils, precision=EXACT) * kernel
        returned_lines = lax.dot_general(
            across, spectral_lines, (((0,), (0,)), ((), ())), precision=EXACT
        )
        returned = lax.all_to_all(
            returned_lines.reshape(rows_in, ky_count, GRID),
            "gx",
            split_axis=0,
            concat_axis=1,
            tiled=True,
        )
        return inverse_lines(returned, fourier_rows)

    def apply(vector):
        ext_vec = extended(vector, (("gx", 1),), halo_atoms)
        near_field = pair_field(positions, ext_pos, ext_vec, tile_list, tile_count)
        charge = spread_dipoles(vector, spline_value, spline_slope, yz_spline)
        far_field = gather_field(reciprocal(charge), spline_value, spline_slope, yz_spline)
        return inv_polar[None, :] * vector + far_field - near_field

    def paired(residual, precond, applied):
        return lax.psum((jnp.sum(residual * precond), jnp.sum(applied * precond)), "gx")

    dipoles = jnp.zeros_like(field)
    residual = field
    precond = field / inv_polar[None, :]
    applied = apply(precond)
    rz_now, curvature = paired(residual, precond, applied)
    step_size = rz_now / curvature
    direction = precond
    applied_dir = applied
    for sweep_index in range(ITERS):
        dipoles = dipoles + step_size * direction
        residual = residual - step_size * applied_dir
        if sweep_index + 1 < ITERS:
            precond = residual / inv_polar[None, :]
            applied = apply(precond)
            rz_next, curvature = paired(residual, precond, applied)
            beta_ratio = rz_next / rz_now
            step_size = rz_next / (curvature - beta_ratio * rz_next / step_size)
            direction = precond + beta_ratio * direction
            applied_dir = applied + beta_ratio * applied_dir
            rz_now = rz_next
    return (dipoles, residual)


F32 = jnp.float32
BF16 = jnp.bfloat16
ROWS = 8
LINES = 2 * ROWS
IN_VMEM = pl.BlockSpec(memory_space=pltpu.VMEM)
IN_SMEM = pl.BlockSpec(memory_space=pltpu.SMEM)
IN_HBM = pl.BlockSpec(memory_space=pl.ANY)
REACH = ORDER - 1
SPAN = 2 * HALO_BLK + 1
PACKED = 6
NT = (((1,), (1,)), ((), ()))


def near(x):
    return pltpu.with_memory_space_constraint(x, pltpu.VMEM)


def params(flops, vmem=None):
    return dict(
        cost_estimate=pl.CostEstimate(flops=flops, bytes_accessed=4 << 20, transcendentals=0),
        compiler_params=pltpu.CompilerParams(vmem_limit_bytes=vmem) if vmem else None,
    )


def halves(x):
    high = x.astype(BF16).astype(F32)
    return high, x - high


def bdot(a, b):
    return jnp.dot(a, b, preferred_element_type=F32)


def spline_values(u):
    w = 1.0 - u
    u2, w2 = u * u, w * w
    c = 1.0 / 24.0
    return [
        c * (w2 * w2),
        c * (11.0 + u * (-12.0 + u * (-6.0 + u * (12.0 - 4.0 * u)))),
        c * (11.0 + u * (12.0 + u * (-6.0 + u * (-12.0 + 6.0 * u)))),
        c * (1.0 + u * (4.0 + u * (6.0 + u * (4.0 - 4.0 * u)))),
        c * (u2 * u2),
    ]


def spline_slopes(u):
    w = 1.0 - u
    c = 1.0 / 6.0
    return [
        -c * (w * w * w),
        c * (-3.0 + u * (-3.0 + u * (9.0 - 4.0 * u))),
        c * (3.0 + u * (-3.0 + u * (-9.0 + 6.0 * u))),
        c * (1.0 + u * (3.0 + u * (3.0 - 4.0 * u))),
        c * (u * u * u),
    ]


def block_rows(ref, row):
    return jnp.concatenate(
        [ref[row : row + 1, b * TILE : (b + 1) * TILE] for b in range(ref.shape[1] // TILE)], axis=0
    )


def pack_kernel(field_ref, ip_ref, xs_ref, yz_ref, own_ref, inv_ref, out_ref):
    parts = out_ref.shape[0]
    blocks = field_ref.shape[1] // TILE
    grid = yz_ref.shape[2]
    inv = block_rows(ip_ref, 0)
    inv_ref[...] = inv
    tiles = [block_rows(field_ref, c) / inv for c in range(3)]
    for c in range(3):
        own_ref[c * blocks : (c + 1) * blocks, :] = tiles[c]
    tiles.append(sum(float(k) * block_rows(xs_ref.at[k], 0) for k in range(1, ORDER)) - 1.5)
    line = lax.broadcasted_iota(jnp.int32, (grid, TILE), 0)
    for axis in range(2):
        spots = []
        for b in range(blocks):
            here = slice(b * TILE, (b + 1) * TILE)
            value = yz_ref[2 * axis, here, :].T
            slope = yz_ref[2 * axis + 1, here, :].T
            used = jnp.where((value != 0.0) | (slope != 0.0), 1.0, 0.0)
            first = used * (1.0 - pltpu.roll(used, 1, 0))
            start = jnp.sum(first * line.astype(F32), axis=0, keepdims=True)
            offset = (line - start.astype(jnp.int32)) & (grid - 1)
            shift = jnp.sum(value * offset.astype(F32), axis=0, keepdims=True) - 1.5
            spots.append((start - float(grid // 2)) + shift)
        tiles.append(jnp.concatenate(spots, axis=0))
    for d in range(parts):
        for i, tile in enumerate(tiles):
            out_ref[d, i * blocks : (i + 1) * blocks, :] = tile


def pack_call(field, inv_row, xs, yz, parts):
    blocks = field.shape[1] // TILE
    return pl.pallas_call(
        pack_kernel,
        in_specs=[IN_VMEM] * 4,
        out_specs=[IN_VMEM] * 3,
        out_shape=[
            pltpu.VMEM((3 * blocks, TILE), F32),
            pltpu.VMEM((blocks, TILE), F32),
            pltpu.VMEM((parts, PACKED * blocks, TILE), F32),
        ],
        name="pack",
        **params(1 << 26),
    )(field, inv_row, xs, yz)


def table_maker(atom_ref, rows_ref, turn_ref, tab_ref, yt_ref):
    slabs = atom_ref.shape[0]
    blocks = tab_ref.shape[0] // slabs
    kept, grid = rows_ref.shape
    high, low = halves(rows_ref[...])
    twice = jnp.concatenate([high, low], axis=0).astype(BF16)
    matrix = jnp.concatenate([twice, twice], axis=1)
    packed = (LINES, TILE)
    line = lax.broadcasted_iota(jnp.int32, (grid, TILE), 0).astype(F32).astype(BF16)
    lines = [line[c * LINES : (c + 1) * LINES] for c in range(grid // LINES)]
    turn = [jnp.broadcast_to(turn_ref[:, c : c + 1], packed) for c in range(2 * ORDER)]
    half = float(grid // 2)

    def spread_row(x, b):
        return jnp.broadcast_to(x[b : b + 1], packed).astype(BF16)

    def one_slab(slab):
        def located(i):
            place = atom_ref[slab, i * blocks : (i + 1) * blocks, :]
            start = jnp.floor(place)
            u = place - start
            return start, spline_values(u), spline_slopes(u)

        start, values, slopes = located(5)
        start = start.astype(jnp.int32) + grid // 2
        spots = [((start + k) & (grid - 1)).astype(F32) for k in range(ORDER)]
        pieces = [halves(x) for x in values], [halves(x) for x in slopes]
        for b in range(blocks):
            at = [spread_row(x, b) for x in spots]
            tables = []
            for part in range(2):
                columns = []
                for kind in range(2):
                    rows = [spread_row(x[part], b) for x in pieces[kind]]
                    column = []
                    for here in lines:
                        dense = jnp.zeros(packed, BF16)
                        for k in range(ORDER):
                            dense = jnp.where(here == at[k], rows[k], dense)
                        column.append(dense)
                    columns.append(jnp.concatenate(column, axis=0))
                tables.append(jnp.concatenate(columns, axis=1))
            both = bdot(matrix, jnp.concatenate(tables, axis=0))
            high, low = halves(both[:kept] + both[kept:])
            tab_ref[slab * blocks + b] = jnp.concatenate([high, low], axis=0).astype(BF16)
        start, values, slopes = located(4)
        mode, sine = turn[0], turn[1]
        for b in range(blocks):
            row = slice(b, b + 1)
            phase = mode * start[row]
            phase = phase - 2.0 * half * jnp.floor(phase * (0.5 / half) + 0.5)
            angle = phase * (jnp.pi / (4.0 * half))
            sq = angle * angle
            s = angle * (1.0 + sq * (-1.0 / 6 + sq * (1.0 / 120 + sq * (-1.0 / 5040 + sq / 362880))))
            c = 1.0 + sq * (-0.5 + sq * (1.0 / 24 + sq * (-1.0 / 720 + sq / 40320)))
            for _ in range(2):
                s, c = 2.0 * s * c, 1.0 - 2.0 * s * s
            lead = jnp.where(sine > 0.0, s, c)
            side = jnp.where(sine > 0.0, -c, s)
            for i, weights in enumerate((values, slopes)):
                even = weights[0][row] + sum(weights[k][row] * turn[1 + k] for k in range(1, ORDER))
                odd = sum(weights[k][row] * turn[ORDER + k] for k in range(1, ORDER))
                yt_ref[slab * blocks + b, i * LINES : (i + 1) * LINES, :] = lead * even - side * odd

    return one_slab


def near_tiles(refs, vec_ref, near_ref, col_ref):
    rank_ref, pos_ref = refs
    blocks = pos_ref.shape[1] // TILE - 2 * HALO_BLK
    total = vec_ref.shape[0] * blocks
    for j in range(blocks + 2 * HALO_BLK):
        i = j - HALO_BLK
        g = rank_ref[0] * blocks + i
        if i < 0:
            g = jnp.where(g < 0, g + total, g)
        elif i >= blocks:
            g = jnp.where(g >= total, g - total, g)
        near_ref[j, 0:3, :] = pos_ref[:, j * TILE : (j + 1) * TILE]
        src = lax.shift_right_logical(g, 3)
        block = g & (ROWS - 1)
        for c in range(3):
            near_ref[j, 3 + c : 4 + c, :] = vec_ref[src, pl.ds(c * blocks + block, 1), :]
        near_ref[j, 6:8, :] = jnp.zeros((2, TILE), F32)
    for b in range(blocks):
        col_ref[b * TILE : (b + 1) * TILE, :] = near_ref[HALO_BLK + b].T


def pair_part(part, size, wts_ref, near_ref, col_ref, sum_ref):
    first = part * size
    b = lax.shift_right_logical(first, 7)
    chunk = min(size, 32)
    shape = (chunk, TILE)
    lane = lax.broadcasted_iota(jnp.int32, shape, 1)
    ahead = lane - lax.broadcasted_iota(jnp.int32, shape, 0)
    for c in range(size // chunk):
        start = pl.multiple_of(first + c * chunk, chunk)
        home = col_ref[pl.ds(start, chunk), :]
        hx = jnp.broadcast_to(home[:, 0:1], shape)
        hy = jnp.broadcast_to(home[:, 1:2], shape)
        hz = jnp.broadcast_to(home[:, 2:3], shape)
        sx = sy = sz = jnp.zeros(shape, F32)
        for e in range(SPAN):
            tile = near_ref[b + e]
            dx, dy, dz = hx - tile[0:1], hy - tile[1:2], hz - tile[2:3]
            vx, vy, vz = tile[3:4], tile[4:5], tile[5:6]
            inverse = lax.rsqrt(dx * dx + dy * dy + dz * dz + 1.0)
            square = inverse * inverse
            third = wts_ref[b * SPAN + e] * (inverse * square)
            if e == HALO_BLK:
                third = jnp.where(ahead == start - b * TILE, 0.0, third)
            wx, wy, wz = 3.0 * vx, 3.0 * vy, 3.0 * vz
            fifth = (third * square) * (dx * wx + dy * wy + dz * wz)
            sx = sx + (third * vx - fifth * dx)
            sy = sy + (third * vy - fifth * dy)
            sz = sz + (third * vz - fifth * dz)
        sums = [jnp.sum(x, axis=1, keepdims=True) for x in (sx, sy, sz)]
        both = jnp.where(lane == 0, sums[0], jnp.where(lane == 1, sums[1], sums[2]))
        sum_ref[pl.ds(start, chunk), :] = both[:, :ROWS]


def moment_rows(energy, v0_ref, v1_ref, v2_ref, inv_ref, pair_ref):
    ip = jnp.concatenate([inv_ref[...]] * 3, axis=0)
    v0, v1, v2 = v0_ref[...], v1_ref[...], v2_ref[...]
    d1, d2 = ip * v1, ip * v2
    terms = [v0 * (ip * v0), v0 * d1, v1 * d1, v1 * d2, v2 * d2, -(v2 * pair_ref[...])]
    rows = [jnp.sum(term, axis=0, keepdims=True) for term in terms]
    rows[5] = rows[5] + energy
    blank = jnp.zeros((ROWS - len(rows), TILE), F32)
    return jnp.concatenate(rows + [blank], axis=0)


def field_kernel(mode, *refs):
    making, closing = mode
    v_ref, rows_ref, cols_ref, kern_ref, *refs = refs
    if making:
        z_ref, turn_ref, out_ref, tab_hbm, yt_hbm, *refs = refs
        atom_ref = v_ref
    elif closing:
        atom_ref, tab_hbm, yt_hbm, wts_ref, *refs = refs
        places, known, refs = refs[:2], refs[2:6], refs[6:]
        out_ref, pair_ref, *refs = refs
    else:
        atom_ref, tab_hbm, yt_hbm, out_ref, *refs = refs
    tab, sem, yt_ref, yt_sem, grid_ref, *refs = refs
    parts = out_ref.shape[0]
    grid = rows_ref.shape[0]
    blocks = tab.shape[0] // parts
    width = LINES * ORDER
    kept = grid // 2

    def table_copies(s):
        part = pl.ds(s * blocks, blocks)
        ends = [(yt_hbm.at[part], yt_ref.at[part]), (tab_hbm.at[part], tab.at[part])]
        if making:
            ends = [(here, there) for there, here in ends]
        return [
            pltpu.make_async_copy(ends[0][0], ends[0][1], yt_sem.at[s]),
            pltpu.make_async_copy(ends[1][0], ends[1][1], sem.at[s]),
        ]

    if not making:
        for s in range(parts):
            for copy in table_copies(s):
                copy.start()
    grid_ref[...] = jnp.zeros(grid_ref.shape, F32)
    if making:
        make_tables = table_maker(atom_ref, z_ref, turn_ref, tab, yt_ref)
    if closing:
        near_ref, col_ref, sum_ref = refs
        near_tiles(places, v_ref, near_ref, col_ref)
        pair_size = blocks * TILE // parts

    def plane(q):
        return pl.ds(pl.multiple_of(q * LINES, LINES), LINES)

    def x_weights(s):
        u = atom_ref[s, 3 * blocks : 4 * blocks, :]
        return spline_values(u), spline_slopes(u)

    def spread(s, carry):
        if making:
            make_tables(s)
        for copy in table_copies(s):
            copy.start() if making else copy.wait()
        value, slope = x_weights(s)
        vec = [v_ref[s, c * blocks : (c + 1) * blocks, :] for c in range(3)]
        a0 = [vec[0] * slope[k] for k in range(ORDER)]
        a1 = [vec[1] * value[k] for k in range(ORDER)]
        a2 = [vec[2] * value[k] for k in range(ORDER)]
        sums = [jnp.zeros((LINES, grid), F32) for _ in range(blocks + REACH)]
        for b in range(blocks):
            g = s * blocks + b
            row = slice(b, b + 1)
            yt, dyt = yt_ref[g, 0:LINES, :], yt_ref[g, LINES : 2 * LINES, :]
            lead = jnp.concatenate([a0[k][row] * yt + a1[k][row] * dyt for k in range(ORDER)], axis=0)
            tail = jnp.concatenate([a2[k][row] * yt for k in range(ORDER)], axis=0)
            high, low = halves(jnp.concatenate([lead, tail], axis=1))
            lhs = jnp.concatenate([high, low], axis=0).astype(BF16)
            out = lax.dot_general(lhs, tab[g], NT, preferred_element_type=F32)
            out = out[:width] + out[width:]
            for k in range(ORDER):
                sums[b + k] = sums[b + k] + out[k * LINES : (k + 1) * LINES]
        for j, tile in enumerate(sums):
            grid_ref[plane(s * blocks + j), :] += tile
        return carry

    lax.fori_loop(0, parts, spread, 0)
    side = REACH // 2
    left, right = slice(0, side * LINES), slice((side + grid) * LINES, (2 * side + grid) * LINES)
    first = slice(side * LINES, 2 * side * LINES)
    last = slice(grid * LINES, (side + grid) * LINES)
    grid_ref[last, :] += grid_ref[left, :]
    grid_ref[first, :] += grid_ref[right, :]

    def product(matrix, x):
        mh, ml = halves(matrix)
        xh, xl = halves(x)
        rhs = jnp.concatenate([xh, xl], axis=0).astype(BF16)
        mh, ml = mh.astype(BF16), ml.astype(BF16)
        return bdot(jnp.concatenate([mh, mh], axis=1), rhs) + bdot(
            jnp.concatenate([ml, ml], axis=1), rhs
        )

    def lines(j):
        return pl.ds(side * LINES + j, grid, stride=LINES)

    lower = lax.broadcasted_iota(jnp.int32, (grid, grid), 1) < kept

    def folded(j):
        x = grid_ref[lines(j), :]
        return x + pltpu.roll(x, kept, 1)

    charge = jnp.concatenate(
        [jnp.where(lower, folded(j), folded(j + ROWS)) for j in range(ROWS)], axis=1
    )
    spectrum = product(rows_ref[...], charge)
    weighted = spectrum * kern_ref[...]
    potential = product(cols_ref[...], weighted)
    for j in range(ROWS):
        x = potential[:, j * grid : (j + 1) * grid]
        y = pltpu.roll(x, kept, 1)
        grid_ref[lines(j), :] = jnp.where(lower, x, y)
        grid_ref[lines(j + ROWS), :] = jnp.where(lower, y, x)
    grid_ref[left, :] = grid_ref[last, :]
    grid_ref[right, :] = grid_ref[first, :]
    if closing:
        energy = jnp.sum(spectrum * weighted, axis=0, keepdims=True)
        energy = sum(energy[:, j * grid : (j + 1) * grid] for j in range(ROWS))

    def gather(s, carry):
        if closing:
            pair_part(s, pair_size, wts_ref, near_ref, col_ref, sum_ref)
        value, slope = x_weights(s)
        pieces = [halves(grid_ref[plane(s * blocks + q), :]) for q in range(blocks + REACH)]
        fields = ([], [], [])
        for b in range(blocks):
            g = s * blocks + b
            row = slice(b, b + 1)
            yt, dyt = yt_ref[g, 0:LINES, :], yt_ref[g, LINES : 2 * LINES, :]
            near = pieces[b : b + ORDER]
            high = jnp.concatenate([x[0] for x in near], axis=0).astype(BF16)
            low = jnp.concatenate([x[1] for x in near], axis=0).astype(BF16)
            table = tab[g]
            out = bdot(
                jnp.concatenate([high, low], axis=1),
                jnp.concatenate([table, table[:kept], jnp.zeros_like(table[:kept])], axis=0),
            )
            tiles = [out[k * LINES : (k + 1) * LINES] for k in range(ORDER)]
            f0 = sum(slope[k][row] * tiles[k][:, :TILE] for k in range(ORDER))
            f1 = sum(value[k][row] * tiles[k][:, :TILE] for k in range(ORDER))
            f2 = sum(value[k][row] * tiles[k][:, TILE:] for k in range(ORDER))
            for i, part in enumerate((yt * f0, dyt * f1, yt * f2)):
                fields[i].append(jnp.sum(part, axis=0, keepdims=True))
        for i in range(3):
            out_ref[s, i * blocks : (i + 1) * blocks, :] = jnp.concatenate(fields[i], axis=0)
        return carry

    lax.fori_loop(0, parts, gather, 0)
    if making:
        for s in range(parts):
            for copy in table_copies(s):
                copy.wait()
    if closing:
        for b in range(blocks):
            turned = PAIR_C * sum_ref[b * TILE : (b + 1) * TILE, :].T
            for c in range(3):
                pair_ref[c * blocks + b : c * blocks + b + 1, :] = turned[c : c + 1]
        sums = moment_rows(energy, *known, pair_ref)
        for d in range(parts):
            out_ref[d, 3 * blocks :, :] = sums


def field_call(vec, rows, cols, kern, first=(), tables=(), final=()):
    parts = vec.shape[0]
    grid = rows.shape[0]
    blocks = grid // parts
    mode = (len(first) > 0, len(final) > 0)
    tab_shape = jax.ShapeDtypeStruct((grid, grid, 2 * TILE), BF16)
    yt_shape = jax.ShapeDtypeStruct((grid, 2 * LINES, TILE), F32)
    tables = [near(tables[0]), *tables[1:]] if tables else []
    first = [near(x) for x in first]
    args = [near(vec), near(rows), near(cols), near(kern), *first, *tables, *final[:2], *map(near, final[2:])]
    specs = [IN_VMEM] * (4 + len(first))
    if tables:
        specs += [IN_VMEM, IN_HBM, IN_HBM]
    if final:
        specs += [IN_SMEM] * 2 + [IN_VMEM] * (len(final) - 2)
    out_rows = 3 * blocks + (ROWS if final else 0)
    shapes = [pltpu.VMEM((parts, out_rows, TILE), F32)]
    out_specs = [IN_VMEM]
    scratch = [
        pltpu.VMEM(tab_shape.shape, BF16),
        pltpu.SemaphoreType.DMA((parts,)),
        pltpu.VMEM(yt_shape.shape, F32),
        pltpu.SemaphoreType.DMA((parts,)),
        pltpu.VMEM(((grid + REACH) * LINES, grid), F32),
    ]
    if first:
        shapes += [tab_shape, yt_shape]
        out_specs += [IN_HBM, IN_HBM]
    if final:
        shapes.append(pltpu.VMEM((3 * blocks, TILE), F32))
        out_specs.append(IN_VMEM)
        scratch += [
            pltpu.VMEM((blocks + 2 * HALO_BLK, ROWS, TILE), F32),
            pltpu.VMEM((blocks * TILE, ROWS), F32),
            pltpu.VMEM((blocks * TILE, ROWS), F32),
        ]
    return pl.pallas_call(
        lambda *refs: field_kernel(mode, *refs),
        in_specs=specs,
        out_specs=out_specs,
        out_shape=shapes,
        scratch_shapes=scratch,
        name="field",
        **params(1 << 31, 56 << 20),
    )(*args)


def pair_kernel(list_ref, count_ref, rank_ref, pos_ref, vec_ref, out_ref, acc_ref, near_ref, col_ref):
    blocks = out_ref.shape[0] // 3
    near_tiles((rank_ref, pos_ref), vec_ref, near_ref, col_ref)
    chunk = TILE // 2
    shape = (chunk, TILE)
    ahead = lax.broadcasted_iota(jnp.int32, shape, 1) - lax.broadcasted_iota(jnp.int32, shape, 0)

    def one_block(b, carry):
        for c in range(TILE // chunk):
            home = col_ref[pl.ds(pl.multiple_of(b * TILE + c * chunk, chunk), chunk), :]
            hx = jnp.broadcast_to(home[:, 0:1], shape)
            hy = jnp.broadcast_to(home[:, 1:2], shape)
            hz = jnp.broadcast_to(home[:, 2:3], shape)

            def one_tile(k, sums):
                sx, sy, sz = sums
                j = list_ref[b, k]
                tile = near_ref[j]
                dx, dy, dz = hx - tile[0:1], hy - tile[1:2], hz - tile[2:3]
                vx, vy, vz = tile[3:4], tile[4:5], tile[5:6]
                wx, wy, wz = 3.0 * vx, 3.0 * vy, 3.0 * vz
                inverse = lax.rsqrt(dx * dx + dy * dy + dz * dz + 1.0)
                square = inverse * inverse
                itself = ahead == c * chunk - (j - b - HALO_BLK) * TILE
                third = jnp.where(itself, 0.0, inverse * square)
                fifth = (third * square) * (dx * wx + dy * wy + dz * wz)
                return (
                    sx + (third * vx - fifth * dx),
                    sy + (third * vy - fifth * dy),
                    sz + (third * vz - fifth * dz),
                )

            zero = jnp.zeros(shape, F32)
            sums = lax.fori_loop(0, count_ref[b], one_tile, (zero, zero, zero))
            for i in range(3):
                acc_ref[i, c * chunk : (c + 1) * chunk, :] = sums[i]
        for i in range(3):
            out_ref[pl.ds(i * blocks + b, 1), :] = PAIR_C * jnp.sum(acc_ref[i].T, axis=0, keepdims=True)
        return carry

    lax.fori_loop(0, blocks, one_block, 0)


def pair_call(tiles, counts, places, vec):
    rank, pos = places
    blocks = pos.shape[1] // TILE - 2 * HALO_BLK
    return pl.pallas_call(
        pair_kernel,
        in_specs=[IN_SMEM] * 3 + [IN_VMEM] * 2,
        out_specs=IN_VMEM,
        out_shape=pltpu.VMEM((3 * blocks, TILE), F32),
        scratch_shapes=[
            pltpu.VMEM((3, TILE, TILE), F32),
            pltpu.VMEM((blocks + 2 * HALO_BLK, ROWS, TILE), F32),
            pltpu.VMEM((blocks * TILE, ROWS), F32),
        ],
        name="pair",
        **params(1 << 30),
    )(tiles, counts, rank, near(pos), near(vec))


def update_kernel(ret_ref, pair_ref, inv_ref, own_ref, out_ref):
    blocks = inv_ref.shape[0]
    far = jnp.sum(ret_ref[...], axis=0) - pair_ref[...]
    inv = inv_ref[...]
    vec = jnp.concatenate([far[c * blocks : (c + 1) * blocks] / inv for c in range(3)], axis=0)
    own_ref[...] = vec
    for d in range(out_ref.shape[0]):
        out_ref[d] = vec


def update_call(returned, pair, inv):
    parts = returned.shape[0]
    return pl.pallas_call(
        update_kernel,
        in_specs=[IN_VMEM] * 3,
        out_specs=[IN_VMEM] * 2,
        out_shape=[
            pltpu.VMEM(pair.shape, F32),
            pltpu.VMEM((parts,) + pair.shape, F32),
        ],
        name="update",
        **params(1 << 24),
    )(near(returned), near(pair), near(inv))


def finish_kernel(ret_ref, pair_ref, v0_ref, v1_ref, v2_ref, inv_ref, dip_ref, res_ref):
    blocks = inv_ref.shape[0]
    summed = jnp.sum(ret_ref[...], axis=0)
    total = jnp.sum(summed[3 * blocks :], axis=1, keepdims=True)
    h = summed[: 3 * blocks] - pair_ref[...]
    m = [total[k : k + 1, 0:1] for k in range(6)]
    s = [lax.rsqrt(m[2 * i]) for i in range(3)]
    g = [[m[i + j] * s[i] * s[j] for j in range(3)] for i in range(3)]
    b = [-m[i + 3] * s[i] for i in range(3)]
    l10 = g[1][0] / g[0][0]
    l20 = g[2][0] / g[0][0]
    p11 = g[1][1] - l10 * g[0][1]
    p12 = g[1][2] - l10 * g[0][2]
    l21 = p12 / p11
    p22 = g[2][2] - l20 * g[0][2] - l21 * p12
    b1 = b[1] - l10 * b[0]
    b2 = b[2] - l20 * b[0] - l21 * b1
    y2 = b2 / p22
    y1 = (b1 - p12 * y2) / p11
    y0 = (b[0] - g[0][1] * y1 - g[0][2] * y2) / g[0][0]
    a0, a1, a2 = s[0] * y0, s[1] * y1, s[2] * y2
    scale = 1.0 / (a0 - a1 + a2 - 1.0)
    a0, a1, a2, a3 = a0 * scale, a1 * scale, a2 * scale, scale
    c2 = -a3
    c1 = a3 - a2
    c0 = a2 - a3 - a1
    ip = jnp.concatenate([inv_ref[...]] * 3, axis=0)
    v0, v1, v2 = v0_ref[...], v1_ref[...], v2_ref[...]
    dip = c0 * v0 + c1 * v1 + c2 * v2
    res = ip * (a0 * v0 + a1 * v1 + a2 * v2) + a3 * h
    for c in range(3):
        for b in range(blocks):
            row = slice(c * blocks + b, c * blocks + b + 1)
            here = slice(b * TILE, (b + 1) * TILE)
            dip_ref[c : c + 1, here] = dip[row]
            res_ref[c : c + 1, here] = res[row]


def finish_call(returned, pair, vectors, inv):
    atoms = inv.shape[0] * TILE
    return pl.pallas_call(
        finish_kernel,
        in_specs=[IN_VMEM] * 6,
        out_specs=[IN_VMEM] * 2,
        out_shape=[jax.ShapeDtypeStruct((3, atoms), F32)] * 2,
        name="finish",
        **params(1 << 24),
    )(*map(near, (returned, pair, *vectors, inv)))


def fourier_matrix(size):
    freq = np.arange(size)
    mode = np.where(freq <= size // 2, freq, freq - size // 2)
    angle = (mode[:, None] * np.arange(size)[None, :] % size) * (2.0 * np.pi / size)
    rows = np.where((freq <= size // 2)[:, None], np.cos(angle), np.sin(angle))
    return rows.astype(np.float32)


def kernel_lines(x_axis, y_axis, z_axis):
    mode_sq = x_axis[0] * x_axis[0] + y_axis[0] * y_axis[0] + z_axis[0] * z_axis[0]
    safe_sq = jnp.where(mode_sq > 0, mode_sq, 1.0)
    green = jnp.where(mode_sq > 0, RECIP_C * jnp.exp(-DAMP * safe_sq) / safe_sq, 0.0)
    return green * x_axis[1] * y_axis[1] * z_axis[1]


def swap(x):
    return lax.all_to_all(x, "gx", split_axis=0, concat_axis=0, tiled=True)


def per_device_modes(positions, field, inv_polar, x_spline, yz_spline, tile_list, tile_count):
    parts = lax.axis_size("gx")
    rank = lax.axis_index("gx")
    atoms = positions.shape[1]
    halo = HALO_BLK * TILE
    blocks = atoms // TILE
    up = [(i, (i + 1) % parts) for i in range(parts)]
    down = [(j, i) for i, j in up]

    own, inv, packed = pack_call(
        field, inv_polar[None, :], x_spline.transpose(1, 0, 2), yz_spline, parts
    )
    everyone = swap(packed)
    left = lax.ppermute(positions[:, atoms - halo :], "gx", up)
    right = lax.ppermute(positions[:, :halo], "gx", down)
    shift = jnp.where(jnp.arange(3) == 0, 1.0 * blocks, 0.0)[:, None]
    joined = jnp.concatenate([left - shift, positions, right + shift], axis=1)

    offsets = jnp.arange(SPAN, dtype=jnp.int32)
    block_ids = jnp.arange(blocks, dtype=jnp.int32)
    live = jnp.arange(tile_list.shape[1], dtype=jnp.int32)[None, :] < tile_count[:, None]
    hit = tile_list[:, :, None] == block_ids[:, None, None] + offsets[None, None, :]
    wts = jnp.sum((hit & live[:, :, None]).astype(F32), axis=1).reshape(-1)

    matrix = fourier_matrix(GRID)
    rows, cols = jnp.asarray(matrix), jnp.asarray(matrix.T)
    all_freq = jnp.arange(GRID, dtype=jnp.int32)
    kept = GRID // 2
    ky_freq = rank // 2 * LINES + jnp.arange(LINES, dtype=jnp.int32)
    kz_freq = rank % 2 * kept + jnp.arange(kept, dtype=jnp.int32)
    z_rows = lax.dynamic_slice_in_dim(rows, rank % 2 * kept, kept, 0)
    full_modes, full_weights = mode_of(all_freq, GRID)
    ky_modes, ky_weights = mode_of(ky_freq, GRID)
    kz_modes, kz_weights = mode_of(kz_freq, GRID)

    def paired_lines(x):
        x = x.reshape(1, 2, ROWS, 1)
        x = jnp.broadcast_to(x.transpose(0, 2, 1, 3), (1, ROWS, 2, kept))
        return x.reshape(1, ROWS * GRID)

    def repeated(x):
        return jnp.tile(x[None, :], (1, LINES))

    kern = kernel_lines(
        (full_modes[:, None], full_weights[:, None]),
        (paired_lines(ky_modes), paired_lines(ky_weights)),
        (repeated(kz_modes), repeated(kz_weights)),
    )
    steps = jnp.arange(1, ORDER).astype(F32)
    angle = steps[:, None] * ky_modes[None, :] * (2.0 * jnp.pi / GRID)
    sine = (ky_freq > GRID // 2).astype(F32)
    turns = jnp.concatenate([ky_modes[None], sine[None], jnp.cos(angle), jnp.sin(angle)])
    turns = jnp.pad(turns.T, ((0, 0), (0, TILE - turns.shape[0])))

    partial, table, yt = field_call(everyone, rows, cols, kern, first=(z_rows, turns))
    tables = (everyone, table, yt)
    places = (rank[None].astype(jnp.int32), joined)
    vec, vectors = everyone, [own]
    for step in range(ITERS):
        last = step + 1 == ITERS
        if last:
            final = (wts, *places, *vectors, inv)
            partial, pair = field_call(vec, rows, cols, kern, tables=tables, final=final)
        elif step > 0:
            (partial,) = field_call(vec, rows, cols, kern, tables=tables)
        returned = swap(partial)
        if not last:
            pair = pair_call(tile_list, tile_count, places, vec)
            own, packed = update_call(returned, pair, inv)
            vectors.append(own)
            vec = swap(packed)
    dipoles, residual = finish_call(returned, pair, vectors, inv)
    return (dipoles, residual)


def per_device(positions, *others):
    parts = lax.axis_size("gx")
    atoms = positions.shape[1]
    planes = GRID // parts
    modes = (
        parts * ROWS == GRID
        and atoms == planes * TILE
        and planes == ROWS
        and atoms >= HALO_BLK * TILE
        and ORDER == 5
        and atoms % parts == 0
        and (atoms // parts) % 32 == 0
        and TILE % (atoms // parts) == 0
        and ITERS == 3
    )
    run = per_device_modes if modes else per_device_general
    return run(positions, *others)


def solution(mesh):
    placed = (
        P(None, ("rep", "gx")),
        P(None, ("rep", "gx")),
        P(("rep", "gx")),
        P(None, None, ("rep", "gx")),
        P(None, ("rep", "gx"), None),
        P(("rep", "gx"), None),
        P(("rep", "gx")),
    )
    return jax.shard_map(
        per_device,
        mesh=mesh,
        in_specs=placed,
        out_specs=(P(None, ("rep", "gx")), P(None, ("rep", "gx"))),
        check_vma=False,
    )
```

```python
import jax
import numpy as np
import jax.numpy as jnp
from jax import lax
from jax.experimental import pallas as pl
from jax.experimental.pallas import tpu as pltpu
from jax.sharding import PartitionSpec as P

GRID = 128
ORDER = 5
TILE = 128
HALO_BLK = 3
ITERS = 3


PAIR_C = 0.025
RECIP_C = 8192.0
DAMP = 0.0008
EXACT = lax.Precision.HIGHEST


def extended(x, sides, width):
    for axis, dim in sides:
        devices, length = (lax.axis_size(axis), x.shape[dim])
        up = [(i, (i + 1) % devices) for i in range(devices)]
        down = [(j, i) for i, j in up]
        last = lax.slice_in_dim(x, length - width, length, axis=dim)
        first = lax.slice_in_dim(x, 0, width, axis=dim)
        before = lax.ppermute(last, axis, up)
        after = lax.ppermute(first, axis, down)
        x = jnp.concatenate([before, x, after], axis=dim)
    return x


def pair_field(home_pos, ext_pos, ext_vec, tile_rows, live_counts):
    slab_blocks = home_pos.shape[1] // TILE
    ext_blocks = ext_pos.shape[1] // TILE
    home_blocks = home_pos.reshape(3, slab_blocks, TILE).transpose(1, 0, 2)
    pos_blocks = ext_pos.reshape(3, ext_blocks, TILE)
    vec_blocks = ext_vec.reshape(3, ext_blocks, TILE)
    slot_index = jnp.arange(tile_rows.shape[1], dtype=jnp.int32)
    self_pair = jnp.eye(TILE, dtype=bool)

    def one_block(carried, scan_item):
        home_block, tile_row, live_count, block_index = scan_item
        near_pos = jnp.take(pos_blocks, tile_row, axis=1)
        near_vec = jnp.take(vec_blocks, tile_row, axis=1)
        offsets = home_block[:, None, :, None] - near_pos[:, :, None, :]
        distance_sq = jnp.sum(offsets * offsets, axis=0) + 1.0
        inverse = lax.rsqrt(distance_sq)
        third_power = inverse * inverse * inverse
        fifth_power = third_power * inverse * inverse
        same_block = (tile_row == block_index + HALO_BLK)[:, None, None]
        live_mask = (slot_index < live_count)[:, None, None] & ~(same_block & self_pair[None])
        third_power = jnp.where(live_mask, third_power, 0.0)
        fifth_power = jnp.where(live_mask, fifth_power, 0.0)
        projection = jnp.sum(offsets * near_vec[:, :, None, :], axis=0)
        field_sum = jnp.sum(
            third_power[None] * near_vec[:, :, None, :]
            - 3.0 * (fifth_power * projection)[None] * offsets,
            axis=(1, 3),
        )
        return (carried, PAIR_C * field_sum)

    block_ids = jnp.arange(slab_blocks, dtype=jnp.int32)
    _, blocks_out = lax.scan(
        one_block, jnp.zeros((), jnp.float32), (home_blocks, tile_rows, live_counts, block_ids)
    )
    return blocks_out.transpose(1, 0, 2).reshape(3, slab_blocks * TILE)


def slab_weights(local_plane, x_spline, planes):
    spline_steps = jnp.arange(ORDER, dtype=jnp.int32)
    plane_index = jnp.arange(planes, dtype=jnp.int32)
    matches = local_plane[None, :, None] + spline_steps[:, None, None] == plane_index[None, None, :]
    spline_value = jnp.sum(jnp.where(matches, x_spline[0][:, :, None], 0.0), axis=0)
    spline_slope = jnp.sum(jnp.where(matches, x_spline[1][:, :, None], 0.0), axis=0)
    return (spline_value, spline_slope)


def spread_dipoles(vector, spline_value, spline_slope, yz_spline):
    atoms_here = spline_value.shape[0]
    planes = spline_value.shape[1]
    grid_lines = yz_spline.shape[2]
    lead_terms = (vector[0][:, None] * spline_slope)[:, :, None] * yz_spline[0][:, None, :]
    lead_terms = (
        lead_terms + (vector[1][:, None] * spline_value)[:, :, None] * yz_spline[1][:, None, :]
    )
    tail_terms = (vector[2][:, None] * spline_value)[:, :, None] * yz_spline[0][:, None, :]
    contract = (((0,), (0,)), ((), ()))
    charge = lax.dot_general(
        lead_terms.reshape(atoms_here, planes * grid_lines), yz_spline[2], contract, precision=EXACT
    )
    charge = charge + lax.dot_general(
        tail_terms.reshape(atoms_here, planes * grid_lines), yz_spline[3], contract, precision=EXACT
    )
    return charge.reshape(planes, grid_lines, grid_lines)


def gather_field(potential, spline_value, spline_slope, yz_spline):
    planes = potential.shape[0]
    grid_lines = potential.shape[1]
    atoms_here = spline_value.shape[0]
    flat_grid = potential.reshape(planes * grid_lines, grid_lines)
    contract = (((1,), (1,)), ((), ()))
    plain_sum = lax.dot_general(yz_spline[2], flat_grid, contract, precision=EXACT).reshape(
        atoms_here, planes, grid_lines
    )
    tilted_sum = lax.dot_general(yz_spline[3], flat_grid, contract, precision=EXACT).reshape(
        atoms_here, planes, grid_lines
    )
    first_comp = jnp.sum(
        spline_slope[:, :, None] * yz_spline[0][:, None, :] * plain_sum, axis=(1, 2)
    )
    second_comp = jnp.sum(
        spline_value[:, :, None] * yz_spline[1][:, None, :] * plain_sum, axis=(1, 2)
    )
    third_comp = jnp.sum(
        spline_value[:, :, None] * yz_spline[0][:, None, :] * tilted_sum, axis=(1, 2)
    )
    return jnp.stack([first_comp, second_comp, third_comp])


def mode_of(freq, size):
    half_size = size // 2
    mode_num = jnp.where(freq <= half_size, freq, freq - half_size)
    weight = jnp.where((freq == 0) | (freq == half_size), 1.0 / size, 2.0 / size)
    return (mode_num.astype(jnp.float32), weight.astype(jnp.float32))


def basis_rows(size, points):
    freq = jnp.arange(size, dtype=jnp.int32)
    half_size = size // 2
    mode_num = jnp.where(freq <= half_size, freq, freq - half_size)
    phase = mode_num[:, None] * points[None, :] % size
    angle = phase.astype(jnp.float32) * (2.0 * jnp.pi / size)
    return jnp.where((freq <= half_size)[:, None], jnp.cos(angle), jnp.sin(angle))


def kernel_block(x_modes, x_weights, y_modes, y_weights, z_modes, z_weights):
    mode_sq = (
        x_modes[:, None, None] * x_modes[:, None, None]
        + y_modes[None, :, None] * y_modes[None, :, None]
        + z_modes[None, None, :] * z_modes[None, None, :]
    )
    safe_sq = jnp.where(mode_sq > 0, mode_sq, 1.0)
    green = jnp.where(mode_sq > 0, RECIP_C * jnp.exp(-DAMP * safe_sq) / safe_sq, 0.0)
    return green * x_weights[:, None, None] * y_weights[None, :, None] * z_weights[None, None, :]


def forward_lines(charge, fourier_rows):
    along_z = jnp.einsum("pyz,kz->pyk", charge, fourier_rows, precision=EXACT)
    return jnp.einsum("jy,pyk->pjk", fourier_rows, along_z, precision=EXACT)


def inverse_lines(spectrum, fourier_rows):
    along_z = jnp.einsum("pjk,kz->pjz", spectrum, fourier_rows, precision=EXACT)
    return jnp.einsum("jy,pjz->pyz", fourier_rows, along_z, precision=EXACT)


def per_device_general(positions, field, inv_polar, x_spline, yz_spline, tile_list, tile_count):
    rank_count = lax.axis_size("gx")
    rank_index = lax.axis_index("gx")
    atoms_here = positions.shape[1]
    planes = GRID // rank_count
    extent = planes + 4
    halo_atoms = HALO_BLK * TILE
    slab_blocks = atoms_here // TILE
    local_plane = jnp.arange(atoms_here, dtype=jnp.int32) * planes // atoms_here
    spline_value, spline_slope = slab_weights(local_plane, x_spline, extent)
    ext_pos = extended(positions, (("gx", 1),), halo_atoms)
    shift_x = jnp.concatenate(
        [
            jnp.full((halo_atoms,), -1.0 * slab_blocks, jnp.float32),
            jnp.zeros((atoms_here,), jnp.float32),
            jnp.full((halo_atoms,), 1.0 * slab_blocks, jnp.float32),
        ]
    )
    ext_pos = ext_pos.at[0].add(shift_x)
    fourier_rows = basis_rows(GRID, jnp.arange(GRID, dtype=jnp.int32))
    ky_count = GRID // rank_count
    all_freq = jnp.arange(GRID, dtype=jnp.int32)
    ky_freq = rank_index * ky_count + jnp.arange(ky_count, dtype=jnp.int32)
    full_modes, full_weights = mode_of(all_freq, GRID)
    ky_modes, ky_weights = mode_of(ky_freq, GRID)
    kernel = kernel_block(full_modes, full_weights, ky_modes, ky_weights, full_modes, full_weights)
    kernel = kernel.reshape(GRID, ky_count * GRID)
    source_rows = jnp.arange(rank_count * extent, dtype=jnp.int32)
    points = (source_rows // extent * planes - 2 + source_rows % extent) % GRID
    across = basis_rows(GRID, points)

    def reciprocal(charge):
        spectrum = forward_lines(charge, fourier_rows)
        pencils = lax.all_to_all(spectrum, "gx", split_axis=1, concat_axis=0, tiled=True)
        rows_in = pencils.shape[0]
        flat_pencils = pencils.reshape(rows_in, ky_count * GRID)
        spectral_lines = jnp.dot(across, flat_pencils, precision=EXACT) * kernel
        returned_lines = lax.dot_general(
            across, spectral_lines, (((0,), (0,)), ((), ())), precision=EXACT
        )
        returned = lax.all_to_all(
            returned_lines.reshape(rows_in, ky_count, GRID),
            "gx",
            split_axis=0,
            concat_axis=1,
            tiled=True,
        )
        return inverse_lines(returned, fourier_rows)

    def apply(vector):
        ext_vec = extended(vector, (("gx", 1),), halo_atoms)
        near_field = pair_field(positions, ext_pos, ext_vec, tile_list, tile_count)
        charge = spread_dipoles(vector, spline_value, spline_slope, yz_spline)
        far_field = gather_field(reciprocal(charge), spline_value, spline_slope, yz_spline)
        return inv_polar[None, :] * vector + far_field - near_field

    def paired(residual, precond, applied):
        return lax.psum((jnp.sum(residual * precond), jnp.sum(applied * precond)), "gx")

    dipoles = jnp.zeros_like(field)
    residual = field
    precond = field / inv_polar[None, :]
    applied = apply(precond)
    rz_now, curvature = paired(residual, precond, applied)
    step_size = rz_now / curvature
    direction = precond
    applied_dir = applied
    for sweep_index in range(ITERS):
        dipoles = dipoles + step_size * direction
        residual = residual - step_size * applied_dir
        if sweep_index + 1 < ITERS:
            precond = residual / inv_polar[None, :]
            applied = apply(precond)
            rz_next, curvature = paired(residual, precond, applied)
            beta_ratio = rz_next / rz_now
            step_size = rz_next / (curvature - beta_ratio * rz_next / step_size)
            direction = precond + beta_ratio * direction
            applied_dir = applied + beta_ratio * applied_dir
            rz_now = rz_next
    return (dipoles, residual)


F32 = jnp.float32
BF16 = jnp.bfloat16
ROWS = 8
LINES = 2 * ROWS
IN_VMEM = pl.BlockSpec(memory_space=pltpu.VMEM)
IN_SMEM = pl.BlockSpec(memory_space=pltpu.SMEM)
IN_HBM = pl.BlockSpec(memory_space=pl.ANY)
REACH = ORDER - 1
SPAN = 2 * HALO_BLK + 1
PACKED = 6
NT = (((1,), (1,)), ((), ()))


def near(x):
    return pltpu.with_memory_space_constraint(x, pltpu.VMEM)


def params(flops, vmem=None):
    return dict(
        cost_estimate=pl.CostEstimate(flops=flops, bytes_accessed=4 << 20, transcendentals=0),
        compiler_params=pltpu.CompilerParams(vmem_limit_bytes=vmem) if vmem else None,
    )


def halves(x):
    high = x.astype(BF16).astype(F32)
    return high, x - high


def bdot(a, b):
    return jnp.dot(a, b, preferred_element_type=F32)


def spline_values(u):
    w = 1.0 - u
    u2, w2 = u * u, w * w
    c = 1.0 / 24.0
    return [
        c * (w2 * w2),
        c * (11.0 + u * (-12.0 + u * (-6.0 + u * (12.0 - 4.0 * u)))),
        c * (11.0 + u * (12.0 + u * (-6.0 + u * (-12.0 + 6.0 * u)))),
        c * (1.0 + u * (4.0 + u * (6.0 + u * (4.0 - 4.0 * u)))),
        c * (u2 * u2),
    ]


def spline_slopes(u):
    w = 1.0 - u
    c = 1.0 / 6.0
    return [
        -c * (w * w * w),
        c * (-3.0 + u * (-3.0 + u * (9.0 - 4.0 * u))),
        c * (3.0 + u * (-3.0 + u * (-9.0 + 6.0 * u))),
        c * (1.0 + u * (3.0 + u * (3.0 - 4.0 * u))),
        c * (u * u * u),
    ]


def block_rows(ref, row):
    return jnp.concatenate(
        [ref[row : row + 1, b * TILE : (b + 1) * TILE] for b in range(ref.shape[1] // TILE)], axis=0
    )


def pack_kernel(field_ref, ip_ref, xs_ref, yz_ref, own_ref, inv_ref, out_ref):
    parts = out_ref.shape[0]
    blocks = field_ref.shape[1] // TILE
    grid = yz_ref.shape[2]
    inv = block_rows(ip_ref, 0)
    inv_ref[...] = inv
    tiles = [block_rows(field_ref, c) / inv for c in range(3)]
    for c in range(3):
        own_ref[c * blocks : (c + 1) * blocks, :] = tiles[c]
    tiles.append(sum(float(k) * block_rows(xs_ref.at[k], 0) for k in range(1, ORDER)) - 1.5)
    line = lax.broadcasted_iota(jnp.int32, (grid, TILE), 0)
    for axis in range(2):
        spots = []
        for b in range(blocks):
            here = slice(b * TILE, (b + 1) * TILE)
            value = yz_ref[2 * axis, here, :].T
            slope = yz_ref[2 * axis + 1, here, :].T
            used = jnp.where((value != 0.0) | (slope != 0.0), 1.0, 0.0)
            first = used * (1.0 - pltpu.roll(used, 1, 0))
            start = jnp.sum(first * line.astype(F32), axis=0, keepdims=True)
            offset = (line - start.astype(jnp.int32)) & (grid - 1)
            shift = jnp.sum(value * offset.astype(F32), axis=0, keepdims=True) - 1.5
            spots.append((start - float(grid // 2)) + shift)
        tiles.append(jnp.concatenate(spots, axis=0))
    for d in range(parts):
        for i, tile in enumerate(tiles):
            out_ref[d, i * blocks : (i + 1) * blocks, :] = tile


def pack_call(field, inv_row, xs, yz, parts):
    blocks = field.shape[1] // TILE
    return pl.pallas_call(
        pack_kernel,
        in_specs=[IN_VMEM] * 4,
        out_specs=[IN_VMEM] * 3,
        out_shape=[
            pltpu.VMEM((3 * blocks, TILE), F32),
            pltpu.VMEM((blocks, TILE), F32),
            pltpu.VMEM((parts, PACKED * blocks, TILE), F32),
        ],
        name="pack",
        **params(1 << 26),
    )(field, inv_row, xs, yz)


def table_maker(atom_ref, rows_ref, turn_ref, tab_ref, yt_ref):
    slabs = atom_ref.shape[0]
    blocks = tab_ref.shape[0] // slabs
    kept, grid = rows_ref.shape
    high, low = halves(rows_ref[...])
    twice = jnp.concatenate([high, low], axis=0).astype(BF16)
    matrix = jnp.concatenate([twice, twice], axis=1)
    packed = (LINES, TILE)
    line = lax.broadcasted_iota(jnp.int32, (grid, TILE), 0).astype(F32).astype(BF16)
    lines = [line[c * LINES : (c + 1) * LINES] for c in range(grid // LINES)]
    turn = [jnp.broadcast_to(turn_ref[:, c : c + 1], packed) for c in range(2 * ORDER)]
    half = float(grid // 2)

    def spread_row(x, b):
        return jnp.broadcast_to(x[b : b + 1], packed).astype(BF16)

    def one_slab(slab):
        def located(i):
            place = atom_ref[slab, i * blocks : (i + 1) * blocks, :]
            start = jnp.floor(place)
            u = place - start
            return start, spline_values(u), spline_slopes(u)

        start, values, slopes = located(5)
        start = start.astype(jnp.int32) + grid // 2
        spots = [((start + k) & (grid - 1)).astype(F32) for k in range(ORDER)]
        pieces = [halves(x) for x in values], [halves(x) for x in slopes]
        for b in range(blocks):
            at = [spread_row(x, b) for x in spots]
            tables = []
            for part in range(2):
                columns = []
                for kind in range(2):
                    rows = [spread_row(x[part], b) for x in pieces[kind]]
                    column = []
                    for here in lines:
                        dense = jnp.zeros(packed, BF16)
                        for k in range(ORDER):
                            dense = jnp.where(here == at[k], rows[k], dense)
                        column.append(dense)
                    columns.append(jnp.concatenate(column, axis=0))
                tables.append(jnp.concatenate(columns, axis=1))
            both = bdot(matrix, jnp.concatenate(tables, axis=0))
            high, low = halves(both[:kept] + both[kept:])
            tab_ref[slab * blocks + b] = jnp.concatenate([high, low], axis=0).astype(BF16)
        start, values, slopes = located(4)
        mode, sine = turn[0], turn[1]
        for b in range(blocks):
            row = slice(b, b + 1)
            phase = mode * start[row]
            phase = phase - 2.0 * half * jnp.floor(phase * (0.5 / half) + 0.5)
            angle = phase * (jnp.pi / (4.0 * half))
            sq = angle * angle
            s = angle * (1.0 + sq * (-1.0 / 6 + sq * (1.0 / 120 + sq * (-1.0 / 5040 + sq / 362880))))
            c = 1.0 + sq * (-0.5 + sq * (1.0 / 24 + sq * (-1.0 / 720 + sq / 40320)))
            for _ in range(2):
                s, c = 2.0 * s * c, 1.0 - 2.0 * s * s
            lead = jnp.where(sine > 0.0, s, c)
            side = jnp.where(sine > 0.0, -c, s)
            for i, weights in enumerate((values, slopes)):
                even = weights[0][row] + sum(weights[k][row] * turn[1 + k] for k in range(1, ORDER))
                odd = sum(weights[k][row] * turn[ORDER + k] for k in range(1, ORDER))
                yt_ref[slab * blocks + b, i * LINES : (i + 1) * LINES, :] = lead * even - side * odd

    return one_slab


def near_tiles(refs, vec_ref, near_ref, col_ref):
    rank_ref, pos_ref = refs
    blocks = pos_ref.shape[1] // TILE - 2 * HALO_BLK
    total = vec_ref.shape[0] * blocks
    for j in range(blocks + 2 * HALO_BLK):
        i = j - HALO_BLK
        g = rank_ref[0] * blocks + i
        if i < 0:
            g = jnp.where(g < 0, g + total, g)
        elif i >= blocks:
            g = jnp.where(g >= total, g - total, g)
        near_ref[j, 0:3, :] = pos_ref[:, j * TILE : (j + 1) * TILE]
        src = lax.shift_right_logical(g, 3)
        block = g & (ROWS - 1)
        for c in range(3):
            near_ref[j, 3 + c : 4 + c, :] = vec_ref[src, pl.ds(c * blocks + block, 1), :]
        near_ref[j, 6:8, :] = jnp.zeros((2, TILE), F32)
    for b in range(blocks):
        col_ref[b * TILE : (b + 1) * TILE, :] = near_ref[HALO_BLK + b].T


def pair_part(part, size, wts_ref, near_ref, col_ref, sum_ref):
    first = part * size
    b = lax.shift_right_logical(first, 7)
    chunk = min(size, 32)
    shape = (chunk, TILE)
    lane = lax.broadcasted_iota(jnp.int32, shape, 1)
    ahead = lane - lax.broadcasted_iota(jnp.int32, shape, 0)
    for c in range(size // chunk):
        start = pl.multiple_of(first + c * chunk, chunk)
        home = col_ref[pl.ds(start, chunk), :]
        hx = jnp.broadcast_to(home[:, 0:1], shape)
        hy = jnp.broadcast_to(home[:, 1:2], shape)
        hz = jnp.broadcast_to(home[:, 2:3], shape)
        sx = sy = sz = jnp.zeros(shape, F32)
        for e in range(SPAN):
            tile = near_ref[b + e]
            dx, dy, dz = hx - tile[0:1], hy - tile[1:2], hz - tile[2:3]
            vx, vy, vz = tile[3:4], tile[4:5], tile[5:6]
            inverse = lax.rsqrt(dx * dx + dy * dy + dz * dz + 1.0)
            square = inverse * inverse
            third = wts_ref[b * SPAN + e] * (inverse * square)
            if e == HALO_BLK:
                third = jnp.where(ahead == start - b * TILE, 0.0, third)
            wx, wy, wz = 3.0 * vx, 3.0 * vy, 3.0 * vz
            fifth = (third * square) * (dx * wx + dy * wy + dz * wz)
            sx = sx + (third * vx - fifth * dx)
            sy = sy + (third * vy - fifth * dy)
            sz = sz + (third * vz - fifth * dz)
        sums = [jnp.sum(x, axis=1, keepdims=True) for x in (sx, sy, sz)]
        both = jnp.where(lane == 0, sums[0], jnp.where(lane == 1, sums[1], sums[2]))
        sum_ref[pl.ds(start, chunk), :] = both[:, :ROWS]


def moment_rows(energy, v0_ref, v1_ref, v2_ref, inv_ref, pair_ref):
    ip = jnp.concatenate([inv_ref[...]] * 3, axis=0)
    v0, v1, v2 = v0_ref[...], v1_ref[...], v2_ref[...]
    d1, d2 = ip * v1, ip * v2
    terms = [v0 * (ip * v0), v0 * d1, v1 * d1, v1 * d2, v2 * d2, -(v2 * pair_ref[...])]
    rows = [jnp.sum(term, axis=0, keepdims=True) for term in terms]
    rows[5] = rows[5] + energy
    blank = jnp.zeros((ROWS - len(rows), TILE), F32)
    return jnp.concatenate(rows + [blank], axis=0)


def field_kernel(mode, *refs):
    making, closing = mode
    v_ref, rows_ref, cols_ref, kern_ref, *refs = refs
    if making:
        z_ref, turn_ref, out_ref, tab_hbm, yt_hbm, *refs = refs
        atom_ref = v_ref
    elif closing:
        atom_ref, tab_hbm, yt_hbm, wts_ref, *refs = refs
        places, known, refs = refs[:2], refs[2:6], refs[6:]
        out_ref, pair_ref, *refs = refs
    else:
        atom_ref, tab_hbm, yt_hbm, out_ref, *refs = refs
    tab, sem, yt_ref, yt_sem, grid_ref, *refs = refs
    parts = out_ref.shape[0]
    grid = rows_ref.shape[0]
    blocks = tab.shape[0] // parts
    width = LINES * ORDER
    kept = grid // 2

    def table_copies(s):
        part = pl.ds(s * blocks, blocks)
        ends = [(yt_hbm.at[part], yt_ref.at[part]), (tab_hbm.at[part], tab.at[part])]
        if making:
            ends = [(here, there) for there, here in ends]
        return [
            pltpu.make_async_copy(ends[0][0], ends[0][1], yt_sem.at[s]),
            pltpu.make_async_copy(ends[1][0], ends[1][1], sem.at[s]),
        ]

    if not making:
        for s in range(parts):
            for copy in table_copies(s):
                copy.start()
    grid_ref[...] = jnp.zeros(grid_ref.shape, F32)
    if making:
        make_tables = table_maker(atom_ref, z_ref, turn_ref, tab, yt_ref)
    if closing:
        near_ref, col_ref, sum_ref = refs
        near_tiles(places, v_ref, near_ref, col_ref)
        pair_size = blocks * TILE // (2 * parts)

    def plane(q):
        return pl.ds(pl.multiple_of(q * LINES, LINES), LINES)

    def x_weights(s):
        u = atom_ref[s, 3 * blocks : 4 * blocks, :]
        return spline_values(u), spline_slopes(u)

    def spread(s, carry):
        if making:
            make_tables(s)
        for copy in table_copies(s):
            copy.start() if making else copy.wait()
        value, slope = x_weights(s)
        if closing:
            pair_part(2 * s, pair_size, wts_ref, near_ref, col_ref, sum_ref)
        vec = [v_ref[s, c * blocks : (c + 1) * blocks, :] for c in range(3)]
        a0 = [vec[0] * slope[k] for k in range(ORDER)]
        a1 = [vec[1] * value[k] for k in range(ORDER)]
        a2 = [vec[2] * value[k] for k in range(ORDER)]
        sums = [jnp.zeros((LINES, grid), F32) for _ in range(blocks + REACH)]
        for b in range(blocks):
            g = s * blocks + b
            row = slice(b, b + 1)
            yt, dyt = yt_ref[g, 0:LINES, :], yt_ref[g, LINES : 2 * LINES, :]
            lead = jnp.concatenate([a0[k][row] * yt + a1[k][row] * dyt for k in range(ORDER)], axis=0)
            tail = jnp.concatenate([a2[k][row] * yt for k in range(ORDER)], axis=0)
            high, low = halves(jnp.concatenate([lead, tail], axis=1))
            lhs = jnp.concatenate([high, low], axis=0).astype(BF16)
            out = lax.dot_general(lhs, tab[g], NT, preferred_element_type=F32)
            out = out[:width] + out[width:]
            for k in range(ORDER):
                sums[b + k] = sums[b + k] + out[k * LINES : (k + 1) * LINES]
        for j, tile in enumerate(sums):
            grid_ref[plane(s * blocks + j), :] += tile
        return carry

    lax.fori_loop(0, parts, spread, 0)
    side = REACH // 2
    left, right = slice(0, side * LINES), slice((side + grid) * LINES, (2 * side + grid) * LINES)
    first = slice(side * LINES, 2 * side * LINES)
    last = slice(grid * LINES, (side + grid) * LINES)
    grid_ref[last, :] += grid_ref[left, :]
    grid_ref[first, :] += grid_ref[right, :]

    def product(matrix, x):
        mh, ml = halves(matrix)
        xh, xl = halves(x)
        rhs = jnp.concatenate([xh, xl], axis=0).astype(BF16)
        mh, ml = mh.astype(BF16), ml.astype(BF16)
        return bdot(jnp.concatenate([mh, mh], axis=1), rhs) + bdot(
            jnp.concatenate([ml, ml], axis=1), rhs
        )

    def lines(j):
        return pl.ds(side * LINES + j, grid, stride=LINES)

    lower = lax.broadcasted_iota(jnp.int32, (grid, grid), 1) < kept

    def folded(j):
        x = grid_ref[lines(j), :]
        return x + pltpu.roll(x, kept, 1)

    energies = []
    for group in range(ROWS // 2):
        pair = (2 * group, 2 * group + 1)
        columns = slice(pair[0] * grid, (pair[1] + 1) * grid)
        charge = jnp.concatenate(
            [jnp.where(lower, folded(j), folded(j + ROWS)) for j in pair], axis=1
        )
        spectrum = product(rows_ref[...], charge)
        weighted = spectrum * kern_ref[:, columns]
        potential = product(cols_ref[...], weighted)
        for i, j in enumerate(pair):
            x = potential[:, i * grid : (i + 1) * grid]
            y = pltpu.roll(x, kept, 1)
            grid_ref[lines(j), :] = jnp.where(lower, x, y)
            grid_ref[lines(j + ROWS), :] = jnp.where(lower, y, x)
        if closing:
            energies.append(jnp.sum(spectrum * weighted, axis=0, keepdims=True))
    grid_ref[left, :] = grid_ref[last, :]
    grid_ref[right, :] = grid_ref[first, :]
    if closing:
        energy = sum(x[:, i * grid : (i + 1) * grid] for x in energies for i in range(2))

    def gather(s, carry):
        if closing:
            pair_part(2 * s + 1, pair_size, wts_ref, near_ref, col_ref, sum_ref)
        value, slope = x_weights(s)
        pieces = [halves(grid_ref[plane(s * blocks + q), :]) for q in range(blocks + REACH)]
        fields = ([], [], [])
        for b in range(blocks):
            g = s * blocks + b
            row = slice(b, b + 1)
            yt, dyt = yt_ref[g, 0:LINES, :], yt_ref[g, LINES : 2 * LINES, :]
            near = pieces[b : b + ORDER]
            high = jnp.concatenate([x[0] for x in near], axis=0).astype(BF16)
            low = jnp.concatenate([x[1] for x in near], axis=0).astype(BF16)
            table = tab[g]
            out = bdot(
                jnp.concatenate([high, low[:, :kept]], axis=1),
                jnp.concatenate([table, table[:kept]], axis=0),
            )
            tiles = [out[k * LINES : (k + 1) * LINES] for k in range(ORDER)]
            f0 = sum(slope[k][row] * tiles[k][:, :TILE] for k in range(ORDER))
            f1 = sum(value[k][row] * tiles[k][:, :TILE] for k in range(ORDER))
            f2 = sum(value[k][row] * tiles[k][:, TILE:] for k in range(ORDER))
            for i, part in enumerate((yt * f0, dyt * f1, yt * f2)):
                fields[i].append(jnp.sum(part, axis=0, keepdims=True))
        for i in range(3):
            out_ref[s, i * blocks : (i + 1) * blocks, :] = jnp.concatenate(fields[i], axis=0)
        return carry

    lax.fori_loop(0, parts, gather, 0)
    if making:
        for s in range(parts):
            for copy in table_copies(s):
                copy.wait()
    if closing:
        for b in range(blocks):
            turned = PAIR_C * sum_ref[b * TILE : (b + 1) * TILE, :].T
            for c in range(3):
                pair_ref[c * blocks + b : c * blocks + b + 1, :] = turned[c : c + 1]
        sums = moment_rows(energy, *known, pair_ref)
        for d in range(parts):
            out_ref[d, 3 * blocks :, :] = sums


def field_call(vec, rows, cols, kern, first=(), tables=(), final=()):
    parts = vec.shape[0]
    grid = rows.shape[0]
    blocks = grid // parts
    mode = (len(first) > 0, len(final) > 0)
    tab_shape = jax.ShapeDtypeStruct((grid, grid, 2 * TILE), BF16)
    yt_shape = jax.ShapeDtypeStruct((grid, 2 * LINES, TILE), F32)
    tables = [near(tables[0]), *tables[1:]] if tables else []
    first = [near(x) for x in first]
    args = [near(vec), near(rows), near(cols), near(kern), *first, *tables, *final[:2], *map(near, final[2:])]
    specs = [IN_VMEM] * (4 + len(first))
    if tables:
        specs += [IN_VMEM, IN_HBM, IN_HBM]
    if final:
        specs += [IN_SMEM] * 2 + [IN_VMEM] * (len(final) - 2)
    out_rows = 3 * blocks + (ROWS if final else 0)
    shapes = [pltpu.VMEM((parts, out_rows, TILE), F32)]
    out_specs = [IN_VMEM]
    scratch = [
        pltpu.VMEM(tab_shape.shape, BF16),
        pltpu.SemaphoreType.DMA((parts,)),
        pltpu.VMEM(yt_shape.shape, F32),
        pltpu.SemaphoreType.DMA((parts,)),
        pltpu.VMEM(((grid + REACH) * LINES, grid), F32),
    ]
    if first:
        shapes += [tab_shape, yt_shape]
        out_specs += [IN_HBM, IN_HBM]
    if final:
        shapes.append(pltpu.VMEM((3 * blocks, TILE), F32))
        out_specs.append(IN_VMEM)
        scratch += [
            pltpu.VMEM((blocks + 2 * HALO_BLK, ROWS, TILE), F32),
            pltpu.VMEM((blocks * TILE, ROWS), F32),
            pltpu.VMEM((blocks * TILE, ROWS), F32),
        ]
    return pl.pallas_call(
        lambda *refs: field_kernel(mode, *refs),
        in_specs=specs,
        out_specs=out_specs,
        out_shape=shapes,
        scratch_shapes=scratch,
        name="field",
        **params(1 << 31, 56 << 20),
    )(*args)


def pair_kernel(list_ref, count_ref, rank_ref, pos_ref, vec_ref, out_ref, acc_ref, near_ref, col_ref):
    blocks = out_ref.shape[0] // 3
    near_tiles((rank_ref, pos_ref), vec_ref, near_ref, col_ref)
    chunk = TILE // 2
    shape = (chunk, TILE)
    ahead = lax.broadcasted_iota(jnp.int32, shape, 1) - lax.broadcasted_iota(jnp.int32, shape, 0)

    def one_block(b, carry):
        for c in range(TILE // chunk):
            home = col_ref[pl.ds(pl.multiple_of(b * TILE + c * chunk, chunk), chunk), :]
            hx = jnp.broadcast_to(home[:, 0:1], shape)
            hy = jnp.broadcast_to(home[:, 1:2], shape)
            hz = jnp.broadcast_to(home[:, 2:3], shape)

            def one_tile(k, sums):
                sx, sy, sz = sums
                j = list_ref[b, k]
                tile = near_ref[j]
                dx, dy, dz = hx - tile[0:1], hy - tile[1:2], hz - tile[2:3]
                vx, vy, vz = tile[3:4], tile[4:5], tile[5:6]
                wx, wy, wz = 3.0 * vx, 3.0 * vy, 3.0 * vz
                inverse = lax.rsqrt(dx * dx + dy * dy + dz * dz + 1.0)
                square = inverse * inverse
                itself = ahead == c * chunk - (j - b - HALO_BLK) * TILE
                third = jnp.where(itself, 0.0, inverse * square)
                fifth = (third * square) * (dx * wx + dy * wy + dz * wz)
                return (
                    sx + (third * vx - fifth * dx),
                    sy + (third * vy - fifth * dy),
                    sz + (third * vz - fifth * dz),
                )

            zero = jnp.zeros(shape, F32)
            sums = lax.fori_loop(0, count_ref[b], one_tile, (zero, zero, zero))
            for i in range(3):
                acc_ref[i, c * chunk : (c + 1) * chunk, :] = sums[i]
        for i in range(3):
            out_ref[pl.ds(i * blocks + b, 1), :] = PAIR_C * jnp.sum(acc_ref[i].T, axis=0, keepdims=True)
        return carry

    lax.fori_loop(0, blocks, one_block, 0)


def pair_call(tiles, counts, places, vec):
    rank, pos = places
    blocks = pos.shape[1] // TILE - 2 * HALO_BLK
    return pl.pallas_call(
        pair_kernel,
        in_specs=[IN_SMEM] * 3 + [IN_VMEM] * 2,
        out_specs=IN_VMEM,
        out_shape=pltpu.VMEM((3 * blocks, TILE), F32),
        scratch_shapes=[
            pltpu.VMEM((3, TILE, TILE), F32),
            pltpu.VMEM((blocks + 2 * HALO_BLK, ROWS, TILE), F32),
            pltpu.VMEM((blocks * TILE, ROWS), F32),
        ],
        name="pair",
        **params(1 << 30),
    )(tiles, counts, rank, near(pos), near(vec))


def update_kernel(ret_ref, pair_ref, inv_ref, own_ref, out_ref):
    blocks = inv_ref.shape[0]
    far = jnp.sum(ret_ref[...], axis=0) - pair_ref[...]
    inv = inv_ref[...]
    vec = jnp.concatenate([far[c * blocks : (c + 1) * blocks] / inv for c in range(3)], axis=0)
    own_ref[...] = vec
    for d in range(out_ref.shape[0]):
        out_ref[d] = vec


def update_call(returned, pair, inv):
    parts = returned.shape[0]
    return pl.pallas_call(
        update_kernel,
        in_specs=[IN_VMEM] * 3,
        out_specs=[IN_VMEM] * 2,
        out_shape=[
            pltpu.VMEM(pair.shape, F32),
            pltpu.VMEM((parts,) + pair.shape, F32),
        ],
        name="update",
        **params(1 << 24),
    )(near(returned), near(pair), near(inv))


def finish_kernel(ret_ref, pair_ref, v0_ref, v1_ref, v2_ref, inv_ref, dip_ref, res_ref):
    blocks = inv_ref.shape[0]
    summed = jnp.sum(ret_ref[...], axis=0)
    total = jnp.sum(summed[3 * blocks :], axis=1, keepdims=True)
    h = summed[: 3 * blocks] - pair_ref[...]
    m = [total[k : k + 1, 0:1] for k in range(6)]
    s = [lax.rsqrt(m[2 * i]) for i in range(3)]
    g = [[m[i + j] * s[i] * s[j] for j in range(3)] for i in range(3)]
    b = [-m[i + 3] * s[i] for i in range(3)]
    l10 = g[1][0] / g[0][0]
    l20 = g[2][0] / g[0][0]
    p11 = g[1][1] - l10 * g[0][1]
    p12 = g[1][2] - l10 * g[0][2]
    l21 = p12 / p11
    p22 = g[2][2] - l20 * g[0][2] - l21 * p12
    b1 = b[1] - l10 * b[0]
    b2 = b[2] - l20 * b[0] - l21 * b1
    y2 = b2 / p22
    y1 = (b1 - p12 * y2) / p11
    y0 = (b[0] - g[0][1] * y1 - g[0][2] * y2) / g[0][0]
    a0, a1, a2 = s[0] * y0, s[1] * y1, s[2] * y2
    scale = 1.0 / (a0 - a1 + a2 - 1.0)
    a0, a1, a2, a3 = a0 * scale, a1 * scale, a2 * scale, scale
    c2 = -a3
    c1 = a3 - a2
    c0 = a2 - a3 - a1
    ip = jnp.concatenate([inv_ref[...]] * 3, axis=0)
    v0, v1, v2 = v0_ref[...], v1_ref[...], v2_ref[...]
    dip = c0 * v0 + c1 * v1 + c2 * v2
    res = ip * (a0 * v0 + a1 * v1 + a2 * v2) + a3 * h
    for c in range(3):
        for b in range(blocks):
            row = slice(c * blocks + b, c * blocks + b + 1)
            here = slice(b * TILE, (b + 1) * TILE)
            dip_ref[c : c + 1, here] = dip[row]
            res_ref[c : c + 1, here] = res[row]


def finish_call(returned, pair, vectors, inv):
    atoms = inv.shape[0] * TILE
    return pl.pallas_call(
        finish_kernel,
        in_specs=[IN_VMEM] * 6,
        out_specs=[IN_VMEM] * 2,
        out_shape=[jax.ShapeDtypeStruct((3, atoms), F32)] * 2,
        name="finish",
        **params(1 << 24),
    )(*map(near, (returned, pair, *vectors, inv)))


def fourier_matrix(size):
    freq = np.arange(size)
    mode = np.where(freq <= size // 2, freq, freq - size // 2)
    angle = (mode[:, None] * np.arange(size)[None, :] % size) * (2.0 * np.pi / size)
    rows = np.where((freq <= size // 2)[:, None], np.cos(angle), np.sin(angle))
    return rows.astype(np.float32)


def kernel_lines(x_axis, y_axis, z_axis):
    mode_sq = x_axis[0] * x_axis[0] + y_axis[0] * y_axis[0] + z_axis[0] * z_axis[0]
    safe_sq = jnp.where(mode_sq > 0, mode_sq, 1.0)
    green = jnp.where(mode_sq > 0, RECIP_C * jnp.exp(-DAMP * safe_sq) / safe_sq, 0.0)
    return green * x_axis[1] * y_axis[1] * z_axis[1]


def swap(x):
    return lax.all_to_all(x, "gx", split_axis=0, concat_axis=0, tiled=True)


def per_device_modes(positions, field, inv_polar, x_spline, yz_spline, tile_list, tile_count):
    parts = lax.axis_size("gx")
    rank = lax.axis_index("gx")
    atoms = positions.shape[1]
    halo = HALO_BLK * TILE
    blocks = atoms // TILE
    up = [(i, (i + 1) % parts) for i in range(parts)]
    down = [(j, i) for i, j in up]

    own, inv, packed = pack_call(
        field, inv_polar[None, :], x_spline.transpose(1, 0, 2), yz_spline, parts
    )
    everyone = swap(packed)
    left = lax.ppermute(positions[:, atoms - halo :], "gx", up)
    right = lax.ppermute(positions[:, :halo], "gx", down)
    shift = jnp.where(jnp.arange(3) == 0, 1.0 * blocks, 0.0)[:, None]
    joined = jnp.concatenate([left - shift, positions, right + shift], axis=1)

    offsets = jnp.arange(SPAN, dtype=jnp.int32)
    block_ids = jnp.arange(blocks, dtype=jnp.int32)
    live = jnp.arange(tile_list.shape[1], dtype=jnp.int32)[None, :] < tile_count[:, None]
    hit = tile_list[:, :, None] == block_ids[:, None, None] + offsets[None, None, :]
    wts = jnp.sum((hit & live[:, :, None]).astype(F32), axis=1).reshape(-1)

    matrix = fourier_matrix(GRID)
    rows, cols = jnp.asarray(matrix), jnp.asarray(matrix.T)
    all_freq = jnp.arange(GRID, dtype=jnp.int32)
    kept = GRID // 2
    ky_freq = rank // 2 * LINES + jnp.arange(LINES, dtype=jnp.int32)
    kz_freq = rank % 2 * kept + jnp.arange(kept, dtype=jnp.int32)
    z_rows = lax.dynamic_slice_in_dim(rows, rank % 2 * kept, kept, 0)
    full_modes, full_weights = mode_of(all_freq, GRID)
    ky_modes, ky_weights = mode_of(ky_freq, GRID)
    kz_modes, kz_weights = mode_of(kz_freq, GRID)

    def paired_lines(x):
        x = x.reshape(1, 2, ROWS, 1)
        x = jnp.broadcast_to(x.transpose(0, 2, 1, 3), (1, ROWS, 2, kept))
        return x.reshape(1, ROWS * GRID)

    def repeated(x):
        return jnp.tile(x[None, :], (1, LINES))

    kern = kernel_lines(
        (full_modes[:, None], full_weights[:, None]),
        (paired_lines(ky_modes), paired_lines(ky_weights)),
        (repeated(kz_modes), repeated(kz_weights)),
    )
    steps = jnp.arange(1, ORDER).astype(F32)
    angle = steps[:, None] * ky_modes[None, :] * (2.0 * jnp.pi / GRID)
    sine = (ky_freq > GRID // 2).astype(F32)
    turns = jnp.concatenate([ky_modes[None], sine[None], jnp.cos(angle), jnp.sin(angle)])
    turns = jnp.pad(turns.T, ((0, 0), (0, TILE - turns.shape[0])))

    partial, table, yt = field_call(everyone, rows, cols, kern, first=(z_rows, turns))
    tables = (everyone, table, yt)
    places = (rank[None].astype(jnp.int32), joined)
    vec, vectors = everyone, [own]
    for step in range(ITERS):
        last = step + 1 == ITERS
        if last:
            final = (wts, *places, *vectors, inv)
            partial, pair = field_call(vec, rows, cols, kern, tables=tables, final=final)
        elif step > 0:
            (partial,) = field_call(vec, rows, cols, kern, tables=tables)
        returned = swap(partial)
        if not last:
            pair = pair_call(tile_list, tile_count, places, vec)
            own, packed = update_call(returned, pair, inv)
            vectors.append(own)
            vec = swap(packed)
    dipoles, residual = finish_call(returned, pair, vectors, inv)
    return (dipoles, residual)


def per_device(positions, *others):
    parts = lax.axis_size("gx")
    atoms = positions.shape[1]
    planes = GRID // parts
    modes = (
        parts * ROWS == GRID
        and atoms == planes * TILE
        and planes == ROWS
        and atoms >= HALO_BLK * TILE
        and ORDER == 5
        and atoms % parts == 0
        and (atoms // parts) % 64 == 0
        and TILE % (atoms // parts) == 0
        and ITERS == 3
    )
    run = per_device_modes if modes else per_device_general
    return run(positions, *others)


def solution(mesh):
    placed = (
        P(None, ("rep", "gx")),
        P(None, ("rep", "gx")),
        P(("rep", "gx")),
        P(None, None, ("rep", "gx")),
        P(None, ("rep", "gx"), None),
        P(("rep", "gx"), None),
        P(("rep", "gx")),
    )
    return jax.shard_map(
        per_device,
        mesh=mesh,
        in_specs=placed,
        out_specs=(P(None, ("rep", "gx")), P(None, ("rep", "gx"))),
        check_vma=False,
    )
```
